256 devices in a mesh: row: 32 (over y, x, core), col: 8 (over z).
Axes of the slice: x: 4, y: 4, z: 8, core: 2. Of those that a mesh axis runs over, the one named last changes fastest.
Arguments:
- sources: float32 [3, 4096, 8192], P(None, 'row', 'col'), may hold values from -32 to 32
- labels: int32 [4096, 8192], P('row', 'col'), may hold values from 0 to 2
Outputs:
- blended: float32 [4096, 8192], P('row', 'col')
- overview_fine: float32 [2048, 4096], P('row', 'col')
- overview_mid: float32 [1024, 2048], P(None, 'col')
- overview_coarse: float32 [512, 1024], P(None, 'col')
The draws below stay inside these ranges and needn't reach their ends.
All inputs are finite; a program needn't handle non-finite values.
Results may differ from the reference program's by a relative error of at most 0.0001.
Values sent between devices are 32-bit elements; how exact they have to be, the bound alone decides.
No kernel may reach another device: no remote copies, remote signals or barrier semaphores. Data moves between devices by JAX's collectives and lax.ppermute only.
A program may use at most 64 MiB of HBM per device.

```python
import jax
import jax.numpy as jnp

K = 3
ITERS = 3
H = 4096
W = 8192


def draw_sources(key, part):
    row_frac = jnp.arange(H, dtype=jnp.float32) / H
    col_frac = jnp.arange(W, dtype=jnp.float32) / W
    amplitude = (1.0 + 2.0 * row_frac)[:, None] * (1.0 + 2.0 * col_frac)[None, :] / 3.0
    noise_draw = jnp.clip(jax.random.normal(key, (K, H, W), jnp.float32), -6.0, 6.0)
    return noise_draw * amplitude


def touch_ends(entries, own_key, smallest, top_value):
    place = [jax.random.randint(jax.random.fold_in(own_key, axis), (), 0, length) for axis, length in enumerate(entries.shape)]
    main_axis = entries.shape.index(max(entries.shape))
    neighbour = place[:main_axis] + [(place[main_axis] + 1) % entries.shape[main_axis]] + place[main_axis + 1:]
    return entries.at[tuple(place)].set(smallest).at[tuple(neighbour)].set(top_value)


def setup_inputs(seed: int = 0) -> dict:
    key_of = jax.random.split(jax.random.key(seed), 3)
    return {
        "sources": draw_sources(jax.random.fold_in(key_of[2], 71), 0),
        "labels": touch_ends(jax.random.randint(key_of[1], (H, W), 0, K), jax.random.fold_in(key_of[1], 1), 0, K - 1).astype(jnp.int32),
    }


def apply_stencil(values):
    padded = jnp.pad(values, 1)
    beside = padded[2:, 1:-1] + padded[:-2, 1:-1]
    beside = beside + padded[1:-1, 2:] + padded[1:-1, :-2]
    return 4.0 * values - beside


def average_pool(values):
    return 0.25 * (values[0::2, 0::2] + values[1::2, 0::2] + values[0::2, 1::2] + values[1::2, 1::2])


def reference(sources, labels):
    right_side = jnp.zeros(labels.shape, jnp.float32)
    for channel in range(K):
        right_side = right_side + jnp.where(labels == channel, apply_stencil(sources[channel]), jnp.float32(0.0))
    blended = jnp.zeros(labels.shape, jnp.float32)
    residual = right_side
    direction = right_side
    norm_now = jnp.sum(residual * residual)
    for iteration in range(ITERS):
        applied = apply_stencil(direction)
        step_size = norm_now / jnp.sum(direction * applied)
        blended = blended + step_size * direction
        residual = residual - step_size * applied
        norm_next = jnp.sum(residual * residual)
        direction = residual + (norm_next / norm_now) * direction
        norm_now = norm_next
    overview_fine = average_pool(blended)
    overview_mid = average_pool(overview_fine)
    overview_coarse = average_pool(overview_mid)
    return (blended, overview_fine, overview_mid, overview_coarse)
```

```python
import jax
import jax.numpy as jnp
from jax import lax
from jax.experimental import pallas as pl
from jax.experimental.pallas import tpu as pltpu
from jax.sharding import Mesh
from jax.sharding import PartitionSpec as P

K = 3
H, W = 128, 1024
TOP = 16
ROWS = TOP + H + 16
LANES = 128
BLOCKS = W // LANES
HALO = 4
ROW = ("row_0", "row_1", "row_2")
CHIP = ("row_0", "row_1")
ALL = ("row_0", "row_1", "row_2", "col")
VMEM = pltpu.MemorySpace.VMEM
ANY = pl.ANY
f32 = jnp.float32


def iota(shape, dim):
    return lax.broadcasted_iota(jnp.int32, shape, dim)


def place():
    row = (lax.axis_index("row_0") * 4 + lax.axis_index("row_1")) * 2 + lax.axis_index("row_2")
    return row, lax.axis_index("col")


def pack_kernel(src, lab, even_out, odd_out, left_out, right_out, rows, cols, lrows, lcols, sem):
    copies = []

    def fetch(a, b):
        c = pltpu.make_async_copy(a, b, sem.at[len(copies)])
        c.start()
        copies.append(c)

    for side, start in ((0, 0), (1, H - 8)):
        fetch(src.at[:, pl.ds(start, 8), :], rows.at[side])
        fetch(lab.at[pl.ds(start, 8), :], lrows.at[side])
    for side, start in ((0, 0), (1, W - LANES)):
        fetch(src.at[:, :, pl.ds(start, LANES)], cols.at[side])
        fetch(lab.at[:, pl.ds(start, LANES)], lcols.at[side])
    for c in copies[:4]:
        c.wait()
    row, _ = place()
    even = (row % 2) == 0
    upper = iota((8, W), 0) < HALO

    def sides(side):
        a = [rows[side, k] for k in range(K)] + [lrows[side].astype(f32)]
        pairs = []
        for x, y in ((a[0], a[1]), (a[2], a[3])):
            if side == 0:
                pairs.append(jnp.where(upper, x, pltpu.roll(y, HALO, 0)))
            else:
                pairs.append(jnp.where(upper, pltpu.roll(x, HALO, 0), y))
        return pairs

    top, bottom = sides(0), sides(1)
    for i in range(2):
        even_out[pl.ds(8 * i, 8), :] = jnp.where(even, bottom[i], top[i])
        odd_out[pl.ds(8 * i, 8), :] = jnp.where(even, top[i], bottom[i])
    for c in copies[4:]:
        c.wait()
    lane = iota((H, LANES), 1)
    for side, out in ((0, left_out), (1, right_out)):
        a = [cols[side, k] for k in range(K)] + [lcols[side].astype(f32)]
        total = jnp.zeros((H, LANES), f32)
        for k in range(K + 1):
            shift = HALO * k + (HALO if side else 0)
            moved = pltpu.roll(a[k], shift, 1) if shift else a[k]
            total = jnp.where((lane >= HALO * k) & (lane < HALO * (k + 1)), moved, total)
        out[...] = total


def pack(sources, labels):
    return pl.pallas_call(
        pack_kernel,
        out_shape=(
            jax.ShapeDtypeStruct((16, W), f32),
            jax.ShapeDtypeStruct((16, W), f32),
            jax.ShapeDtypeStruct((H, LANES), f32),
            jax.ShapeDtypeStruct((H, LANES), f32),
        ),
        in_specs=[pl.BlockSpec(memory_space=ANY)] * 2,
        out_specs=(pl.BlockSpec(memory_space=VMEM),) * 4,
        scratch_shapes=[
            pltpu.VMEM((2, K, 8, W), f32),
            pltpu.VMEM((2, K, H, LANES), f32),
            pltpu.VMEM((2, 8, W), jnp.int32),
            pltpu.VMEM((2, H, LANES), jnp.int32),
            pltpu.SemaphoreType.DMA((8,)),
        ],
        name="pack_rows",
    )(sources, labels)


def corner_kernel(got_even, got_odd, left, right, even_out, odd_out):
    row, col = place()
    row_even = (row % 2) == 0
    col_even = (col % 2) == 0
    upper = iota((8, LANES), 0) < HALO
    lane = iota((8, LANES), 1)
    strips = []
    for side, start in ((0, 0), (1, W - LANES)):
        total = jnp.zeros((8, LANES), f32)
        for k in range(K + 1):
            tile, half = divmod(k, 2)
            at = (pl.ds(8 * tile, 8), pl.ds(start, LANES))
            e, o = got_even[at], got_odd[at]
            above = jnp.where(row_even, o, e)
            below = jnp.where(row_even, e, o)
            if half:
                both = jnp.where(upper, pltpu.roll(above, HALO, 0), below)
            else:
                both = jnp.where(upper, above, pltpu.roll(below, HALO, 0))
            shift = HALO * k + (HALO if side else 0)
            moved = pltpu.roll(both, shift, 1) if shift else both
            total = jnp.where((lane >= HALO * k) & (lane < HALO * (k + 1)), moved, total)
        strips.append(total)
    even_out[pl.ds(0, H), :] = jnp.where(col_even, right[...], left[...])
    odd_out[pl.ds(0, H), :] = jnp.where(col_even, left[...], right[...])
    even_out[pl.ds(H, 8), :] = jnp.where(col_even, strips[1], strips[0])
    odd_out[pl.ds(H, 8), :] = jnp.where(col_even, strips[0], strips[1])


def pack_columns(got_even, got_odd, left, right):
    return pl.pallas_call(
        corner_kernel,
        out_shape=(jax.ShapeDtypeStruct((H + 8, LANES), f32),) * 2,
        in_specs=[pl.BlockSpec(memory_space=VMEM)] * 4,
        out_specs=(pl.BlockSpec(memory_space=VMEM),) * 2,
        name="pack_columns",
    )(got_even, got_odd, left, right)


def two_sum(a, b):
    s = a + b
    t = s - a
    return s, (a - (s - t)) + (b - t)


def exact_total(x):
    s, e = x, jnp.zeros_like(x)
    for shift in (4, 2, 1):
        s, more = two_sum(s, pltpu.roll(s, shift, 0))
        e = e + pltpu.roll(e, shift, 0) + more
    for shift in (64, 32, 16, 8, 4, 2, 1):
        s, more = two_sum(s, pltpu.roll(s, shift, 1))
        e = e + pltpu.roll(e, shift, 1) + more
    return s, e


def beside(ref, j, base):
    vertical = ref[j, pl.ds(base + 1, 8), :] + ref[j, pl.ds(base - 1, 8), :]
    return vertical


def shifted(tiles):
    lane = iota((8, LANES), 1)
    to_left = [pltpu.roll(t, LANES - 1, 1) for t in tiles]
    to_right = [pltpu.roll(t, 1, 1) for t in tiles]
    last, first = lane == LANES - 1, lane == 0
    after, before = [], []
    for j in range(len(tiles)):
        after.append(jnp.where(last, to_left[min(j + 1, len(tiles) - 1)], to_left[j]))
        before.append(jnp.where(first, to_right[max(j - 1, 0)], to_right[j]))
    return after, before


def main_kernel(
    src, lab, r_even, r_odd, c_even, c_odd, v0, v1, v2, sums_out, pooled_out, ext, lext, sem
):
    copies = []
    for k in range(K + 1):
        for j in range(BLOCKS):
            lanes = pl.ds(j * LANES, LANES)
            a = src.at[k, :, lanes] if k < K else lab.at[:, lanes]
            b = ext.at[k, j + 1, pl.ds(TOP, H), :] if k < K else lext.at[j + 1, pl.ds(TOP, H), :]
            c = pltpu.make_async_copy(a, b, sem.at[k, j])
            c.start()
            copies.append(c)
    row, col = place()
    row_even = (row % 2) == 0
    col_even = (col % 2) == 0

    def put(k, j, start, size, value):
        if k < K:
            ext[k, j, pl.ds(start, size), :] = value
        else:
            lext[j, pl.ds(start, size), :] = value.astype(jnp.int32)

    for k in range(K + 1):
        at = pl.ds(HALO * k, HALO)
        for j in range(BLOCKS):
            lanes = pl.ds(j * LANES, LANES)
            e, o = r_even[at, lanes], r_odd[at, lanes]
            put(k, j + 1, TOP - HALO, HALO, jnp.where(row_even, o, e))
            put(k, j + 1, TOP + H, HALO, jnp.where(row_even, e, o))
    for side, j in ((0, 0), (1, BLOCKS + 1)):
        e, o = c_even[...], c_odd[...]
        got = jnp.where(col_even, o, e) if side == 0 else jnp.where(col_even, e, o)
        for k in range(K + 1):
            shift = (LANES - HALO - HALO * k) if side == 0 else (LANES - HALO * k) % LANES
            moved = pltpu.roll(got, shift, 1) if shift else got
            put(k, j, TOP, H, moved[:H])
            put(k, j, TOP - HALO, HALO, moved[H : H + HALO])
            put(k, j, TOP + H, HALO, moved[H + HALO :])

    def outside(ref):
        @pl.when(row == 0)
        def _():
            ref[:, pl.ds(TOP - 8, 8), :] = jnp.zeros((BLOCKS + 2, 8, LANES), f32)

        @pl.when(row == 31)
        def _():
            ref[:, pl.ds(TOP + H, 8), :] = jnp.zeros((BLOCKS + 2, 8, LANES), f32)

        @pl.when(col == 0)
        def _():
            ref[0, :, :] = jnp.zeros((ROWS, LANES), f32)

        @pl.when(col == 7)
        def _():
            ref[BLOCKS + 1, :, :] = jnp.zeros((ROWS, LANES), f32)

    for c in copies:
        c.wait()

    def right_side(t, carry):
        base = pl.multiple_of(TOP - 8 + 8 * t, 8)
        out = [jnp.zeros((8, LANES), f32)] * (BLOCKS + 2)
        picked = [lext[j, pl.ds(base, 8), :] for j in range(BLOCKS + 2)]
        for k in range(K):
            plane = ext.at[k]
            tiles = [plane[j, pl.ds(base, 8), :] for j in range(BLOCKS + 2)]
            after, before = shifted(tiles)
            for j in range(BLOCKS + 2):
                term = 4.0 * tiles[j] - (beside(plane, j, base) + after[j] + before[j])
                out[j] = jnp.where(picked[j] == k, term, out[j])
        for j in range(BLOCKS + 2):
            v0[j, pl.ds(base, 8), :] = out[j]
        return carry

    lax.fori_loop(0, H // 8 + 2, right_side, 0)
    outside(v0)

    def neighbours(source, target):
        def step(t, carry):
            base = pl.multiple_of(TOP - 8 + 8 * t, 8)
            tiles = [source[j, pl.ds(base, 8), :] for j in range(BLOCKS + 2)]
            after, before = shifted(tiles)
            for j in range(BLOCKS + 2):
                target[j, pl.ds(base, 8), :] = beside(source, j, base) + after[j] + before[j]
            return carry

        lax.fori_loop(0, H // 8 + 2, step, 0)
        outside(target)

    neighbours(v0, v1)
    neighbours(v1, v2)

    def products(t, carry):
        base = pl.multiple_of(TOP + 8 * t, 8)
        at = pl.ds(base, 8)
        last = iota((8, LANES), 1) == LANES - 1
        c = [v2[j, at, :] for j in range(1, BLOCKS + 2)]
        rolled = [pltpu.roll(x, LANES - 1, 1) for x in c]
        found = [[] for _ in range(6)]
        for j in range(BLOCKS):
            x0, x1, x2 = v0[j + 1, at, :], v1[j + 1, at, :], c[j]
            x3 = v2[j + 1, pl.ds(base + 1, 8), :] + jnp.where(last, rolled[j + 1], rolled[j])
            for i, (a, b) in enumerate(((x0, x0), (x0, x1), (x1, x1), (x1, x2), (x2, x2), (x2, x3))):
                found[i].append(a * b)
        out = []
        for i in range(6):
            x = found[i]
            while len(x) > 1:
                x = [a + b for a, b in zip(x[0::2], x[1::2])]
            out.append(carry[i] + x[0])
        return tuple(out)

    zero = jnp.zeros((8, LANES), f32)
    totals = lax.fori_loop(0, H // 8, products, (zero,) * 6)
    lane = iota((8, LANES), 1)
    line = zero
    for i in range(6):
        s, e = exact_total(totals[i])
        if i == 5:
            s, e = s + s, e + e
        line = jnp.where(lane == i, s, jnp.where(lane == i + 8, e, line))
    sums_out[...] = jnp.broadcast_to(line[:1], (256, LANES))

    groups = W // 2 // LANES // 2
    spread = jnp.where(iota((512, LANES), 0) // 4 == iota((512, LANES), 1), f32(0.0625), f32(0.0))
    for i, ref in enumerate((v0, v1, v2)):
        for g in range(groups):
            parts = []
            for j in range(4):
                block = 1 + 4 * g + j
                at = [ref[block, pl.ds(TOP + q, H // 4, stride=4), :] for q in range(4)]
                parts.append((at[0] + at[1]) + (at[2] + at[3]))
            pooled_out[i, :, pl.ds(g * LANES, LANES)] = jnp.dot(
                jnp.concatenate(parts, 1), spread, precision=lax.Precision.HIGHEST, preferred_element_type=f32
            )


def main_stage(sources, labels, r_even, r_odd, c_even, c_odd):
    field = jax.ShapeDtypeStruct((BLOCKS + 2, ROWS, LANES), f32)
    return pl.pallas_call(
        main_kernel,
        out_shape=(
            field,
            field,
            field,
            jax.ShapeDtypeStruct((256, LANES), f32),
            jax.ShapeDtypeStruct((3, H // 4, W // 4), f32),
        ),
        in_specs=[pl.BlockSpec(memory_space=ANY)] * 2 + [pl.BlockSpec(memory_space=VMEM)] * 4,
        out_specs=(pl.BlockSpec(memory_space=VMEM),) * 5,
        scratch_shapes=[
            pltpu.VMEM((K, BLOCKS + 2, ROWS, LANES), f32),
            pltpu.VMEM((BLOCKS + 2, ROWS, LANES), jnp.int32),
            pltpu.SemaphoreType.DMA((K + 1, BLOCKS)),
        ],
        name="fields_and_products",
    )(sources, labels, r_even, r_odd, c_even, c_odd)


def two_product(a, b):
    p = a * b
    big = f32(4097.0)
    t = big * a
    ah = t - (t - a)
    al = a - ah
    t = big * b
    bh = t - (t - b)
    bl = b - bh
    return p, ((ah * bh - p) + ah * bl + al * bh) + al * bl


def less_scaled(a, b, scale):
    p, low = two_product(b[0], scale)
    low = low + b[1] * scale
    s, e = two_sum(a[0], -p)
    e = e + (a[1] - low)
    return two_sum(s, e)


def coefficients(n):
    shift = n[1][0] / n[0][0]
    current = n
    m = [n[0][0]]
    for _ in range(5):
        current = [less_scaled(current[i + 1], current[i], shift) for i in range(len(current) - 1)]
        m.append(current[0][0] + current[0][1])
    m0, m1, m2, m3, m4, m5 = m
    t = m1 / m0
    theta0 = shift + t
    m5 = m5 - 5.0 * t * m4
    m4 = m4 - 4.0 * t * m3
    m3 = m3 - 3.0 * t * m2
    m2 = m2 - t * m1
    one = jnp.ones_like(m0)
    zero = jnp.zeros_like(m0)
    second = m2 > 0.0
    safe2 = jnp.where(second, m2, one)
    b1 = jnp.where(second, m2 / m0, zero)
    s = jnp.where(second, m3 / safe2, zero)
    h2 = m4 - s * m3 - b1 * m2
    third = second & (h2 > 0.0)
    safe3 = jnp.where(third, h2, one)
    theta1 = theta0 + s
    theta2 = theta0 - s + (m5 - s * m4 - b1 * m3) / safe3
    b2 = h2 / safe2
    d0, d1, d2 = 4.0 - theta0, 4.0 - theta1, 4.0 - theta2
    e = d1 * d2 - b2
    y2 = jnp.where(third, one / (d0 * e - b1 * d2), zero)
    y1 = jnp.where(third, d2 * y2, jnp.where(second, one / (d0 * d1 - b1), zero))
    y0 = jnp.where(third, e * y2, jnp.where(second, d1 * y1, one / d0))
    return (
        y0 - theta0 * y1 + (theta0 * theta1 - b1) * y2,
        y1 - (theta0 + theta1) * y2,
        y2,
    )


def solve_kernel(all_sums, pooled, coef_out, mid_out):
    tiles = [(all_sums[pl.ds(8 * i, 8), :], jnp.zeros((8, LANES), f32)) for i in range(32)]
    while len(tiles) > 1:
        merged = []
        for a, b in zip(tiles[0::2], tiles[1::2]):
            s, e = two_sum(a[0], b[0])
            merged.append((s, e + (a[1] + b[1])))
        tiles = merged
    s, e = tiles[0]
    for shift in (4, 2, 1):
        s, more = two_sum(s, pltpu.roll(s, shift, 0))
        e = e + pltpu.roll(e, shift, 0) + more
    lane = iota((8, LANES), 1)

    def lane_of(x, i):
        return jnp.broadcast_to(
            jnp.sum(jnp.where(lane == i, x, f32(0.0)), axis=1, keepdims=True), (8, LANES)
        )

    n = [two_sum(lane_of(s, i), lane_of(e, i) + lane_of(s, i + 8)) for i in range(6)]
    c = coefficients(n)
    for i in range(3):
        coef_out[i] = c[i]
    for q in range(H // 4 // 8):
        for g in range(2):
            at = (pl.ds(8 * q, 8), pl.ds(g * LANES, LANES))
            value = c[0] * pooled[(0, *at)] + c[1] * pooled[(1, *at)] + c[2] * pooled[(2, *at)]
            for d in range(16):
                mid_out[(d, *at)] = value


def solve(all_sums, pooled):
    return pl.pallas_call(
        solve_kernel,
        out_shape=(
            jax.ShapeDtypeStruct((3, 8, LANES), f32),
            jax.ShapeDtypeStruct((16, H // 4, W // 4), f32),
        ),
        in_specs=[pl.BlockSpec(memory_space=VMEM)] * 2,
        out_specs=(pl.BlockSpec(memory_space=VMEM),) * 2,
        name="coefficients",
    )(all_sums, pooled)


def half_matrix(rows):
    return jnp.where(iota((rows, rows // 2), 0) // 2 == iota((rows, rows // 2), 1), f32(0.25), f32(0.0))


def blend_kernel(coef, v0, v1, v2, blended_out, fine_out, scratch):
    c = [coef[i] for i in range(3)]

    def step(t, carry):
        base = pl.multiple_of(8 * t, 8)
        for j in range(BLOCKS):
            at = (j + 1, pl.ds(base + TOP, 8), slice(None))
            value = c[0] * v0[at] + c[1] * v1[at] + c[2] * v2[at]
            blended_out[pl.ds(base, 8), pl.ds(j * LANES, LANES)] = value
            scratch[j, pl.ds(base, 8), :] = value
        return carry

    lax.fori_loop(0, H // 8, step, 0)
    half = half_matrix(2 * LANES)
    for g in range(BLOCKS // 2):
        parts = [
            scratch[2 * g + i, pl.ds(0, H // 2, stride=2), :] + scratch[2 * g + i, pl.ds(1, H // 2, stride=2), :]
            for i in range(2)
        ]
        fine_out[:, pl.ds(g * LANES, LANES)] = jnp.dot(
            jnp.concatenate(parts, 1), half, precision=lax.Precision.HIGHEST, preferred_element_type=f32
        )


def blend(coef, v0, v1, v2):
    return pl.pallas_call(
        blend_kernel,
        out_shape=(
            jax.ShapeDtypeStruct((H, W), f32),
            jax.ShapeDtypeStruct((H // 2, W // 2), f32),
        ),
        in_specs=[pl.BlockSpec(memory_space=VMEM)] * 4,
        out_specs=(pl.BlockSpec(memory_space=VMEM),) * 2,
        scratch_shapes=[pltpu.VMEM((BLOCKS, H, LANES), f32)],
        name="blend",
    )(coef, v0, v1, v2)


def assemble_kernel(own, other, mid_out, coarse_out, scratch):
    core = lax.axis_index("row_2")
    n = H // 4
    half = half_matrix(2 * LANES)
    first = core == 0

    def step(d, carry):
        at = pl.multiple_of(d * 2 * n, 2 * n)
        a, b = own[d], other[d]
        low, high = jnp.where(first, a, b), jnp.where(first, b, a)
        mid_out[pl.ds(at, n), :] = low
        mid_out[pl.ds(at + n, n), :] = high
        for g in range(2):
            lanes = slice(g * LANES, (g + 1) * LANES)
            scratch[g, pl.ds(at, n), :] = low[:, lanes]
            scratch[g, pl.ds(at + n, n), :] = high[:, lanes]
        return carry

    lax.fori_loop(0, 16, step, 0)
    parts = [
        scratch[g, pl.ds(0, 16 * n, stride=2), :] + scratch[g, pl.ds(1, 16 * n, stride=2), :] for g in range(2)
    ]
    coarse_out[...] = jnp.dot(
        jnp.concatenate(parts, 1), half, precision=lax.Precision.HIGHEST, preferred_element_type=f32
    )


def assemble(own, other):
    n = H // 4
    return pl.pallas_call(
        assemble_kernel,
        out_shape=(
            jax.ShapeDtypeStruct((32 * n, W // 4), f32),
            jax.ShapeDtypeStruct((16 * n, W // 8), f32),
        ),
        in_specs=[pl.BlockSpec(memory_space=VMEM)] * 2,
        out_specs=(pl.BlockSpec(memory_space=VMEM),) * 2,
        scratch_shapes=[pltpu.VMEM((2, 32 * n, LANES), f32)],
        name="assemble",
    )(own, other)


def swaps(devices, first):
    pairs = [(i, i + 1) for i in range(first, devices - 1, 2)]
    return pairs + [(b, a) for a, b in pairs]


def exchange(even, odd, axis):
    devices = lax.axis_size(axis)
    return lax.ppermute(even, axis, swaps(devices, 0)), lax.ppermute(odd, axis, swaps(devices, 1))


def per_device(sources, labels):
    even, odd, left, right = pack(sources, labels)
    r_even, r_odd = exchange(even, odd, ROW)
    c_even, c_odd = exchange(*pack_columns(r_even, r_odd, left, right), "col")
    v0, v1, v2, sums, pooled = main_stage(sources, labels, r_even, r_odd, c_even, c_odd)
    sums = lax.all_to_all(sums.reshape(256, 1, LANES), ALL, split_axis=0, concat_axis=0, tiled=True)
    coef, mid = solve(sums.reshape(256, LANES), pooled)
    mid = lax.all_to_all(mid, CHIP, split_axis=0, concat_axis=0, tiled=True)
    other = lax.ppermute(mid, "row_2", [(0, 1), (1, 0)])
    blended, fine = blend(coef, v0, v1, v2)
    overview_mid, overview_coarse = assemble(mid, other)
    return (blended, fine, overview_mid, overview_coarse)


def solution(mesh):
    finer = Mesh(
        mesh.devices.reshape(4, 4, 2, mesh.shape["col"]), ("row_0", "row_1", "row_2", "col")
    )
    return jax.shard_map(
        per_device,
        mesh=finer,
        in_specs=(P(None, ROW, "col"), P(ROW, "col")),
        out_specs=(P(ROW, "col"), P(ROW, "col"), P(None, "col"), P(None, "col")),
        check_vma=False,
    )
```

```python
import jax
import jax.numpy as jnp
from jax import lax
from jax.experimental import pallas as pl
from jax.experimental.pallas import tpu as pltpu
from jax.sharding import Mesh
from jax.sharding import PartitionSpec as P

K = 3
H, W = 128, 1024
TOP = 16
ROWS = TOP + H + 16
LANES = 128
BLOCKS = W // LANES
HALO = 4
ROW = ("row_0", "row_1", "row_2")
CHIP = ("row_0", "row_1")
ALL = ("row_0", "row_1", "row_2", "col")
VMEM = pltpu.MemorySpace.VMEM
WHOLE = pl.BlockSpec(memory_space=VMEM)
FAR = pl.BlockSpec(memory_space=pltpu.MemorySpace.HBM)
LIMIT = pltpu.CompilerParams(vmem_limit_bytes=24 * 2**20)
CHUNK = 3
f32 = jnp.float32


def iota(shape, dim):
    return lax.broadcasted_iota(jnp.int32, shape, dim)


def place():
    row = (lax.axis_index("row_0") * 4 + lax.axis_index("row_1")) * 2 + lax.axis_index("row_2")
    return row, lax.axis_index("col")


def near(shape, dtype=f32):
    return pltpu.VMEM(shape, dtype)


def held(*values):
    return [pltpu.with_memory_space_constraint(v, VMEM) for v in values]


def far(*values):
    return [pltpu.with_memory_space_constraint(v, pltpu.MemorySpace.HBM) for v in values]


def cost(us):
    return pl.CostEstimate(flops=int(us * 3e8), bytes_accessed=0, transcendentals=0)


def merge_strips(parts, side, lane):
    total = jnp.zeros_like(parts[0])
    for k in range(K + 1):
        shift = HALO * k + (HALO if side else 0)
        moved = pltpu.roll(parts[k], shift, 1) if shift else parts[k]
        total = jnp.where((lane >= HALO * k) & (lane < HALO * (k + 1)), moved, total)
    return total


def pack_kernel(src, lab, even_out, odd_out, rows, lrows, sem):
    copies = []
    for side, start in ((0, 0), (1, H - 8)):
        for i, (a, b) in enumerate(
            (
                (src.at[:, pl.ds(start, 8), :], rows.at[side]),
                (lab.at[pl.ds(start, 8), :], lrows.at[side]),
            )
        ):
            c = pltpu.make_async_copy(a, b, sem.at[side, i])
            c.start()
            copies.append(c)
    for c in copies:
        c.wait()
    row, _ = place()
    even = (row % 2) == 0
    upper = iota((8, W), 0) < HALO

    def sides(side):
        a = [rows[side, k] for k in range(K)] + [lrows[side].astype(f32)]
        pairs = []
        for x, y in ((a[0], a[1]), (a[2], a[3])):
            if side == 0:
                pairs.append(jnp.where(upper, x, pltpu.roll(y, HALO, 0)))
            else:
                pairs.append(jnp.where(upper, pltpu.roll(x, HALO, 0), y))
        return pairs

    top, bottom = sides(0), sides(1)
    for i in range(2):
        even_out[pl.ds(8 * i, 8), :] = jnp.where(even, bottom[i], top[i])
        odd_out[pl.ds(8 * i, 8), :] = jnp.where(even, top[i], bottom[i])


def pack_rows(sources, labels):
    return pl.pallas_call(
        pack_kernel,
        out_shape=(near((16, W)), near((16, W))),
        in_specs=[FAR] * 2,
        out_specs=(WHOLE,) * 2,
        scratch_shapes=[
            pltpu.VMEM((2, K, 8, W), f32),
            pltpu.VMEM((2, 8, W), jnp.int32),
            pltpu.SemaphoreType.DMA((2, 2)),
        ],
        compiler_params=LIMIT,
        cost_estimate=cost(1),
        name="pack_rows",
    )(*far(sources, labels))


def load_kernel(src, lab, ext, lext, left_out, right_out, sem):
    copies = {}
    for j in (0, BLOCKS - 1, *range(1, BLOCKS - 1)):
        lanes = pl.ds(j * LANES, LANES)
        for k in range(K + 1):
            a = src.at[k, :, lanes] if k < K else lab.at[:, lanes]
            b = ext.at[k, j + 1, pl.ds(TOP, H), :] if k < K else lext.at[j + 1, pl.ds(TOP, H), :]
            c = pltpu.make_async_copy(a, b, sem.at[k, j])
            c.start()
            copies[k, j] = c
    own = pl.ds(TOP, H)
    lane = iota((H, LANES), 1)
    for side, out in ((0, left_out), (1, right_out)):
        j = side * (BLOCKS - 1)
        for k in range(K + 1):
            copies.pop((k, j)).wait()
        parts = [ext[k, j + 1, own, :] for k in range(K)] + [lext[j + 1, own, :].astype(f32)]
        out[...] = merge_strips(parts, side, lane)
    for c in copies.values():
        c.wait()


def load(sources, labels):
    return pl.pallas_call(
        load_kernel,
        out_shape=(
            near((K, BLOCKS + 2, ROWS, LANES)),
            near((BLOCKS + 2, ROWS, LANES), jnp.int32),
            near((H, LANES)),
            near((H, LANES)),
        ),
        in_specs=[FAR] * 2,
        out_specs=(WHOLE,) * 4,
        scratch_shapes=[pltpu.SemaphoreType.DMA((K + 1, BLOCKS))],
        compiler_params=LIMIT,
        cost_estimate=cost(2),
        name="load_block",
    )(*far(sources, labels))


def corner_kernel(got_even, got_odd, left, right, even_out, odd_out):
    row, col = place()
    row_even = (row % 2) == 0
    col_even = (col % 2) == 0
    upper = iota((8, LANES), 0) < HALO
    lane = iota((8, LANES), 1)
    strips = []
    for side, start in ((0, 0), (1, W - LANES)):
        parts = []
        for k in range(K + 1):
            tile, half = divmod(k, 2)
            at = (pl.ds(8 * tile, 8), pl.ds(start, LANES))
            e, o = got_even[at], got_odd[at]
            above = jnp.where(row_even, o, e)
            below = jnp.where(row_even, e, o)
            if half:
                parts.append(jnp.where(upper, pltpu.roll(above, HALO, 0), below))
            else:
                parts.append(jnp.where(upper, above, pltpu.roll(below, HALO, 0)))
        strips.append(merge_strips(parts, side, lane))
    even_out[pl.ds(0, H), :] = jnp.where(col_even, right[...], left[...])
    odd_out[pl.ds(0, H), :] = jnp.where(col_even, left[...], right[...])
    even_out[pl.ds(H, 8), :] = jnp.where(col_even, strips[1], strips[0])
    odd_out[pl.ds(H, 8), :] = jnp.where(col_even, strips[0], strips[1])


def pack_columns(got_even, got_odd, left, right):
    return pl.pallas_call(
        corner_kernel,
        out_shape=(near((H + 8, LANES)),) * 2,
        in_specs=[WHOLE] * 4,
        out_specs=(WHOLE,) * 2,
        compiler_params=LIMIT,
        cost_estimate=cost(0.5),
        name="pack_columns",
    )(*held(got_even, got_odd, left, right))


def two_sum(a, b):
    s = a + b
    t = s - a
    return s, (a - (s - t)) + (b - t)


def shifted(tiles):
    lane = iota((8, LANES), 1)
    to_left = [pltpu.roll(t, LANES - 1, 1) for t in tiles]
    to_right = [pltpu.roll(t, 1, 1) for t in tiles]
    last, first = lane == LANES - 1, lane == 0
    n = len(tiles)
    after = [jnp.where(last, to_left[min(j + 1, n - 1)], to_left[j]) for j in range(n)]
    before = [jnp.where(first, to_right[max(j - 1, 0)], to_right[j]) for j in range(n)]
    return after, before


def right_side(ext, lext, out, runs):
    def step(t, carry):
        for u in range(CHUNK):
            base = pl.multiple_of(TOP - 8 + 8 * (CHUNK * t + u), 8)
            for start, count, keep in runs:
                total = {j: jnp.zeros((8, LANES), f32) for j in keep}
                picked = {j: lext[j, pl.ds(base, 8), :] for j in keep}
                for k in range(K):
                    tiles = [ext[k, start + i, pl.ds(base, 8), :] for i in range(count)]
                    after, before = shifted(tiles)
                    for j in keep:
                        i = j - start
                        vertical = ext[k, j, pl.ds(base + 1, 8), :] + ext[k, j, pl.ds(base - 1, 8), :]
                        term = 4.0 * tiles[i] - (vertical + after[i] + before[i])
                        total[j] = jnp.where(picked[j] == k, term, total[j])
                for j in keep:
                    out[j, pl.ds(base, 8), :] = total[j]
        return carry

    lax.fori_loop(0, (H // 8 + 2) // CHUNK, step, 0)


def neighbours(source, target, runs):
    def step(t, carry):
        for u in range(2 * CHUNK):
            base = pl.multiple_of(TOP - 8 + 8 * (2 * CHUNK * t + u), 8)
            for start, count, keep in runs:
                tiles = [source[start + i, pl.ds(base, 8), :] for i in range(count)]
                after, before = shifted(tiles)
                for j in keep:
                    i = j - start
                    vertical = source[j, pl.ds(base + 1, 8), :] + source[j, pl.ds(base - 1, 8), :]
                    target[j, pl.ds(base, 8), :] = vertical + after[i] + before[i]
        return carry

    lax.fori_loop(0, (H // 8 + 2) // CHUNK // 2, step, 0)


def products(v0, v1, v2, blocks, totals):
    def step(t, carry):
        totals = carry
        for u in range(2):
            base = pl.multiple_of(TOP + 8 * (2 * t + u), 8)
            at = pl.ds(base, 8)
            last = iota((8, LANES), 1) == LANES - 1
            found = [[] for _ in range(6)]
            rolled = {}
            for j in blocks:
                for i in (j, j + 1):
                    if i not in rolled:
                        rolled[i] = pltpu.roll(v2[i, at, :], LANES - 1, 1)
                x0, x1, x2 = v0[j, at, :], v1[j, at, :], v2[j, at, :]
                x3 = v2[j, pl.ds(base + 1, 8), :] + jnp.where(last, rolled[j + 1], rolled[j])
                for i, (a, b) in enumerate(((x0, x0), (x0, x1), (x1, x1), (x1, x2), (x2, x2), (x2, x3))):
                    found[i].append(a * b)
            out = []
            for i in range(6):
                x = found[i]
                while len(x) > 1:
                    x = [sum(x[a : a + 2][1:], x[a]) for a in range(0, len(x), 2)]
                out.append(totals[i] + x[0])
            totals = tuple(out)
        return totals

    return lax.fori_loop(0, H // 16, step, totals)


def clear_outside(ref, blocks, rows, columns):
    row, col = place()
    zero = jnp.zeros((8, LANES), f32)
    if rows:

        @pl.when(row == 0)
        def _():
            for j in blocks:
                ref[j, pl.ds(TOP - 8, 8), :] = zero

        @pl.when(row == 31)
        def _():
            for j in blocks:
                ref[j, pl.ds(TOP + H, 8), :] = zero

    if columns:

        @pl.when(col == 0)
        def _():
            ref[0, :, :] = jnp.zeros((ROWS, LANES), f32)

        @pl.when(col == 7)
        def _():
            ref[BLOCKS + 1, :, :] = jnp.zeros((ROWS, LANES), f32)


def inner_kernel(ext_in, lext_in, r_even, r_odd, ext, lext, v0, v1, v2, totals_out):
    del ext_in, lext_in
    row, _ = place()
    row_even = (row % 2) == 0
    for k in range(K + 1):
        at = pl.ds(HALO * k, HALO)
        for j in range(BLOCKS):
            lanes = pl.ds(j * LANES, LANES)
            e, o = r_even[at, lanes], r_odd[at, lanes]
            above, below = jnp.where(row_even, o, e), jnp.where(row_even, e, o)
            for start, value in ((TOP - HALO, above), (TOP + H, below)):
                if k < K:
                    ext[k, j + 1, pl.ds(start, HALO), :] = value
                else:
                    lext[j + 1, pl.ds(start, HALO), :] = value.astype(jnp.int32)
    runs = ((1, BLOCKS, range(1, BLOCKS + 1)),)
    right_side(ext, lext, v0, runs)
    clear_outside(v0, range(1, BLOCKS + 1), True, False)
    neighbours(v0, v1, runs)
    clear_outside(v1, range(1, BLOCKS + 1), True, False)
    neighbours(v1, v2, runs)
    clear_outside(v2, range(1, BLOCKS + 1), True, False)
    totals = products(v0, v1, v2, range(2, BLOCKS), (jnp.zeros((8, LANES), f32),) * 6)
    for i in range(6):
        totals_out[i] = totals[i]


def inner(ext, lext, r_even, r_odd):
    field = near((BLOCKS + 2, ROWS, LANES))
    return pl.pallas_call(
        inner_kernel,
        out_shape=(
            near((K, BLOCKS + 2, ROWS, LANES)),
            near((BLOCKS + 2, ROWS, LANES), jnp.int32),
            field,
            field,
            field,
            near((6, 8, LANES)),
        ),
        in_specs=[WHOLE] * 4,
        out_specs=(WHOLE,) * 6,
        input_output_aliases={0: 0, 1: 1},
        compiler_params=LIMIT,
        cost_estimate=cost(3),
        name="inner_fields",
    )(*held(ext, lext, r_even, r_odd))


def outer_kernel(
    ext_in, lext_in, v0_in, v1_in, v2_in, totals_in, c_even, c_odd, ext, lext, v0, v1, v2, sums_out
):
    del ext_in, lext_in, v0_in, v1_in, v2_in
    _, col = place()
    col_even = (col % 2) == 0
    for side, j in ((0, 0), (1, BLOCKS + 1)):
        e, o = c_even[...], c_odd[...]
        got = jnp.where(col_even, o, e) if side == 0 else jnp.where(col_even, e, o)
        for k in range(K + 1):
            shift = (LANES - HALO - HALO * k) if side == 0 else (LANES - HALO * k) % LANES
            moved = pltpu.roll(got, shift, 1) if shift else got
            for start, size, value in (
                (TOP, H, moved[:H]),
                (TOP - HALO, HALO, moved[H : H + HALO]),
                (TOP + H, HALO, moved[H + HALO :]),
            ):
                if k < K:
                    ext[k, j, pl.ds(start, size), :] = value
                else:
                    lext[j, pl.ds(start, size), :] = value.astype(jnp.int32)
    last = BLOCKS + 1
    runs = ((0, 3, (0, 1)), (last - 2, 3, (last - 1, last)))
    blocks = (0, 1, last - 1, last)
    right_side(ext, lext, v0, runs)
    clear_outside(v0, blocks, True, True)
    neighbours(v0, v1, runs)
    clear_outside(v1, blocks, True, True)
    neighbours(v1, v2, runs)
    clear_outside(v2, blocks, True, True)
    totals = products(v0, v1, v2, (1, BLOCKS), tuple(totals_in[i] for i in range(6)))

    lane = iota((8, LANES), 1)
    line = jnp.zeros((8, LANES), f32)
    for i in range(6):
        x = totals[i] + totals[i] if i == 5 else totals[i]
        big = 512.0 * jnp.max(jnp.abs(x), axis=1, keepdims=True)
        high = (x + big) - big
        line = jnp.where(
            (lane == i) | (lane == i + 16),
            jnp.sum(high, axis=1, keepdims=True),
            jnp.where(lane == i + 8, jnp.sum(x - high, axis=1, keepdims=True), line),
        )
    s, e = line, jnp.zeros_like(line)
    for shift in (4, 2, 1):
        s, more = two_sum(s, pltpu.roll(s, shift, 0))
        e = e + pltpu.roll(e, shift, 0) + more
    sums_out[...] = jnp.broadcast_to(jnp.where(lane < 16, s, e)[:1], (256, LANES))


def outer(ext, lext, v0, v1, v2, totals, c_even, c_odd):
    field = near((BLOCKS + 2, ROWS, LANES))
    return pl.pallas_call(
        outer_kernel,
        out_shape=(
            near((K, BLOCKS + 2, ROWS, LANES)),
            near((BLOCKS + 2, ROWS, LANES), jnp.int32),
            field,
            field,
            field,
            near((256, LANES)),
        ),
        in_specs=[WHOLE] * 8,
        out_specs=(WHOLE,) * 6,
        input_output_aliases={i: i for i in range(5)},
        compiler_params=LIMIT,
        cost_estimate=cost(2),
        name="outer_fields",
    )(*held(ext, lext, v0, v1, v2, totals, c_even, c_odd))[2:]


def pool_kernel(v0, v1, v2, out):
    spread = jnp.where(iota((512, LANES), 0) // 4 == iota((512, LANES), 1), f32(0.0625), f32(0.0))
    for i, ref in enumerate((v0, v1, v2)):
        for g in range(2):
            parts = []
            for j in range(4):
                block = 1 + 4 * g + j
                at = [ref[block, pl.ds(TOP + q, H // 4, stride=4), :] for q in range(4)]
                parts.append((at[0] + at[1]) + (at[2] + at[3]))
            out[i, g] = jnp.dot(
                jnp.concatenate(parts, 1), spread, precision=lax.Precision.HIGHEST, preferred_element_type=f32
            )


def pool(v0, v1, v2):
    return pl.pallas_call(
        pool_kernel,
        out_shape=near((3, 2, H // 4, LANES)),
        in_specs=[WHOLE] * 3,
        out_specs=WHOLE,
        compiler_params=LIMIT,
        cost_estimate=cost(2),
        name="pool_fields",
    )(*held(v0, v1, v2))


def two_product(a, b):
    p = a * b
    big = f32(4097.0)
    t = big * a
    ah = t - (t - a)
    al = a - ah
    t = big * b
    bh = t - (t - b)
    bl = b - bh
    return p, ((ah * bh - p) + ah * bl + al * bh) + al * bl


def less_scaled(a, b, scale):
    p, low = two_product(b[0], scale)
    low = low + b[1] * scale
    s, e = two_sum(a[0], -p)
    e = e + (a[1] - low)
    return two_sum(s, e)


def coefficients(n):
    shift = n[1][0] / n[0][0]
    current = n
    m = [n[0][0]]
    for _ in range(5):
        current = [less_scaled(current[i + 1], current[i], shift) for i in range(len(current) - 1)]
        m.append(current[0][0] + current[0][1])
    m0, m1, m2, m3, m4, m5 = m
    t = m1 / m0
    theta0 = shift + t
    m5 = m5 - 5.0 * t * m4
    m4 = m4 - 4.0 * t * m3
    m3 = m3 - 3.0 * t * m2
    m2 = m2 - t * m1
    one = jnp.ones_like(m0)
    zero = jnp.zeros_like(m0)
    second = m2 > 0.0
    safe2 = jnp.where(second, m2, one)
    b1 = jnp.where(second, m2 / m0, zero)
    s = jnp.where(second, m3 / safe2, zero)
    h2 = m4 - s * m3 - b1 * m2
    third = second & (h2 > 0.0)
    safe3 = jnp.where(third, h2, one)
    theta1 = theta0 + s
    theta2 = theta0 - s + (m5 - s * m4 - b1 * m3) / safe3
    b2 = h2 / safe2
    d0, d1, d2 = 4.0 - theta0, 4.0 - theta1, 4.0 - theta2
    e = d1 * d2 - b2
    y2 = jnp.where(third, one / (d0 * e - b1 * d2), zero)
    y1 = jnp.where(third, d2 * y2, jnp.where(second, one / (d0 * d1 - b1), zero))
    y0 = jnp.where(third, e * y2, jnp.where(second, d1 * y1, one / d0))
    return (
        y0 - theta0 * y1 + (theta0 * theta1 - b1) * y2,
        y1 - (theta0 + theta1) * y2,
        y2,
    )


def solve_kernel(all_sums, pooled, coef_out, mid_out):
    tiles = [(all_sums[pl.ds(8 * i, 8), :], jnp.zeros((8, LANES), f32)) for i in range(32)]
    while len(tiles) > 1:
        merged = []
        for a, b in zip(tiles[0::2], tiles[1::2]):
            s, e = two_sum(a[0], b[0])
            merged.append((s, e + (a[1] + b[1])))
        tiles = merged
    s, e = tiles[0]
    for shift in (4, 2, 1):
        s, more = two_sum(s, pltpu.roll(s, shift, 0))
        e = e + pltpu.roll(e, shift, 0) + more
    lane = iota((8, LANES), 1)
    zero = jnp.zeros((8, LANES), f32)

    def over_lanes(x):
        return jnp.broadcast_to(jnp.sum(x, axis=1, keepdims=True), (8, LANES))

    n = []
    for i in range(6):
        high = over_lanes(jnp.where(lane == i, s, zero))
        low = over_lanes(jnp.where((lane == i + 8) | (lane == i + 16), s, jnp.where(lane == i, e, zero)))
        n.append(two_sum(high, low))
    c = coefficients(n)
    for i in range(3):
        coef_out[i] = c[i]
    for g in range(2):
        for q in range(H // 4 // 8):
            at = (g, pl.ds(8 * q, 8), slice(None))
            value = c[0] * pooled[(0, *at)] + c[1] * pooled[(1, *at)] + c[2] * pooled[(2, *at)]
            for d in range(16):
                mid_out[(d, *at)] = value


def solve(all_sums, pooled):
    return pl.pallas_call(
        solve_kernel,
        out_shape=(near((3, 8, LANES)), near((16, 2, H // 4, LANES))),
        in_specs=[WHOLE] * 2,
        out_specs=(WHOLE,) * 2,
        compiler_params=LIMIT,
        cost_estimate=cost(1),
        name="coefficients",
    )(*held(all_sums, pooled))


def half_matrix(rows):
    return jnp.where(iota((rows, rows // 2), 0) // 2 == iota((rows, rows // 2), 1), f32(0.25), f32(0.0))


def blend_kernel(coef, v0, v1, v2, blended_out, fine_out, scratch):
    c = [coef[i] for i in range(3)]

    def step(t, carry):
        for u in range(4):
            base = pl.multiple_of(32 * t + 8 * u, 8)
            for j in range(BLOCKS):
                at = (j + 1, pl.ds(base + TOP, 8), slice(None))
                value = c[0] * v0[at] + c[1] * v1[at] + c[2] * v2[at]
                blended_out[pl.ds(base, 8), pl.ds(j * LANES, LANES)] = value
                scratch[j, pl.ds(base, 8), :] = value
        return carry

    lax.fori_loop(0, H // 32, step, 0)
    half = half_matrix(2 * LANES)
    for g in range(BLOCKS // 2):
        parts = [
            scratch[2 * g + i, pl.ds(0, H // 2, stride=2), :] + scratch[2 * g + i, pl.ds(1, H // 2, stride=2), :]
            for i in range(2)
        ]
        fine_out[:, pl.ds(g * LANES, LANES)] = jnp.dot(
            jnp.concatenate(parts, 1), half, precision=lax.Precision.HIGHEST, preferred_element_type=f32
        )


def blend(coef, v0, v1, v2):
    return pl.pallas_call(
        blend_kernel,
        out_shape=(
            jax.ShapeDtypeStruct((H, W), f32),
            jax.ShapeDtypeStruct((H // 2, W // 2), f32),
        ),
        in_specs=[WHOLE] * 4,
        out_specs=(WHOLE,) * 2,
        scratch_shapes=[pltpu.VMEM((BLOCKS, H, LANES), f32)],
        compiler_params=LIMIT,
        cost_estimate=cost(3),
        name="blend",
    )(*held(coef, v0, v1, v2))


def assemble_kernel(own, other, mid_out, coarse_out, scratch, sem):
    core = lax.axis_index("row_2")
    half = half_matrix(2 * LANES)
    copies = []
    for i, (x, c) in enumerate(((own, core), (other, 1 - core))):
        for g in range(2):
            copy = pltpu.make_async_copy(
                x.at[:, g], mid_out.at[:, c, :, pl.ds(g * LANES, LANES)], sem.at[i, g]
            )
            copy.start()
            copies.append(copy)
    rows = H // 8
    for x, c in ((own, core), (other, 1 - core)):
        parts = [
            jnp.concatenate(
                [x[d, g, pl.ds(0, rows, stride=2), :] + x[d, g, pl.ds(1, rows, stride=2), :] for d in range(16)], 0
            )
            for g in range(2)
        ]
        pooled = jnp.dot(
            jnp.concatenate(parts, 1), half, precision=lax.Precision.HIGHEST, preferred_element_type=f32
        )
        for d in range(16):
            scratch[d, c] = pooled[d * rows : (d + 1) * rows]
    copy = pltpu.make_async_copy(scratch, coarse_out, sem.at[2, 0])
    copy.start()
    copies.append(copy)
    for copy in copies:
        copy.wait()


def assemble(own, other):
    mid, coarse = pl.pallas_call(
        assemble_kernel,
        out_shape=(
            jax.ShapeDtypeStruct((16, 2, H // 4, W // 4), f32),
            jax.ShapeDtypeStruct((16, 2, H // 8, W // 8), f32),
        ),
        in_specs=[WHOLE] * 2,
        out_specs=(FAR,) * 2,
        scratch_shapes=[
            pltpu.VMEM((16, 2, H // 8, LANES), f32),
            pltpu.SemaphoreType.DMA((3, 2)),
        ],
        compiler_params=LIMIT,
        cost_estimate=cost(2),
        name="assemble",
    )(*held(own, other))
    return mid.reshape(8 * H, W // 4), coarse.reshape(4 * H, W // 8)


def swaps(devices, first):
    pairs = [(i, i + 1) for i in range(first, devices - 1, 2)]
    return pairs + [(b, a) for a, b in pairs]


def exchange(even, odd, axis):
    devices = lax.axis_size(axis)
    return lax.ppermute(even, axis, swaps(devices, 0)), lax.ppermute(odd, axis, swaps(devices, 1))


def per_device(sources, labels):
    r_even, r_odd = exchange(*pack_rows(sources, labels), ROW)
    ext, lext, left, right = load(sources, labels)
    c_even, c_odd = exchange(*pack_columns(r_even, r_odd, left, right), "col")
    ext, lext, v0, v1, v2, totals = inner(ext, lext, r_even, r_odd)
    v0, v1, v2, sums = outer(ext, lext, v0, v1, v2, totals, c_even, c_odd)
    pooled = pool(v0, v1, v2)
    sums = lax.all_to_all(sums.reshape(256, 1, LANES), ALL, split_axis=0, concat_axis=0, tiled=True)
    coef, mid = solve(sums.reshape(256, LANES), pooled)
    mid = lax.all_to_all(mid, CHIP, split_axis=0, concat_axis=0, tiled=True)
    other = lax.ppermute(mid, "row_2", [(0, 1), (1, 0)])
    blended, fine = blend(coef, v0, v1, v2)
    overview_mid, overview_coarse = assemble(mid, other)
    return (blended, fine, overview_mid, overview_coarse)


def solution(mesh):
    finer = Mesh(
        mesh.devices.reshape(4, 4, 2, mesh.shape["col"]), ("row_0", "row_1", "row_2", "col")
    )
    return jax.shard_map(
        per_device,
        mesh=finer,
        in_specs=(P(None, ROW, "col"), P(ROW, "col")),
        out_specs=(P(ROW, "col"), P(ROW, "col"), P(None, "col"), P(None, "col")),
        check_vma=False,
    )
```

```python
import jax
import jax.numpy as jnp
from jax import lax
from jax.experimental import pallas as pl
from jax.experimental.pallas import tpu as pltpu
from jax.sharding import Mesh
from jax.sharding import PartitionSpec as P

K = 3
H, W = 128, 1024
TOP = 16
ROWS = TOP + H + 24
LANES = 128
BLOCKS = W // LANES
HALO = 4
ROW = ("row_0", "row_1", "row_2")
CHIP = ("row_0", "row_1")
ALL = ("row_0", "row_1", "row_2", "col")
VMEM = pltpu.MemorySpace.VMEM
WHOLE = pl.BlockSpec(memory_space=VMEM)
FAR = pl.BlockSpec(memory_space=pltpu.MemorySpace.HBM)
LIMIT = pltpu.CompilerParams(vmem_limit_bytes=24 * 2**20)
CHUNK = 3
TILES = H // 8
LEFT, RIGHT = HALO, 64
SEAM = 12
f32 = jnp.float32


def iota(shape, dim):
    return lax.broadcasted_iota(jnp.int32, shape, dim)


def place():
    row = (lax.axis_index("row_0") * 4 + lax.axis_index("row_1")) * 2 + lax.axis_index("row_2")
    return row, lax.axis_index("col")


def near(shape, dtype=f32):
    return pltpu.VMEM(shape, dtype)


def held(*values):
    return [pltpu.with_memory_space_constraint(v, VMEM) for v in values]


def far(*values):
    return [pltpu.with_memory_space_constraint(v, pltpu.MemorySpace.HBM) for v in values]


def cost(us):
    return pl.CostEstimate(flops=int(us * 3e8), bytes_accessed=0, transcendentals=0)


def pack_kernel(src, lab, even_out, odd_out, rows, lrows, sem):
    copies = []
    for side, start in ((0, 0), (1, H - 8)):
        for i, (a, b) in enumerate(
            (
                (src.at[:, pl.ds(start, 8), :], rows.at[side]),
                (lab.at[pl.ds(start, 8), :], lrows.at[side]),
            )
        ):
            c = pltpu.make_async_copy(a, b, sem.at[side, i])
            c.start()
            copies.append(c)
    for c in copies:
        c.wait()
    row, _ = place()
    even = (row % 2) == 0
    upper = iota((8, W), 0) < HALO

    def sides(side):
        a = [rows[side, k] for k in range(K)] + [lrows[side].astype(f32)]
        pairs = []
        for x, y in ((a[0], a[1]), (a[2], a[3])):
            if side == 0:
                pairs.append(jnp.where(upper, x, pltpu.roll(y, HALO, 0)))
            else:
                pairs.append(jnp.where(upper, pltpu.roll(x, HALO, 0), y))
        return pairs

    top, bottom = sides(0), sides(1)
    for i in range(2):
        even_out[pl.ds(8 * i, 8), :] = jnp.where(even, bottom[i], top[i])
        odd_out[pl.ds(8 * i, 8), :] = jnp.where(even, top[i], bottom[i])


def pack_rows(sources, labels):
    return pl.pallas_call(
        pack_kernel,
        out_shape=(near((16, W)), near((16, W))),
        in_specs=[FAR] * 2,
        out_specs=(WHOLE,) * 2,
        scratch_shapes=[
            pltpu.VMEM((2, K, 8, W), f32),
            pltpu.VMEM((2, 8, W), jnp.int32),
            pltpu.SemaphoreType.DMA((2, 2)),
        ],
        compiler_params=LIMIT,
        cost_estimate=cost(1),
        name="pack_rows",
    )(*far(sources, labels))


def window(lane, start, size):
    return (lane >= start) & (lane < start + size)


def turn(x, shift):
    shift %= LANES
    return pltpu.roll(x, shift, 1) if shift else x


def load_kernel(src, lab, ext, lext, left_out, right_out, sem):
    copies = {}
    for j in (0, BLOCKS - 1, *range(1, BLOCKS - 1)):
        lanes = pl.ds(j * LANES, LANES)
        for k in range(K + 1):
            a = src.at[k, :, lanes] if k < K else lab.at[:, lanes]
            b = ext.at[k, j, pl.ds(TOP, H), :] if k < K else lext.at[j, pl.ds(TOP, H), :]
            c = pltpu.make_async_copy(a, b, sem.at[k, j])
            c.start()
            copies[k, j] = c
    lane = iota((8, LANES), 1)
    for j, out, first in ((0, left_out, 0), (BLOCKS - 1, right_out, LANES - HALO)):
        for k in range(K + 1):
            copies.pop((k, j)).wait()
        for half in range(2):
            total = jnp.zeros((8, LANES), f32)
            for g in range(8):
                at = pl.ds(TOP + 64 * half + 8 * g, 8)
                for k in range(K + 1):
                    x = ext[k, j, at, :] if k < K else lext[j, at, :].astype(f32)
                    to = 16 * g + HALO * k
                    total = jnp.where(window(lane, to, HALO), turn(x, to - first), total)
            out[pl.ds(8 * half, 8), :] = total
    for c in copies.values():
        c.wait()


def load(sources, labels):
    return pl.pallas_call(
        load_kernel,
        out_shape=(
            near((K, BLOCKS, ROWS, LANES)),
            near((BLOCKS, ROWS, LANES), jnp.int32),
            near((16, LANES)),
            near((16, LANES)),
        ),
        in_specs=[FAR] * 2,
        out_specs=(WHOLE,) * 4,
        scratch_shapes=[pltpu.SemaphoreType.DMA((K + 1, BLOCKS))],
        compiler_params=LIMIT,
        cost_estimate=cost(2),
        name="load_block",
    )(*far(sources, labels))


def corner_kernel(got_even, got_odd, left, right, even_out, odd_out):
    row, col = place()
    row_even = (row % 2) == 0
    col_even = (col % 2) == 0
    upper = iota((8, LANES), 0) < HALO
    lane = iota((8, LANES), 1)
    strips = []
    for start, first in ((0, 0), (W - LANES, LANES - HALO)):
        total = jnp.zeros((8, LANES), f32)
        for k in range(K + 1):
            tile, half = divmod(k, 2)
            at = (pl.ds(8 * tile, 8), pl.ds(start, LANES))
            e, o = got_even[at], got_odd[at]
            above = jnp.where(row_even, o, e)
            below = jnp.where(row_even, e, o)
            if half:
                both = jnp.where(upper, pltpu.roll(above, HALO, 0), below)
            else:
                both = jnp.where(upper, above, pltpu.roll(below, HALO, 0))
            total = jnp.where(window(lane, HALO * k, HALO), turn(both, HALO * k - first), total)
        strips.append(total)
    even_out[pl.ds(0, 16), :] = jnp.where(col_even, right[...], left[...])
    odd_out[pl.ds(0, 16), :] = jnp.where(col_even, left[...], right[...])
    even_out[pl.ds(16, 8), :] = jnp.where(col_even, strips[1], strips[0])
    odd_out[pl.ds(16, 8), :] = jnp.where(col_even, strips[0], strips[1])


def pack_columns(got_even, got_odd, left, right):
    return pl.pallas_call(
        corner_kernel,
        out_shape=(near((24, LANES)),) * 2,
        in_specs=[WHOLE] * 4,
        out_specs=(WHOLE,) * 2,
        compiler_params=LIMIT,
        cost_estimate=cost(0.5),
        name="pack_columns",
    )(*held(got_even, got_odd, left, right))


def two_sum(a, b):
    s = a + b
    t = s - a
    return s, (a - (s - t)) + (b - t)


def shifted(tiles):
    lane = iota((8, LANES), 1)
    to_left = [pltpu.roll(t, LANES - 1, 1) for t in tiles]
    to_right = [pltpu.roll(t, 1, 1) for t in tiles]
    last, first = lane == LANES - 1, lane == 0
    n = len(tiles)
    after = [jnp.where(last, to_left[min(j + 1, n - 1)], to_left[j]) for j in range(n)]
    before = [jnp.where(first, to_right[max(j - 1, 0)], to_right[j]) for j in range(n)]
    return after, before


PAIRS = ((0, 0), (0, 1), (1, 1), (1, 2), (2, 2), (2, 3))


def right_side(ext, lext, out):
    def step(t, carry):
        for u in range(CHUNK):
            base = pl.multiple_of(TOP - 8 + 8 * (CHUNK * t + u), 8)
            total = [jnp.zeros((8, LANES), f32)] * BLOCKS
            picked = [lext[j, pl.ds(base, 8), :] for j in range(BLOCKS)]
            for k in range(K):
                tiles = [ext[k, j, pl.ds(base, 8), :] for j in range(BLOCKS)]
                after, before = shifted(tiles)
                for j in range(BLOCKS):
                    vertical = ext[k, j, pl.ds(base + 1, 8), :] + ext[k, j, pl.ds(base - 1, 8), :]
                    term = 4.0 * tiles[j] - (vertical + after[j] + before[j])
                    total[j] = jnp.where(picked[j] == k, term, total[j])
            for j in range(BLOCKS):
                out[j, pl.ds(base, 8), :] = total[j]
        return carry

    lax.fori_loop(0, (TILES + 2) // CHUNK, step, 0)


def neighbours(source, target):
    def step(t, carry):
        for u in range(2 * CHUNK):
            base = pl.multiple_of(TOP - 8 + 8 * (2 * CHUNK * t + u), 8)
            tiles = [source[j, pl.ds(base, 8), :] for j in range(BLOCKS)]
            after, before = shifted(tiles)
            for j in range(BLOCKS):
                vertical = source[j, pl.ds(base + 1, 8), :] + source[j, pl.ds(base - 1, 8), :]
                target[j, pl.ds(base, 8), :] = vertical + after[j] + before[j]
        return carry

    lax.fori_loop(0, (TILES + 2) // CHUNK // 2, step, 0)


def tree(x):
    while len(x) > 1:
        x = [sum(x[a : a + 2][1:], x[a]) for a in range(0, len(x), 2)]
    return x[0]


def products(v0, v1, v2):
    lane = iota((8, LANES), 1)
    last = lane == LANES - 1
    kept = {0: lane >= HALO, BLOCKS - 1: lane < LANES - HALO}

    def step(t, totals):
        for u in range(2):
            base = pl.multiple_of(TOP + 8 * (2 * t + u), 8)
            at = pl.ds(base, 8)
            found = [[] for _ in PAIRS]
            rolled = [turn(v2[j, at, :], -1) for j in range(BLOCKS)]
            for j in range(BLOCKS):
                x = [v[j, at, :] for v in (v0, v1, v2)]
                right = jnp.where(last, rolled[min(j + 1, BLOCKS - 1)], rolled[j])
                x.append(v2[j, pl.ds(base + 1, 8), :] + right)
                own = [jnp.where(kept[j], a, 0.0) for a in x[:3]] if j in kept else x
                for i, (a, b) in enumerate(PAIRS):
                    found[i].append(own[a] * x[b])
            totals = tuple(total + tree(f) for total, f in zip(totals, found))
        return totals

    return lax.fori_loop(0, TILES // 2, step, (jnp.zeros((8, LANES), f32),) * 6)


def clear_rows(ref, row):
    @pl.when(row == 0)
    def _():
        for j in range(BLOCKS):
            ref[j, pl.ds(TOP - 8, 8), :] = jnp.zeros((8, LANES), f32)

    @pl.when(row == 31)
    def _():
        for j in range(BLOCKS):
            ref[j, pl.ds(TOP + H, 8), :] = jnp.zeros((8, LANES), f32)


def inner_kernel(ext_in, lext_in, r_even, r_odd, ext, lext, v0, v1, v2, totals_out, seam_out):
    del ext_in, lext_in
    row, _ = place()
    row_even = (row % 2) == 0
    for k in range(K + 1):
        at = pl.ds(HALO * k, HALO)
        for j in range(BLOCKS):
            lanes = pl.ds(j * LANES, LANES)
            e, o = r_even[at, lanes], r_odd[at, lanes]
            above, below = jnp.where(row_even, o, e), jnp.where(row_even, e, o)
            for start, value in ((TOP - HALO, above), (TOP + H, below)):
                if k < K:
                    ext[k, j, pl.ds(start, HALO), :] = value
                else:
                    lext[j, pl.ds(start, HALO), :] = value.astype(jnp.int32)
    right_side(ext, lext, v0)
    clear_rows(v0, row)
    neighbours(v0, v1)
    clear_rows(v1, row)
    neighbours(v1, v2)
    clear_rows(v2, row)
    totals = products(v0, v1, v2)
    for i in range(6):
        totals_out[i] = totals[i]
    lane = iota((8, LANES), 1)
    for k in range(K + 1):
        for t in range(TILES + 2):
            at = pl.ds(TOP - 8 + 8 * t, 8)
            a, b = [
                ext[k, j, at, :] if k < K else lext[j, at, :].astype(f32) for j in (0, BLOCKS - 1)
            ]
            seam_out[k, at, :] = jnp.where(lane < 64, turn(a, LEFT), turn(b, RIGHT + SEAM))


def inner(ext, lext, r_even, r_odd):
    field = near((BLOCKS, ROWS, LANES))
    return pl.pallas_call(
        inner_kernel,
        out_shape=(
            near((K, BLOCKS, ROWS, LANES)),
            near((BLOCKS, ROWS, LANES), jnp.int32),
            field,
            field,
            field,
            near((6, 8, LANES)),
            near((K + 1, ROWS, LANES)),
        ),
        in_specs=[WHOLE] * 4,
        out_specs=(WHOLE,) * 7,
        input_output_aliases={0: 0, 1: 1},
        compiler_params=LIMIT,
        cost_estimate=cost(3),
        name="inner_fields",
    )(*held(ext, lext, r_even, r_odd))[2:]


def seam_kernel(base, totals_in, c_even, c_odd, w, sums_out, planes):
    row, col = place()
    col_even = (col % 2) == 0
    lane = iota((8, LANES), 1)
    from_left, from_right = lane < LEFT, window(lane, RIGHT + SEAM, HALO)
    outside = (from_left & (col == 0)) | (from_right & (col == 7))
    for t in range(TILES + 2):
        at = pl.ds(TOP - 8 + 8 * t, 8)
        corner = t in (0, TILES + 1)
        tile, g = (2, 0) if corner else divmod(t - 1, 8)
        e, o = c_even[pl.ds(8 * tile, 8), :], c_odd[pl.ds(8 * tile, 8), :]
        a, b = jnp.where(col_even, o, e), jnp.where(col_even, e, o)
        if corner:
            a, b = pltpu.roll(a, HALO, 0), pltpu.roll(b, HALO, 0)
        for k in range(K + 1):
            lanes = 16 * g + HALO * k
            planes[k, at, :] = jnp.where(
                from_left,
                turn(a, -lanes),
                jnp.where(from_right, turn(b, RIGHT + SEAM - lanes), base[k, at, :]),
            )

    def put(i, t, value):
        hidden = outside
        if t == 0:
            hidden = hidden | (row == 0)
        if t == TILES + 1:
            hidden = hidden | (row == 31)
        w[i, pl.ds(TOP - 8 + 8 * t, 8), :] = jnp.where(hidden, 0.0, value)

    for t in range(TILES + 2):
        start = TOP - 8 + 8 * t
        total = jnp.zeros((8, LANES), f32)
        picked = planes[K, pl.ds(start, 8), :]
        for k in range(K):
            x = planes[k, pl.ds(start, 8), :]
            vertical = planes[k, pl.ds(start + 1, 8), :] + planes[k, pl.ds(start - 1, 8), :]
            term = 4.0 * x - (vertical + turn(x, -1) + turn(x, 1))
            total = jnp.where(picked == k, term, total)
        put(0, t, total)
    for i in range(2):
        for t in range(TILES + 2):
            start = TOP - 8 + 8 * t
            x = w[i, pl.ds(start, 8), :]
            vertical = w[i, pl.ds(start + 1, 8), :] + w[i, pl.ds(start - 1, 8), :]
            put(i + 1, t, vertical + turn(x, -1) + turn(x, 1))
    own_lane = window(lane, LEFT, HALO) | window(lane, RIGHT + SEAM - HALO, HALO)
    found = [[] for _ in PAIRS]
    for t in range(TILES):
        start = TOP + 8 * t
        x = [w[i, pl.ds(start, 8), :] for i in range(3)]
        x.append(w[2, pl.ds(start + 1, 8), :] + turn(x[2], -1))
        for i, (a, b) in enumerate(PAIRS):
            found[i].append(x[a] * x[b])
    totals = [totals_in[i] + jnp.where(own_lane, tree(found[i]), 0.0) for i in range(6)]

    line = jnp.zeros((8, LANES), f32)
    for i in range(6):
        x = totals[i] + totals[i] if i == 5 else totals[i]
        big = 512.0 * jnp.max(jnp.abs(x), axis=1, keepdims=True)
        high = (x + big) - big
        line = jnp.where(
            (lane == i) | (lane == i + 16),
            jnp.sum(high, axis=1, keepdims=True),
            jnp.where(lane == i + 8, jnp.sum(x - high, axis=1, keepdims=True), line),
        )
    s, e = line, jnp.zeros_like(line)
    for shift in (4, 2, 1):
        s, more = two_sum(s, pltpu.roll(s, shift, 0))
        e = e + pltpu.roll(e, shift, 0) + more
    sums_out[...] = jnp.broadcast_to(jnp.where(lane < 16, s, e)[:1], (256, LANES))


def seam(base, totals, c_even, c_odd):
    return pl.pallas_call(
        seam_kernel,
        out_shape=(near((3, ROWS, LANES)), near((256, LANES))),
        in_specs=[WHOLE] * 4,
        out_specs=(WHOLE,) * 2,
        scratch_shapes=[pltpu.VMEM((K + 1, ROWS, LANES), f32)],
        compiler_params=LIMIT,
        cost_estimate=cost(1),
        name="seam_fields",
    )(*held(base, totals, c_even, c_odd))


def pool_kernel(v0_in, v1_in, v2_in, w, v0, v1, v2, out):
    del v0_in, v1_in, v2_in
    lane = iota((H, LANES), 1)
    rows = pl.ds(TOP, H)
    spread = jnp.where(iota((512, LANES), 0) // 4 == iota((512, LANES), 1), f32(0.0625), f32(0.0))
    for i, ref in enumerate((v0, v1, v2)):
        edge = w[i, rows, :]
        ref[0, rows, :] = jnp.where(lane < HALO, turn(edge, -LEFT), ref[0, rows, :])
        to = LANES - RIGHT - SEAM
        ref[BLOCKS - 1, rows, :] = jnp.where(
            lane >= LANES - HALO, turn(edge, to), ref[BLOCKS - 1, rows, :]
        )
        for g in range(2):
            parts = []
            for j in range(4):
                at = [ref[4 * g + j, pl.ds(TOP + q, H // 4, stride=4), :] for q in range(4)]
                parts.append((at[0] + at[1]) + (at[2] + at[3]))
            out[i, g] = jnp.dot(
                jnp.concatenate(parts, 1), spread, precision=lax.Precision.HIGHEST, preferred_element_type=f32
            )


def pool(v0, v1, v2, w):
    field = near((BLOCKS, ROWS, LANES))
    return pl.pallas_call(
        pool_kernel,
        out_shape=(field, field, field, near((3, 2, H // 4, LANES))),
        in_specs=[WHOLE] * 4,
        out_specs=(WHOLE,) * 4,
        input_output_aliases={0: 0, 1: 1, 2: 2},
        compiler_params=LIMIT,
        cost_estimate=cost(2),
        name="pool_fields",
    )(*held(v0, v1, v2, w))


def two_product(a, b):
    p = a * b
    big = f32(4097.0)
    t = big * a
    ah = t - (t - a)
    al = a - ah
    t = big * b
    bh = t - (t - b)
    bl = b - bh
    return p, ((ah * bh - p) + ah * bl + al * bh) + al * bl


def less_scaled(a, b, scale):
    p, low = two_product(b[0], scale)
    low = low + b[1] * scale
    s, e = two_sum(a[0], -p)
    e = e + (a[1] - low)
    return two_sum(s, e)


def coefficients(n):
    shift = n[1][0] / n[0][0]
    current = n
    m = [n[0][0]]
    for _ in range(5):
        current = [less_scaled(current[i + 1], current[i], shift) for i in range(len(current) - 1)]
        m.append(current[0][0] + current[0][1])
    m0, m1, m2, m3, m4, m5 = m
    t = m1 / m0
    theta0 = shift + t
    m5 = m5 - 5.0 * t * m4
    m4 = m4 - 4.0 * t * m3
    m3 = m3 - 3.0 * t * m2
    m2 = m2 - t * m1
    one = jnp.ones_like(m0)
    zero = jnp.zeros_like(m0)
    second = m2 > 0.0
    safe2 = jnp.where(second, m2, one)
    b1 = jnp.where(second, m2 / m0, zero)
    s = jnp.where(second, m3 / safe2, zero)
    h2 = m4 - s * m3 - b1 * m2
    third = second & (h2 > 0.0)
    safe3 = jnp.where(third, h2, one)
    theta1 = theta0 + s
    theta2 = theta0 - s + (m5 - s * m4 - b1 * m3) / safe3
    b2 = h2 / safe2
    d0, d1, d2 = 4.0 - theta0, 4.0 - theta1, 4.0 - theta2
    e = d1 * d2 - b2
    y2 = jnp.where(third, one / (d0 * e - b1 * d2), zero)
    y1 = jnp.where(third, d2 * y2, jnp.where(second, one / (d0 * d1 - b1), zero))
    y0 = jnp.where(third, e * y2, jnp.where(second, d1 * y1, one / d0))
    return (
        y0 - theta0 * y1 + (theta0 * theta1 - b1) * y2,
        y1 - (theta0 + theta1) * y2,
        y2,
    )


def solve_kernel(all_sums, pooled, coef_out, mid_out):
    tiles = [(all_sums[pl.ds(8 * i, 8), :], jnp.zeros((8, LANES), f32)) for i in range(32)]
    while len(tiles) > 1:
        merged = []
        for a, b in zip(tiles[0::2], tiles[1::2]):
            s, e = two_sum(a[0], b[0])
            merged.append((s, e + (a[1] + b[1])))
        tiles = merged
    s, e = tiles[0]
    for shift in (4, 2, 1):
        s, more = two_sum(s, pltpu.roll(s, shift, 0))
        e = e + pltpu.roll(e, shift, 0) + more
    lane = iota((8, LANES), 1)
    zero = jnp.zeros((8, LANES), f32)

    def over_lanes(x):
        return jnp.broadcast_to(jnp.sum(x, axis=1, keepdims=True), (8, LANES))

    n = []
    for i in range(6):
        high = over_lanes(jnp.where(lane == i, s, zero))
        low = over_lanes(jnp.where((lane == i + 8) | (lane == i + 16), s, jnp.where(lane == i, e, zero)))
        n.append(two_sum(high, low))
    c = coefficients(n)
    for i in range(3):
        coef_out[i] = c[i]
    for g in range(2):
        for q in range(H // 4 // 8):
            at = (g, pl.ds(8 * q, 8), slice(None))
            value = c[0] * pooled[(0, *at)] + c[1] * pooled[(1, *at)] + c[2] * pooled[(2, *at)]
            for d in range(16):
                mid_out[(d, *at)] = value


def solve(all_sums, pooled):
    return pl.pallas_call(
        solve_kernel,
        out_shape=(near((3, 8, LANES)), near((16, 2, H // 4, LANES))),
        in_specs=[WHOLE] * 2,
        out_specs=(WHOLE,) * 2,
        compiler_params=LIMIT,
        cost_estimate=cost(1),
        name="coefficients",
    )(*held(all_sums, pooled))


def half_matrix(rows):
    return jnp.where(iota((rows, rows // 2), 0) // 2 == iota((rows, rows // 2), 1), f32(0.25), f32(0.0))


def blend_kernel(coef, v0, v1, v2, blended_out, fine_out, scratch):
    c = [coef[i] for i in range(3)]

    def step(t, carry):
        for u in range(4):
            base = pl.multiple_of(32 * t + 8 * u, 8)
            for j in range(BLOCKS):
                at = (j, pl.ds(base + TOP, 8), slice(None))
                value = c[0] * v0[at] + c[1] * v1[at] + c[2] * v2[at]
                blended_out[pl.ds(base, 8), pl.ds(j * LANES, LANES)] = value
                scratch[j, pl.ds(base, 8), :] = value
        return carry

    lax.fori_loop(0, H // 32, step, 0)
    half = half_matrix(2 * LANES)
    for g in range(BLOCKS // 2):
        parts = [
            scratch[2 * g + i, pl.ds(0, H // 2, stride=2), :] + scratch[2 * g + i, pl.ds(1, H // 2, stride=2), :]
            for i in range(2)
        ]
        fine_out[:, pl.ds(g * LANES, LANES)] = jnp.dot(
            jnp.concatenate(parts, 1), half, precision=lax.Precision.HIGHEST, preferred_element_type=f32
        )


def blend(coef, v0, v1, v2):
    return pl.pallas_call(
        blend_kernel,
        out_shape=(
            jax.ShapeDtypeStruct((H, W), f32),
            jax.ShapeDtypeStruct((H // 2, W // 2), f32),
        ),
        in_specs=[WHOLE] * 4,
        out_specs=(WHOLE,) * 2,
        scratch_shapes=[pltpu.VMEM((BLOCKS, H, LANES), f32)],
        compiler_params=LIMIT,
        cost_estimate=cost(3),
        name="blend",
    )(*held(coef, v0, v1, v2))


def assemble_kernel(own, other, mid_out, coarse_out, scratch, sem):
    core = lax.axis_index("row_2")
    half = half_matrix(2 * LANES)
    copies = []
    for i, (x, c) in enumerate(((own, core), (other, 1 - core))):
        for g in range(2):
            copy = pltpu.make_async_copy(
                x.at[:, g], mid_out.at[:, c, :, pl.ds(g * LANES, LANES)], sem.at[i, g]
            )
            copy.start()
            copies.append(copy)
    rows = H // 8
    for x, c in ((own, core), (other, 1 - core)):
        parts = [
            jnp.concatenate(
                [x[d, g, pl.ds(0, rows, stride=2), :] + x[d, g, pl.ds(1, rows, stride=2), :] for d in range(16)], 0
            )
            for g in range(2)
        ]
        pooled = jnp.dot(
            jnp.concatenate(parts, 1), half, precision=lax.Precision.HIGHEST, preferred_element_type=f32
        )
        for d in range(16):
            scratch[d, c] = pooled[d * rows : (d + 1) * rows]
    copy = pltpu.make_async_copy(scratch, coarse_out, sem.at[2, 0])
    copy.start()
    copies.append(copy)
    for copy in copies:
        copy.wait()


def assemble(own, other):
    mid, coarse = pl.pallas_call(
        assemble_kernel,
        out_shape=(
            jax.ShapeDtypeStruct((16, 2, H // 4, W // 4), f32),
            jax.ShapeDtypeStruct((16, 2, H // 8, W // 8), f32),
        ),
        in_specs=[WHOLE] * 2,
        out_specs=(FAR,) * 2,
        scratch_shapes=[
            pltpu.VMEM((16, 2, H // 8, LANES), f32),
            pltpu.SemaphoreType.DMA((3, 2)),
        ],
        compiler_params=LIMIT,
        cost_estimate=cost(2),
        name="assemble",
    )(*held(own, other))
    return mid.reshape(8 * H, W // 4), coarse.reshape(4 * H, W // 8)


def swaps(devices, first):
    pairs = [(i, i + 1) for i in range(first, devices - 1, 2)]
    return pairs + [(b, a) for a, b in pairs]


def exchange(even, odd, axis):
    devices = lax.axis_size(axis)
    return lax.ppermute(even, axis, swaps(devices, 0)), lax.ppermute(odd, axis, swaps(devices, 1))


def per_device(sources, labels):
    r_even, r_odd = exchange(*pack_rows(sources, labels), ROW)
    ext, lext, left, right = load(sources, labels)
    c_even, c_odd = exchange(*pack_columns(r_even, r_odd, left, right), "col")
    v0, v1, v2, totals, base = inner(ext, lext, r_even, r_odd)
    w, sums = seam(base, totals, c_even, c_odd)
    v0, v1, v2, pooled = pool(v0, v1, v2, w)
    sums = lax.all_to_all(sums.reshape(256, 1, LANES), ALL, split_axis=0, concat_axis=0, tiled=True)
    coef, mid = solve(sums.reshape(256, LANES), pooled)
    mid = lax.all_to_all(mid, CHIP, split_axis=0, concat_axis=0, tiled=True)
    other = lax.ppermute(mid, "row_2", [(0, 1), (1, 0)])
    blended, fine = blend(coef, v0, v1, v2)
    overview_mid, overview_coarse = assemble(mid, other)
    return (blended, fine, overview_mid, overview_coarse)


def solution(mesh):
    finer = Mesh(
        mesh.devices.reshape(4, 4, 2, mesh.shape["col"]), ("row_0", "row_1", "row_2", "col")
    )
    return jax.shard_map(
        per_device,
        mesh=finer,
        in_specs=(P(None, ROW, "col"), P(ROW, "col")),
        out_specs=(P(ROW, "col"), P(ROW, "col"), P(None, "col"), P(None, "col")),
        check_vma=False,
    )
```

```python
import jax
import jax.numpy as jnp
from jax import lax
from jax.experimental import pallas as pl
from jax.experimental.pallas import tpu as pltpu
from jax.sharding import Mesh
from jax.sharding import PartitionSpec as P

K = 3
H, W = 128, 1024
TOP = 16
ROWS = TOP + H + 24
LANES = 128
BLOCKS = W // LANES
HALO = 4
ROW = ("row_0", "row_1", "row_2")
CHIP = ("row_0", "row_1")
ALL = ("row_0", "row_1", "row_2", "col")
VMEM = pltpu.MemorySpace.VMEM
WHOLE = pl.BlockSpec(memory_space=VMEM)
FAR = pl.BlockSpec(memory_space=pltpu.MemorySpace.HBM)
LIMIT = pltpu.CompilerParams(vmem_limit_bytes=24 * 2**20)
CHUNK, NEAR, MANY = 7, 9, 4
TILES = H // 8
LEFT, RIGHT = HALO, 64
SEAM = 12
f32 = jnp.float32


def iota(shape, dim):
    return lax.broadcasted_iota(jnp.int32, shape, dim)


def place():
    row = (lax.axis_index("row_0") * 4 + lax.axis_index("row_1")) * 2 + lax.axis_index("row_2")
    return row, lax.axis_index("col")


def near(shape, dtype=f32):
    return pltpu.VMEM(shape, dtype)


def held(*values):
    return [pltpu.with_memory_space_constraint(v, VMEM) for v in values]


def far(*values):
    return [pltpu.with_memory_space_constraint(v, pltpu.MemorySpace.HBM) for v in values]


def cost(us):
    return pl.CostEstimate(flops=int(us * 3e8), bytes_accessed=0, transcendentals=0)


def pack_kernel(src, lab, even_out, odd_out, rows, lrows, sem):
    copies = []
    for side, start in ((0, 0), (1, H - 8)):
        for i, (a, b) in enumerate(
            (
                (src.at[:, pl.ds(start, 8), :], rows.at[side]),
                (lab.at[pl.ds(start, 8), :], lrows.at[side]),
            )
        ):
            c = pltpu.make_async_copy(a, b, sem.at[side, i])
            c.start()
            copies.append(c)
    for c in copies:
        c.wait()
    row, _ = place()
    even = (row % 2) == 0
    upper = iota((8, W), 0) < HALO

    def sides(side):
        a = [rows[side, k] for k in range(K)] + [lrows[side].astype(f32)]
        pairs = []
        for x, y in ((a[0], a[1]), (a[2], a[3])):
            if side == 0:
                pairs.append(jnp.where(upper, x, pltpu.roll(y, HALO, 0)))
            else:
                pairs.append(jnp.where(upper, pltpu.roll(x, HALO, 0), y))
        return pairs

    top, bottom = sides(0), sides(1)
    for i in range(2):
        even_out[pl.ds(8 * i, 8), :] = jnp.where(even, bottom[i], top[i])
        odd_out[pl.ds(8 * i, 8), :] = jnp.where(even, top[i], bottom[i])


def pack_rows(sources, labels):
    return pl.pallas_call(
        pack_kernel,
        out_shape=(near((16, W)), near((16, W))),
        in_specs=[FAR] * 2,
        out_specs=(WHOLE,) * 2,
        scratch_shapes=[
            pltpu.VMEM((2, K, 8, W), f32),
            pltpu.VMEM((2, 8, W), jnp.int32),
            pltpu.SemaphoreType.DMA((2, 2)),
        ],
        compiler_params=LIMIT,
        cost_estimate=cost(1),
        name="pack_rows",
    )(*far(sources, labels))


def window(lane, start, size):
    return (lane >= start) & (lane < start + size)


def turn(x, shift):
    shift %= LANES
    return pltpu.roll(x, shift, 1) if shift else x


def load_kernel(src, lab, ext, lext, left_out, right_out, v0, sem):
    copies = {}
    for j in (0, BLOCKS - 1, *range(1, BLOCKS - 1)):
        lanes = pl.ds(j * LANES, LANES)
        for k in range(K + 1):
            a = src.at[k, :, lanes] if k < K else lab.at[:, lanes]
            b = ext.at[k, j, pl.ds(TOP, H), :] if k < K else lext.at[j, pl.ds(TOP, H), :]
            c = pltpu.make_async_copy(a, b, sem.at[k, j])
            c.start()
            copies[k, j] = c
    lane = iota((8, LANES), 1)
    for j, out, first in ((0, left_out, 0), (BLOCKS - 1, right_out, LANES - HALO)):
        for k in range(K + 1):
            copies.pop((k, j)).wait()
        for half in range(2):
            total = jnp.zeros((8, LANES), f32)
            for g in range(8):
                at = pl.ds(TOP + 64 * half + 8 * g, 8)
                for k in range(K + 1):
                    x = ext[k, j, at, :] if k < K else lext[j, at, :].astype(f32)
                    to = 16 * g + HALO * k
                    total = jnp.where(window(lane, to, HALO), turn(x, to - first), total)
            out[pl.ds(8 * half, 8), :] = total
    for c in copies.values():
        c.wait()

    def step(t, carry):
        for u in range(CHUNK):
            right_side(ext, lext, v0, pl.multiple_of(TOP + 8 + 8 * (CHUNK * t + u), 8))
        return carry

    lax.fori_loop(0, (TILES - 2) // CHUNK, step, 0)


def load(sources, labels):
    return pl.pallas_call(
        load_kernel,
        out_shape=(
            near((K, BLOCKS, ROWS, LANES)),
            near((BLOCKS, ROWS, LANES), jnp.int32),
            near((16, LANES)),
            near((16, LANES)),
            near((BLOCKS, ROWS, LANES)),
        ),
        in_specs=[FAR] * 2,
        out_specs=(WHOLE,) * 5,
        scratch_shapes=[pltpu.SemaphoreType.DMA((K + 1, BLOCKS))],
        compiler_params=LIMIT,
        cost_estimate=cost(2),
        name="load_block",
    )(*far(sources, labels))


def corner_kernel(got_even, got_odd, left, right, even_out, odd_out):
    row, col = place()
    row_even = (row % 2) == 0
    col_even = (col % 2) == 0
    upper = iota((8, LANES), 0) < HALO
    lane = iota((8, LANES), 1)
    strips = []
    for start, first in ((0, 0), (W - LANES, LANES - HALO)):
        total = jnp.zeros((8, LANES), f32)
        for k in range(K + 1):
            tile, half = divmod(k, 2)
            at = (pl.ds(8 * tile, 8), pl.ds(start, LANES))
            e, o = got_even[at], got_odd[at]
            above = jnp.where(row_even, o, e)
            below = jnp.where(row_even, e, o)
            if half:
                both = jnp.where(upper, pltpu.roll(above, HALO, 0), below)
            else:
                both = jnp.where(upper, above, pltpu.roll(below, HALO, 0))
            total = jnp.where(window(lane, HALO * k, HALO), turn(both, HALO * k - first), total)
        strips.append(total)
    even_out[pl.ds(0, 16), :] = jnp.where(col_even, right[...], left[...])
    odd_out[pl.ds(0, 16), :] = jnp.where(col_even, left[...], right[...])
    even_out[pl.ds(16, 8), :] = jnp.where(col_even, strips[1], strips[0])
    odd_out[pl.ds(16, 8), :] = jnp.where(col_even, strips[0], strips[1])


def pack_columns(got_even, got_odd, left, right):
    return pl.pallas_call(
        corner_kernel,
        out_shape=(near((24, LANES)),) * 2,
        in_specs=[WHOLE] * 4,
        out_specs=(WHOLE,) * 2,
        compiler_params=LIMIT,
        cost_estimate=cost(0.5),
        name="pack_columns",
    )(*held(got_even, got_odd, left, right))


def two_sum(a, b):
    s = a + b
    t = s - a
    return s, (a - (s - t)) + (b - t)


def shifted(tiles):
    lane = iota((8, LANES), 1)
    to_left = [pltpu.roll(t, LANES - 1, 1) for t in tiles]
    to_right = [pltpu.roll(t, 1, 1) for t in tiles]
    last, first = lane == LANES - 1, lane == 0
    n = len(tiles)
    after = [jnp.where(last, to_left[min(j + 1, n - 1)], to_left[j]) for j in range(n)]
    before = [jnp.where(first, to_right[max(j - 1, 0)], to_right[j]) for j in range(n)]
    return after, before


PAIRS = ((0, 0), (0, 1), (1, 1), (1, 2), (2, 2), (2, 3))


def right_side(ext, lext, out, base):
    at = pl.ds(base, 8)
    picked = [lext[j, at, :] for j in range(BLOCKS)]
    center, around = [None] * BLOCKS, [None] * BLOCKS
    for k in range(K):
        tiles = [ext[k, j, at, :] for j in range(BLOCKS)]
        after, before = shifted(tiles)
        for j in range(BLOCKS):
            near_sum = ext[k, j, pl.ds(base + 1, 8), :] + ext[k, j, pl.ds(base - 1, 8), :]
            near_sum = near_sum + after[j] + before[j]
            here = picked[j] == k
            center[j] = jnp.where(here, tiles[j], center[j]) if k else tiles[j]
            around[j] = jnp.where(here, near_sum, around[j]) if k else near_sum
    for j in range(BLOCKS):
        out[j, at, :] = 4.0 * center[j] - around[j]


def neighbours(source, target):
    def step(t, carry):
        for u in range(NEAR):
            base = pl.multiple_of(TOP - 8 + 8 * (NEAR * t + u), 8)
            tiles = [source[j, pl.ds(base, 8), :] for j in range(BLOCKS)]
            after, before = shifted(tiles)
            for j in range(BLOCKS):
                vertical = source[j, pl.ds(base + 1, 8), :] + source[j, pl.ds(base - 1, 8), :]
                target[j, pl.ds(base, 8), :] = vertical + after[j] + before[j]
        return carry

    lax.fori_loop(0, (TILES + 2) // NEAR, step, 0)


def tree(x):
    while len(x) > 1:
        x = [sum(x[a : a + 2][1:], x[a]) for a in range(0, len(x), 2)]
    return x[0]


def products(v0, v1, v2):
    lane = iota((8, LANES), 1)
    last = lane == LANES - 1
    kept = {0: lane >= HALO, BLOCKS - 1: lane < LANES - HALO}

    def step(t, totals):
        for u in range(MANY):
            base = pl.multiple_of(TOP + 8 * (MANY * t + u), 8)
            at = pl.ds(base, 8)
            found = [[] for _ in PAIRS]
            rolled = [turn(v2[j, at, :], -1) for j in range(BLOCKS)]
            for j in range(BLOCKS):
                x = [v[j, at, :] for v in (v0, v1, v2)]
                right = jnp.where(last, rolled[min(j + 1, BLOCKS - 1)], rolled[j])
                x.append(v2[j, pl.ds(base + 1, 8), :] + right)
                own = [jnp.where(kept[j], a, 0.0) for a in x[:3]] if j in kept else x
                for i, (a, b) in enumerate(PAIRS):
                    found[i].append(own[a] * x[b])
            totals = tuple(total + tree(f) for total, f in zip(totals, found))
        return totals

    return lax.fori_loop(0, TILES // MANY, step, (jnp.zeros((8, LANES), f32),) * 6)


def clear_rows(ref, row):
    @pl.when(row == 0)
    def _():
        for j in range(BLOCKS):
            ref[j, pl.ds(TOP - 8, 8), :] = jnp.zeros((8, LANES), f32)

    @pl.when(row == 31)
    def _():
        for j in range(BLOCKS):
            ref[j, pl.ds(TOP + H, 8), :] = jnp.zeros((8, LANES), f32)


def inner_kernel(
    ext_in, lext_in, v0_in, r_even, r_odd, ext, lext, v0, v1, v2, totals_out, seam_out
):
    del ext_in, lext_in, v0_in
    row, _ = place()
    row_even = (row % 2) == 0
    for k in range(K + 1):
        at = pl.ds(HALO * k, HALO)
        for j in range(BLOCKS):
            lanes = pl.ds(j * LANES, LANES)
            e, o = r_even[at, lanes], r_odd[at, lanes]
            above, below = jnp.where(row_even, o, e), jnp.where(row_even, e, o)
            for start, value in ((TOP - HALO, above), (TOP + H, below)):
                if k < K:
                    ext[k, j, pl.ds(start, HALO), :] = value
                else:
                    lext[j, pl.ds(start, HALO), :] = value.astype(jnp.int32)
    for t in (-1, 0, TILES - 1, TILES):
        right_side(ext, lext, v0, TOP + 8 * t)
    clear_rows(v0, row)
    neighbours(v0, v1)
    clear_rows(v1, row)
    neighbours(v1, v2)
    clear_rows(v2, row)
    totals = products(v0, v1, v2)
    for i in range(6):
        totals_out[i] = totals[i]
    lane = iota((8, LANES), 1)
    for k in range(K + 1):
        for t in range(TILES + 2):
            at = pl.ds(TOP - 8 + 8 * t, 8)
            a, b = [
                ext[k, j, at, :] if k < K else lext[j, at, :].astype(f32) for j in (0, BLOCKS - 1)
            ]
            seam_out[k, at, :] = jnp.where(lane < 64, turn(a, LEFT), turn(b, RIGHT + SEAM))


def inner(ext, lext, v0, r_even, r_odd):
    field = near((BLOCKS, ROWS, LANES))
    return pl.pallas_call(
        inner_kernel,
        out_shape=(
            near((K, BLOCKS, ROWS, LANES)),
            near((BLOCKS, ROWS, LANES), jnp.int32),
            field,
            field,
            field,
            near((6, 8, LANES)),
            near((K + 1, ROWS, LANES)),
        ),
        in_specs=[WHOLE] * 5,
        out_specs=(WHOLE,) * 7,
        input_output_aliases={0: 0, 1: 1, 2: 2},
        compiler_params=LIMIT,
        cost_estimate=cost(3),
        name="inner_fields",
    )(*held(ext, lext, v0, r_even, r_odd))[2:]


def seam_kernel(base, totals_in, c_even, c_odd, w, sums_out, planes):
    row, col = place()
    col_even = (col % 2) == 0
    lane = iota((8, LANES), 1)
    from_left, from_right = lane < LEFT, window(lane, RIGHT + SEAM, HALO)
    outside = (from_left & (col == 0)) | (from_right & (col == 7))
    for t in range(TILES + 2):
        at = pl.ds(TOP - 8 + 8 * t, 8)
        corner = t in (0, TILES + 1)
        tile, g = (2, 0) if corner else divmod(t - 1, 8)
        e, o = c_even[pl.ds(8 * tile, 8), :], c_odd[pl.ds(8 * tile, 8), :]
        a, b = jnp.where(col_even, o, e), jnp.where(col_even, e, o)
        if corner:
            a, b = pltpu.roll(a, HALO, 0), pltpu.roll(b, HALO, 0)
        for k in range(K + 1):
            lanes = 16 * g + HALO * k
            planes[k, at, :] = jnp.where(
                from_left,
                turn(a, -lanes),
                jnp.where(from_right, turn(b, RIGHT + SEAM - lanes), base[k, at, :]),
            )

    def put(i, t, value):
        hidden = outside
        if t == 0:
            hidden = hidden | (row == 0)
        if t == TILES + 1:
            hidden = hidden | (row == 31)
        w[i, pl.ds(TOP - 8 + 8 * t, 8), :] = jnp.where(hidden, 0.0, value)

    for t in range(TILES + 2):
        start = TOP - 8 + 8 * t
        total = jnp.zeros((8, LANES), f32)
        picked = planes[K, pl.ds(start, 8), :]
        for k in range(K):
            x = planes[k, pl.ds(start, 8), :]
            vertical = planes[k, pl.ds(start + 1, 8), :] + planes[k, pl.ds(start - 1, 8), :]
            term = 4.0 * x - (vertical + turn(x, -1) + turn(x, 1))
            total = jnp.where(picked == k, term, total)
        put(0, t, total)
    for i in range(2):
        for t in range(TILES + 2):
            start = TOP - 8 + 8 * t
            x = w[i, pl.ds(start, 8), :]
            vertical = w[i, pl.ds(start + 1, 8), :] + w[i, pl.ds(start - 1, 8), :]
            put(i + 1, t, vertical + turn(x, -1) + turn(x, 1))
    own_lane = window(lane, LEFT, HALO) | window(lane, RIGHT + SEAM - HALO, HALO)
    found = [[] for _ in PAIRS]
    for t in range(TILES):
        start = TOP + 8 * t
        x = [w[i, pl.ds(start, 8), :] for i in range(3)]
        x.append(w[2, pl.ds(start + 1, 8), :] + turn(x[2], -1))
        for i, (a, b) in enumerate(PAIRS):
            found[i].append(x[a] * x[b])
    totals = [totals_in[i] + jnp.where(own_lane, tree(found[i]), 0.0) for i in range(6)]

    line = jnp.zeros((8, LANES), f32)
    for i in range(6):
        x = totals[i] + totals[i] if i == 5 else totals[i]
        big = 512.0 * jnp.max(jnp.abs(x), axis=1, keepdims=True)
        high = (x + big) - big
        line = jnp.where(
            (lane == i) | (lane == i + 16),
            jnp.sum(high, axis=1, keepdims=True),
            jnp.where(lane == i + 8, jnp.sum(x - high, axis=1, keepdims=True), line),
        )
    s, e = line, jnp.zeros_like(line)
    for shift in (4, 2, 1):
        s, more = two_sum(s, pltpu.roll(s, shift, 0))
        e = e + pltpu.roll(e, shift, 0) + more
    line = jnp.where(lane < 16, s, e)[:1].reshape(1, 1, LANES)
    sums_out[...] = jnp.broadcast_to(line, (256, 1, LANES))


def seam(base, totals, c_even, c_odd):
    return pl.pallas_call(
        seam_kernel,
        out_shape=(near((3, ROWS, LANES)), near((256, 1, LANES))),
        in_specs=[WHOLE] * 4,
        out_specs=(WHOLE,) * 2,
        scratch_shapes=[pltpu.VMEM((K + 1, ROWS, LANES), f32)],
        compiler_params=LIMIT,
        cost_estimate=cost(1),
        name="seam_fields",
    )(*held(base, totals, c_even, c_odd))


def pool_kernel(v0_in, v1_in, v2_in, w, v0, v1, v2, out):
    del v0_in, v1_in, v2_in
    lane = iota((H, LANES), 1)
    rows = pl.ds(TOP, H)
    spread = jnp.where(iota((512, LANES), 0) // 4 == iota((512, LANES), 1), f32(0.0625), f32(0.0))
    for i, ref in enumerate((v0, v1, v2)):
        edge = w[i, rows, :]
        ref[0, rows, :] = jnp.where(lane < HALO, turn(edge, -LEFT), ref[0, rows, :])
        to = LANES - RIGHT - SEAM
        ref[BLOCKS - 1, rows, :] = jnp.where(
            lane >= LANES - HALO, turn(edge, to), ref[BLOCKS - 1, rows, :]
        )
        for g in range(2):
            parts = []
            for j in range(4):
                at = [ref[4 * g + j, pl.ds(TOP + q, H // 4, stride=4), :] for q in range(4)]
                parts.append((at[0] + at[1]) + (at[2] + at[3]))
            out[i, g] = jnp.dot(
                jnp.concatenate(parts, 1), spread, precision=lax.Precision.HIGHEST, preferred_element_type=f32
            )


def pool(v0, v1, v2, w):
    field = near((BLOCKS, ROWS, LANES))
    return pl.pallas_call(
        pool_kernel,
        out_shape=(field, field, field, near((3, 2, H // 4, LANES))),
        in_specs=[WHOLE] * 4,
        out_specs=(WHOLE,) * 4,
        input_output_aliases={0: 0, 1: 1, 2: 2},
        compiler_params=LIMIT,
        cost_estimate=cost(2),
        name="pool_fields",
    )(*held(v0, v1, v2, w))


def two_product(a, b):
    p = a * b
    big = f32(4097.0)
    t = big * a
    ah = t - (t - a)
    al = a - ah
    t = big * b
    bh = t - (t - b)
    bl = b - bh
    return p, ((ah * bh - p) + ah * bl + al * bh) + al * bl


def less_scaled(a, b, scale):
    p, low = two_product(b[0], scale)
    low = low + b[1] * scale
    s, e = two_sum(a[0], -p)
    e = e + (a[1] - low)
    return two_sum(s, e)


def coefficients(n):
    shift = n[1][0] / n[0][0]
    current = n
    m = [n[0][0]]
    for _ in range(5):
        current = [less_scaled(current[i + 1], current[i], shift) for i in range(len(current) - 1)]
        m.append(current[0][0] + current[0][1])
    m0, m1, m2, m3, m4, m5 = m
    t = m1 / m0
    theta0 = shift + t
    m5 = m5 - 5.0 * t * m4
    m4 = m4 - 4.0 * t * m3
    m3 = m3 - 3.0 * t * m2
    m2 = m2 - t * m1
    one = jnp.ones_like(m0)
    zero = jnp.zeros_like(m0)
    second = m2 > 0.0
    safe2 = jnp.where(second, m2, one)
    b1 = jnp.where(second, m2 / m0, zero)
    s = jnp.where(second, m3 / safe2, zero)
    h2 = m4 - s * m3 - b1 * m2
    third = second & (h2 > 0.0)
    safe3 = jnp.where(third, h2, one)
    theta1 = theta0 + s
    theta2 = theta0 - s + (m5 - s * m4 - b1 * m3) / safe3
    b2 = h2 / safe2
    d0, d1, d2 = 4.0 - theta0, 4.0 - theta1, 4.0 - theta2
    e = d1 * d2 - b2
    y2 = jnp.where(third, one / (d0 * e - b1 * d2), zero)
    y1 = jnp.where(third, d2 * y2, jnp.where(second, one / (d0 * d1 - b1), zero))
    y0 = jnp.where(third, e * y2, jnp.where(second, d1 * y1, one / d0))
    return (
        y0 - theta0 * y1 + (theta0 * theta1 - b1) * y2,
        y1 - (theta0 + theta1) * y2,
        y2,
    )


def solve_kernel(all_sums, pooled, coef_out, mid_out):
    tiles = [(all_sums[pl.ds(8 * i, 8), :], jnp.zeros((8, LANES), f32)) for i in range(32)]
    while len(tiles) > 1:
        merged = []
        for a, b in zip(tiles[0::2], tiles[1::2]):
            s, e = two_sum(a[0], b[0])
            merged.append((s, e + (a[1] + b[1])))
        tiles = merged
    s, e = tiles[0]
    for shift in (4, 2, 1):
        s, more = two_sum(s, pltpu.roll(s, shift, 0))
        e = e + pltpu.roll(e, shift, 0) + more
    lane = iota((8, LANES), 1)
    zero = jnp.zeros((8, LANES), f32)

    def over_lanes(x):
        return jnp.broadcast_to(jnp.sum(x, axis=1, keepdims=True), (8, LANES))

    n = []
    for i in range(6):
        high = over_lanes(jnp.where(lane == i, s, zero))
        low = over_lanes(jnp.where((lane == i + 8) | (lane == i + 16), s, jnp.where(lane == i, e, zero)))
        n.append(two_sum(high, low))
    c = coefficients(n)
    for i in range(3):
        coef_out[i] = c[i]
    for g in range(2):
        for q in range(H // 4 // 8):
            at = (g, pl.ds(8 * q, 8), slice(None))
            value = c[0] * pooled[(0, *at)] + c[1] * pooled[(1, *at)] + c[2] * pooled[(2, *at)]
            for d in range(16):
                mid_out[(d, *at)] = value


def solve(all_sums, pooled):
    return pl.pallas_call(
        solve_kernel,
        out_shape=(near((3, 8, LANES)), near((16, 2, H // 4, LANES))),
        in_specs=[WHOLE] * 2,
        out_specs=(WHOLE,) * 2,
        compiler_params=LIMIT,
        cost_estimate=cost(1),
        name="coefficients",
    )(*held(all_sums, pooled))


def half_matrix(rows):
    return jnp.where(iota((rows, rows // 2), 0) // 2 == iota((rows, rows // 2), 1), f32(0.25), f32(0.0))


def pooled_rows(parts):
    return jnp.dot(
        jnp.concatenate(parts, 1),
        half_matrix(2 * LANES),
        precision=lax.Precision.HIGHEST,
        preferred_element_type=f32,
    )


def store_mid(x, core, mid_out, sem):
    copies = []
    for g in range(2):
        to = mid_out.at[:, core, :, pl.ds(g * LANES, LANES)]
        copies.append(pltpu.make_async_copy(x.at[:, g], to, sem.at[g]))
        copies[-1].start()
    return copies


def store_coarse(x, core, coarse_out, scratch, sem):
    rows = H // 8
    parts = [
        jnp.concatenate(
            [x[d, g, pl.ds(0, rows, stride=2), :] + x[d, g, pl.ds(1, rows, stride=2), :] for d in range(16)], 0
        )
        for g in range(2)
    ]
    pooled = pooled_rows(parts)
    for d in range(16):
        scratch[d] = pooled[d * rows : (d + 1) * rows]
    copy = pltpu.make_async_copy(scratch, coarse_out.at[:, core], sem)
    copy.start()
    return copy


def own_kernel(
    x, coef, v0, v1, v2, blended_out, fine_out, mid_out, coarse_out, flat, stacked, fine, coarse, sem
):
    core = lax.axis_index("row_2")
    copies = store_mid(x, core, mid_out, sem)
    c = [coef[i] for i in range(3)]
    parts = 4
    for p in range(parts):
        for u in range(TILES // parts):
            base = 8 * (p * (TILES // parts) + u)
            for j in range(BLOCKS):
                at = (j, pl.ds(base + TOP, 8), slice(None))
                value = c[0] * v0[at] + c[1] * v1[at] + c[2] * v2[at]
                flat[pl.ds(base, 8), pl.ds(j * LANES, LANES)] = value
                stacked[j, pl.ds(base, 8), :] = value
        rows = pl.ds(p * H // parts, H // parts)
        copies.append(pltpu.make_async_copy(flat.at[rows, :], blended_out.at[rows, :], sem.at[3 + p]))
        copies[-1].start()
    for g in range(BLOCKS // 2):
        halves = [
            stacked[2 * g + i, pl.ds(0, H // 2, stride=2), :] + stacked[2 * g + i, pl.ds(1, H // 2, stride=2), :]
            for i in range(2)
        ]
        fine[:, pl.ds(g * LANES, LANES)] = pooled_rows(halves)
    copies.append(pltpu.make_async_copy(fine, fine_out, sem.at[3 + parts]))
    copies[-1].start()
    copies.append(store_coarse(x, core, coarse_out, coarse, sem.at[2]))
    for copy in copies:
        copy.wait()


LEVELS = (
    jax.ShapeDtypeStruct((16, 2, H // 4, W // 4), f32),
    jax.ShapeDtypeStruct((16, 2, H // 8, W // 8), f32),
)


def own_levels(x, coef, v0, v1, v2):
    return pl.pallas_call(
        own_kernel,
        out_shape=(
            jax.ShapeDtypeStruct((H, W), f32),
            jax.ShapeDtypeStruct((H // 2, W // 2), f32),
            *LEVELS,
        ),
        in_specs=[WHOLE] * 5,
        out_specs=(FAR,) * 4,
        scratch_shapes=[
            pltpu.VMEM((H, W), f32),
            pltpu.VMEM((BLOCKS, H, LANES), f32),
            pltpu.VMEM((H // 2, W // 2), f32),
            pltpu.VMEM((16, H // 8, LANES), f32),
            pltpu.SemaphoreType.DMA((8,)),
        ],
        compiler_params=LIMIT,
        cost_estimate=cost(2),
        name="own_levels",
    )(*held(x, coef, v0, v1, v2))


def other_kernel(x, mid_in, coarse_in, mid_out, coarse_out, coarse, sem):
    del mid_in, coarse_in
    core = 1 - lax.axis_index("row_2")
    copies = store_mid(x, core, mid_out, sem)
    copies.append(store_coarse(x, core, coarse_out, coarse, sem.at[2]))
    for copy in copies:
        copy.wait()


def other_levels(x, mid, coarse):
    return pl.pallas_call(
        other_kernel,
        out_shape=LEVELS,
        in_specs=[WHOLE, FAR, FAR],
        out_specs=(FAR,) * 2,
        scratch_shapes=[
            pltpu.VMEM((16, H // 8, LANES), f32),
            pltpu.SemaphoreType.DMA((3,)),
        ],
        input_output_aliases={1: 0, 2: 1},
        compiler_params=LIMIT,
        cost_estimate=cost(1),
        name="other_levels",
    )(*held(x), *far(mid, coarse))


def swaps(devices, first):
    pairs = [(i, i + 1) for i in range(first, devices - 1, 2)]
    return pairs + [(b, a) for a, b in pairs]


def exchange(even, odd, axis):
    devices = lax.axis_size(axis)
    return lax.ppermute(even, axis, swaps(devices, 0)), lax.ppermute(odd, axis, swaps(devices, 1))


def per_device(sources, labels):
    r_even, r_odd = exchange(*pack_rows(sources, labels), ROW)
    ext, lext, left, right, v0 = load(sources, labels)
    c_even, c_odd = exchange(*pack_columns(r_even, r_odd, left, right), "col")
    v0, v1, v2, totals, base = inner(ext, lext, v0, r_even, r_odd)
    w, sums = seam(base, totals, c_even, c_odd)
    v0, v1, v2, pooled = pool(v0, v1, v2, w)
    sums = lax.all_to_all(sums, ALL, split_axis=0, concat_axis=0, tiled=True)
    coef, mid = solve(sums.reshape(256, LANES), pooled)
    mid = lax.all_to_all(mid, CHIP, split_axis=0, concat_axis=0, tiled=True)
    other = lax.ppermute(mid, "row_2", [(0, 1), (1, 0)])
    blended, fine, overview_mid, overview_coarse = own_levels(mid, coef, v0, v1, v2)
    overview_mid, overview_coarse = other_levels(other, overview_mid, overview_coarse)
    overview_mid = overview_mid.reshape(8 * H, W // 4)
    overview_coarse = overview_coarse.reshape(4 * H, W // 8)
    return (blended, fine, overview_mid, overview_coarse)


def solution(mesh):
    finer = Mesh(
        mesh.devices.reshape(4, 4, 2, mesh.shape["col"]), ("row_0", "row_1", "row_2", "col")
    )
    return jax.shard_map(
        per_device,
        mesh=finer,
        in_specs=(P(None, ROW, "col"), P(ROW, "col")),
        out_specs=(P(ROW, "col"), P(ROW, "col"), P(None, "col"), P(None, "col")),
        check_vma=False,
    )
```

```python
import jax
import jax.numpy as jnp
from jax import lax
from jax.experimental import pallas as pl
from jax.experimental.pallas import tpu as pltpu
from jax.sharding import Mesh
from jax.sharding import PartitionSpec as P


K = 3
H, W = 128, 1024
TOP = 16
ROWS = TOP + H + 24
LANES = 128
BLOCKS = W // LANES
HALO = 4
ROW = ("row_0", "row_1", "row_2")
CHIP = ("row_0", "row_1")
ALL = ("row_0", "row_1", "row_2", "col")
VMEM = pltpu.MemorySpace.VMEM
WHOLE = pl.BlockSpec(memory_space=VMEM)
FAR = pl.BlockSpec(memory_space=pltpu.MemorySpace.HBM)
LIMIT = pltpu.CompilerParams(vmem_limit_bytes=24 * 2**20)
TILES = H // 8
LEFT, RIGHT = HALO, 64
SEAM = 12
f32 = jnp.float32


def iota(shape, dim):
    return lax.broadcasted_iota(jnp.int32, shape, dim)


def place():
    row = (lax.axis_index("row_0") * 4 + lax.axis_index("row_1")) * 2 + lax.axis_index("row_2")
    return row, lax.axis_index("col")


def near(shape, dtype=f32):
    return pltpu.VMEM(shape, dtype)


def held(*values):
    return [pltpu.with_memory_space_constraint(v, VMEM) for v in values]


def far(*values):
    return [pltpu.with_memory_space_constraint(v, pltpu.MemorySpace.HBM) for v in values]


def cost(us):
    return pl.CostEstimate(flops=int(us * 3e8), bytes_accessed=0, transcendentals=0)


def pack_kernel(src, lab, even_out, odd_out, rows, lrows, sem):
    copies = []
    for side, start in ((0, 0), (1, H - 8)):
        for i, (a, b) in enumerate(
            (
                (src.at[:, pl.ds(start, 8), :], rows.at[side]),
                (lab.at[pl.ds(start, 8), :], lrows.at[side]),
            )
        ):
            c = pltpu.make_async_copy(a, b, sem.at[side, i])
            c.start()
            copies.append(c)
    for c in copies:
        c.wait()
    row, _ = place()
    even = (row % 2) == 0
    upper = iota((8, W), 0) < HALO

    def sides(side):
        a = [rows[side, k] for k in range(K)] + [lrows[side].astype(f32)]
        pairs = []
        for x, y in ((a[0], a[1]), (a[2], a[3])):
            if side == 0:
                pairs.append(jnp.where(upper, x, pltpu.roll(y, HALO, 0)))
            else:
                pairs.append(jnp.where(upper, pltpu.roll(x, HALO, 0), y))
        return pairs

    top, bottom = sides(0), sides(1)
    for i in range(2):
        even_out[pl.ds(8 * i, 8), :] = jnp.where(even, bottom[i], top[i])
        odd_out[pl.ds(8 * i, 8), :] = jnp.where(even, top[i], bottom[i])


def pack_rows(sources, labels):
    return pl.pallas_call(
        pack_kernel,
        out_shape=(near((16, W)), near((16, W))),
        in_specs=[FAR] * 2,
        out_specs=(WHOLE,) * 2,
        scratch_shapes=[
            pltpu.VMEM((2, K, 8, W), f32),
            pltpu.VMEM((2, 8, W), jnp.int32),
            pltpu.SemaphoreType.DMA((2, 2)),
        ],
        compiler_params=LIMIT,
        cost_estimate=cost(1),
        name="pack_rows",
    )(*far(sources, labels))


def window(lane, start, size):
    return (lane >= start) & (lane < start + size)


def turn(x, shift):
    shift %= LANES
    return pltpu.roll(x, shift, 1) if shift else x


def load_kernel(
    src, lab, ext, lext, left_out, right_out, v0, v1, v2, totals_out, seam_out
):
    own = pl.ds(TOP, H)
    for j in (0, BLOCKS - 1, *range(1, BLOCKS - 1)):
        lanes = pl.ds(j * LANES, LANES)
        for k in range(K):
            ext[k, j, own, :] = src[k, :, lanes]
        lext[j, own, :] = lab[:, lanes]
    lane = iota((8, LANES), 1)
    for j, out, first in ((0, left_out, 0), (BLOCKS - 1, right_out, LANES - HALO)):
        for half in range(2):
            total = jnp.zeros((8, LANES), f32)
            for g in range(8):
                at = pl.ds(TOP + 64 * half + 8 * g, 8)
                for k in range(K + 1):
                    x = ext[k, j, at, :] if k < K else lext[j, at, :].astype(f32)
                    to = 16 * g + HALO * k
                    total = jnp.where(window(lane, to, HALO), turn(x, to - first), total)
            out[pl.ds(8 * half, 8), :] = total

    over_tiles(1, TILES - 2, 7, lambda base, c: (right_side(ext, lext, v0, base), c)[1], 0)
    over_tiles(2, TILES - 3, 6, lambda base, c: (neighbours(v0, v1, base), c)[1], 0)
    over_tiles(3, TILES - 4, 5, lambda base, c: (neighbours(v1, v2, base), c)[1], 0)
    zero = jnp.zeros((8, LANES), f32)
    totals = over_tiles(3, TILES - 5, 3, lambda base, c: products(v0, v1, v2, base, c), (zero,) * 6)
    for i in range(6):
        totals_out[i] = totals[i]
    for tile in range(TILES):
        seam_base(ext, lext, seam_out, tile)


def load(sources, labels):
    field = near((BLOCKS, ROWS, LANES))
    return pl.pallas_call(
        load_kernel,
        out_shape=(
            near((K, BLOCKS, ROWS, LANES)),
            near((BLOCKS, ROWS, LANES), jnp.int32),
            near((16, LANES)),
            near((16, LANES)),
            field,
            field,
            field,
            near((6, 8, LANES)),
            near((K + 1, ROWS, LANES)),
        ),
        in_specs=[WHOLE] * 2,
        out_specs=(WHOLE,) * 9,
        compiler_params=LIMIT,
        cost_estimate=cost(3),
        name="load_block",
    )(*held(sources, labels))


def corner_kernel(got_even, got_odd, left, right, even_out, odd_out):
    row, col = place()
    row_even = (row % 2) == 0
    col_even = (col % 2) == 0
    upper = iota((8, LANES), 0) < HALO
    lane = iota((8, LANES), 1)
    strips = []
    for start, first in ((0, 0), (W - LANES, LANES - HALO)):
        total = jnp.zeros((8, LANES), f32)
        for k in range(K + 1):
            tile, half = divmod(k, 2)
            at = (pl.ds(8 * tile, 8), pl.ds(start, LANES))
            e, o = got_even[at], got_odd[at]
            above = jnp.where(row_even, o, e)
            below = jnp.where(row_even, e, o)
            if half:
                both = jnp.where(upper, pltpu.roll(above, HALO, 0), below)
            else:
                both = jnp.where(upper, above, pltpu.roll(below, HALO, 0))
            total = jnp.where(window(lane, HALO * k, HALO), turn(both, HALO * k - first), total)
        strips.append(total)
    even_out[pl.ds(0, 16), :] = jnp.where(col_even, right[...], left[...])
    odd_out[pl.ds(0, 16), :] = jnp.where(col_even, left[...], right[...])
    even_out[pl.ds(16, 8), :] = jnp.where(col_even, strips[1], strips[0])
    odd_out[pl.ds(16, 8), :] = jnp.where(col_even, strips[0], strips[1])


def pack_columns(got_even, got_odd, left, right):
    return pl.pallas_call(
        corner_kernel,
        out_shape=(near((24, LANES)),) * 2,
        in_specs=[WHOLE] * 4,
        out_specs=(WHOLE,) * 2,
        compiler_params=LIMIT,
        cost_estimate=cost(0.5),
        name="pack_columns",
    )(*held(got_even, got_odd, left, right))


def two_sum(a, b):
    s = a + b
    t = s - a
    return s, (a - (s - t)) + (b - t)


def shifted(tiles):
    lane = iota((8, LANES), 1)
    to_left = [pltpu.roll(t, LANES - 1, 1) for t in tiles]
    to_right = [pltpu.roll(t, 1, 1) for t in tiles]
    last, first = lane == LANES - 1, lane == 0
    n = len(tiles)
    after = [jnp.where(last, to_left[min(j + 1, n - 1)], to_left[j]) for j in range(n)]
    before = [jnp.where(first, to_right[max(j - 1, 0)], to_right[j]) for j in range(n)]
    return after, before


PAIRS = ((0, 0), (0, 1), (1, 1), (1, 2), (2, 2), (2, 3))


def right_side(ext, lext, out, base):
    at = pl.ds(base, 8)
    picked = [lext[j, at, :] for j in range(BLOCKS)]
    center, around = [None] * BLOCKS, [None] * BLOCKS
    for k in range(K):
        tiles = [ext[k, j, at, :] for j in range(BLOCKS)]
        after, before = shifted(tiles)
        for j in range(BLOCKS):
            near_sum = ext[k, j, pl.ds(base + 1, 8), :] + ext[k, j, pl.ds(base - 1, 8), :]
            near_sum = near_sum + after[j] + before[j]
            here = picked[j] == k
            center[j] = jnp.where(here, tiles[j], center[j]) if k else tiles[j]
            around[j] = jnp.where(here, near_sum, around[j]) if k else near_sum
    for j in range(BLOCKS):
        out[j, at, :] = 4.0 * center[j] - around[j]


def neighbours(source, target, base):
    tiles = [source[j, pl.ds(base, 8), :] for j in range(BLOCKS)]
    after, before = shifted(tiles)
    for j in range(BLOCKS):
        vertical = source[j, pl.ds(base + 1, 8), :] + source[j, pl.ds(base - 1, 8), :]
        target[j, pl.ds(base, 8), :] = vertical + after[j] + before[j]


def over_tiles(first, last, chunk, step, carry):
    def turn_of(t, carry):
        for u in range(chunk):
            carry = step(pl.multiple_of(TOP + 8 * first + 8 * (chunk * t + u), 8), carry)
        return carry

    return lax.fori_loop(0, (last - first + 1) // chunk, turn_of, carry)


def tree(x):
    while len(x) > 1:
        x = [sum(x[a : a + 2][1:], x[a]) for a in range(0, len(x), 2)]
    return x[0]


def products(v0, v1, v2, base, totals):
    lane = iota((8, LANES), 1)
    last = lane == LANES - 1
    kept = {0: lane >= HALO, BLOCKS - 1: lane < LANES - HALO}
    at = pl.ds(base, 8)
    found = [[] for _ in PAIRS]
    rolled = [turn(v2[j, at, :], -1) for j in range(BLOCKS)]
    for j in range(BLOCKS):
        x = [v[j, at, :] for v in (v0, v1, v2)]
        right = jnp.where(last, rolled[min(j + 1, BLOCKS - 1)], rolled[j])
        x.append(v2[j, pl.ds(base + 1, 8), :] + right)
        own = [jnp.where(kept[j], a, 0.0) for a in x[:3]] if j in kept else x
        for i, (a, b) in enumerate(PAIRS):
            found[i].append(own[a] * x[b])
    return tuple(total + tree(f) for total, f in zip(totals, found))


def seam_base(ext, lext, out, tile):
    lane = iota((8, LANES), 1)
    at = pl.ds(TOP + 8 * tile, 8)
    for k in range(K + 1):
        a, b = [ext[k, j, at, :] if k < K else lext[j, at, :].astype(f32) for j in (0, BLOCKS - 1)]
        out[k, at, :] = jnp.where(lane < 64, turn(a, LEFT), turn(b, RIGHT + SEAM))


def clear_rows(ref, row):
    @pl.when(row == 0)
    def _():
        for j in range(BLOCKS):
            ref[j, pl.ds(TOP - 8, 8), :] = jnp.zeros((8, LANES), f32)

    @pl.when(row == 31)
    def _():
        for j in range(BLOCKS):
            ref[j, pl.ds(TOP + H, 8), :] = jnp.zeros((8, LANES), f32)


def inner_kernel(*refs):
    r_even, r_odd, totals_in = refs[6:9]
    ext, lext, v0, v1, v2, seam_out, totals_out = refs[9:]
    row, _ = place()
    row_even = (row % 2) == 0
    for k in range(K + 1):
        at = pl.ds(HALO * k, HALO)
        for j in range(BLOCKS):
            lanes = pl.ds(j * LANES, LANES)
            e, o = r_even[at, lanes], r_odd[at, lanes]
            above, below = jnp.where(row_even, o, e), jnp.where(row_even, e, o)
            for start, value in ((TOP - HALO, above), (TOP + H, below)):
                if k < K:
                    ext[k, j, pl.ds(start, HALO), :] = value
                else:
                    lext[j, pl.ds(start, HALO), :] = value.astype(jnp.int32)
    seam_base(ext, lext, seam_out, -1)
    seam_base(ext, lext, seam_out, TILES)
    for t in (-1, 0, TILES - 1, TILES):
        right_side(ext, lext, v0, TOP + 8 * t)
    clear_rows(v0, row)
    for t in (-1, 0, 1, TILES - 2, TILES - 1, TILES):
        neighbours(v0, v1, TOP + 8 * t)
    clear_rows(v1, row)
    for t in (-1, 0, 1, 2, TILES - 3, TILES - 2, TILES - 1, TILES):
        neighbours(v1, v2, TOP + 8 * t)
    clear_rows(v2, row)
    totals = tuple(totals_in[i] for i in range(6))
    for t in (0, 1, 2, *range(TILES - 4, TILES)):
        totals = products(v0, v1, v2, TOP + 8 * t, totals)
    for i in range(6):
        totals_out[i] = totals[i]


def inner(ext, lext, v0, v1, v2, base, r_even, r_odd, totals):
    field = near((BLOCKS, ROWS, LANES))
    return pl.pallas_call(
        inner_kernel,
        out_shape=(
            near((K, BLOCKS, ROWS, LANES)),
            near((BLOCKS, ROWS, LANES), jnp.int32),
            field,
            field,
            field,
            near((K + 1, ROWS, LANES)),
            near((6, 8, LANES)),
        ),
        in_specs=[WHOLE] * 9,
        out_specs=(WHOLE,) * 7,
        input_output_aliases={i: i for i in range(6)},
        compiler_params=LIMIT,
        cost_estimate=cost(2),
        name="inner_fields",
    )(*held(ext, lext, v0, v1, v2, base, r_even, r_odd, totals))[2:]


def seam_kernel(base, totals_in, c_even, c_odd, w, sums_out, planes):
    row, col = place()
    col_even = (col % 2) == 0
    lane = iota((8, LANES), 1)
    from_left, from_right = lane < LEFT, window(lane, RIGHT + SEAM, HALO)
    outside = (from_left & (col == 0)) | (from_right & (col == 7))
    for t in range(TILES + 2):
        at = pl.ds(TOP - 8 + 8 * t, 8)
        corner = t in (0, TILES + 1)
        tile, g = (2, 0) if corner else divmod(t - 1, 8)
        e, o = c_even[pl.ds(8 * tile, 8), :], c_odd[pl.ds(8 * tile, 8), :]
        a, b = jnp.where(col_even, o, e), jnp.where(col_even, e, o)
        if corner:
            a, b = pltpu.roll(a, HALO, 0), pltpu.roll(b, HALO, 0)
        for k in range(K + 1):
            lanes = 16 * g + HALO * k
            planes[k, at, :] = jnp.where(
                from_left,
                turn(a, -lanes),
                jnp.where(from_right, turn(b, RIGHT + SEAM - lanes), base[k, at, :]),
            )

    def put(i, t, value):
        hidden = outside
        if t == 0:
            hidden = hidden | (row == 0)
        if t == TILES + 1:
            hidden = hidden | (row == 31)
        w[i, pl.ds(TOP - 8 + 8 * t, 8), :] = jnp.where(hidden, 0.0, value)

    for t in range(TILES + 2):
        start = TOP - 8 + 8 * t
        total = jnp.zeros((8, LANES), f32)
        picked = planes[K, pl.ds(start, 8), :]
        for k in range(K):
            x = planes[k, pl.ds(start, 8), :]
            vertical = planes[k, pl.ds(start + 1, 8), :] + planes[k, pl.ds(start - 1, 8), :]
            term = 4.0 * x - (vertical + turn(x, -1) + turn(x, 1))
            total = jnp.where(picked == k, term, total)
        put(0, t, total)
    for i in range(2):
        for t in range(TILES + 2):
            start = TOP - 8 + 8 * t
            x = w[i, pl.ds(start, 8), :]
            vertical = w[i, pl.ds(start + 1, 8), :] + w[i, pl.ds(start - 1, 8), :]
            put(i + 1, t, vertical + turn(x, -1) + turn(x, 1))
    own_lane = window(lane, LEFT, HALO) | window(lane, RIGHT + SEAM - HALO, HALO)
    found = [[] for _ in PAIRS]
    for t in range(TILES):
        start = TOP + 8 * t
        x = [w[i, pl.ds(start, 8), :] for i in range(3)]
        x.append(w[2, pl.ds(start + 1, 8), :] + turn(x[2], -1))
        for i, (a, b) in enumerate(PAIRS):
            found[i].append(x[a] * x[b])
    totals = [totals_in[i] + jnp.where(own_lane, tree(found[i]), 0.0) for i in range(6)]

    line = jnp.zeros((8, LANES), f32)
    for i in range(6):
        x = totals[i] + totals[i] if i == 5 else totals[i]
        big = 512.0 * jnp.max(jnp.abs(x), axis=1, keepdims=True)
        high = (x + big) - big
        line = jnp.where(
            (lane == i) | (lane == i + 16),
            jnp.sum(high, axis=1, keepdims=True),
            jnp.where(lane == i + 8, jnp.sum(x - high, axis=1, keepdims=True), line),
        )
    s, e = line, jnp.zeros_like(line)
    for shift in (4, 2, 1):
        s, more = two_sum(s, pltpu.roll(s, shift, 0))
        e = e + pltpu.roll(e, shift, 0) + more
    line = jnp.where(lane < 16, s, e)[:1].reshape(1, 1, LANES)
    sums_out[...] = jnp.broadcast_to(line, (256, 1, LANES))


def seam(base, totals, c_even, c_odd):
    return pl.pallas_call(
        seam_kernel,
        out_shape=(near((3, ROWS, LANES)), near((256, 1, LANES))),
        in_specs=[WHOLE] * 4,
        out_specs=(WHOLE,) * 2,
        scratch_shapes=[pltpu.VMEM((K + 1, ROWS, LANES), f32)],
        compiler_params=LIMIT,
        cost_estimate=cost(1),
        name="seam_fields",
    )(*held(base, totals, c_even, c_odd))


def pool_kernel(v0_in, v1_in, v2_in, w, v0, v1, v2, out):
    del v0_in, v1_in, v2_in
    lane = iota((H, LANES), 1)
    rows = pl.ds(TOP, H)
    spread = jnp.where(iota((512, LANES), 0) // 4 == iota((512, LANES), 1), f32(0.0625), f32(0.0))
    for i, ref in enumerate((v0, v1, v2)):
        edge = w[i, rows, :]
        ref[0, rows, :] = jnp.where(lane < HALO, turn(edge, -LEFT), ref[0, rows, :])
        to = LANES - RIGHT - SEAM
        ref[BLOCKS - 1, rows, :] = jnp.where(
            lane >= LANES - HALO, turn(edge, to), ref[BLOCKS - 1, rows, :]
        )
        for g in range(2):
            parts = []
            for j in range(4):
                at = [ref[4 * g + j, pl.ds(TOP + q, H // 4, stride=4), :] for q in range(4)]
                parts.append((at[0] + at[1]) + (at[2] + at[3]))
            out[i, g] = jnp.dot(
                jnp.concatenate(parts, 1), spread, precision=lax.Precision.HIGHEST, preferred_element_type=f32
            )


def pool(v0, v1, v2, w):
    field = near((BLOCKS, ROWS, LANES))
    return pl.pallas_call(
        pool_kernel,
        out_shape=(field, field, field, near((3, 2, H // 4, LANES))),
        in_specs=[WHOLE] * 4,
        out_specs=(WHOLE,) * 4,
        input_output_aliases={0: 0, 1: 1, 2: 2},
        compiler_params=LIMIT,
        cost_estimate=cost(2),
        name="pool_fields",
    )(*held(v0, v1, v2, w))


def two_product(a, b):
    p = a * b
    big = f32(4097.0)
    t = big * a
    ah = t - (t - a)
    al = a - ah
    t = big * b
    bh = t - (t - b)
    bl = b - bh
    return p, ((ah * bh - p) + ah * bl + al * bh) + al * bl


def less_scaled(a, b, scale):
    p, low = two_product(b[0], scale)
    low = low + b[1] * scale
    s, e = two_sum(a[0], -p)
    e = e + (a[1] - low)
    return two_sum(s, e)


def coefficients(n):
    shift = n[1][0] / n[0][0]
    current = n
    m = [n[0][0]]
    for _ in range(5):
        current = [less_scaled(current[i + 1], current[i], shift) for i in range(len(current) - 1)]
        m.append(current[0][0] + current[0][1])
    m0, m1, m2, m3, m4, m5 = m
    t = m1 / m0
    theta0 = shift + t
    m5 = m5 - 5.0 * t * m4
    m4 = m4 - 4.0 * t * m3
    m3 = m3 - 3.0 * t * m2
    m2 = m2 - t * m1
    one = jnp.ones_like(m0)
    zero = jnp.zeros_like(m0)
    second = m2 > 0.0
    safe2 = jnp.where(second, m2, one)
    b1 = jnp.where(second, m2 / m0, zero)
    s = jnp.where(second, m3 / safe2, zero)
    h2 = m4 - s * m3 - b1 * m2
    third = second & (h2 > 0.0)
    safe3 = jnp.where(third, h2, one)
    theta1 = theta0 + s
    theta2 = theta0 - s + (m5 - s * m4 - b1 * m3) / safe3
    b2 = h2 / safe2
    d0, d1, d2 = 4.0 - theta0, 4.0 - theta1, 4.0 - theta2
    e = d1 * d2 - b2
    y2 = jnp.where(third, one / (d0 * e - b1 * d2), zero)
    y1 = jnp.where(third, d2 * y2, jnp.where(second, one / (d0 * d1 - b1), zero))
    y0 = jnp.where(third, e * y2, jnp.where(second, d1 * y1, one / d0))
    return (
        y0 - theta0 * y1 + (theta0 * theta1 - b1) * y2,
        y1 - (theta0 + theta1) * y2,
        y2,
    )


def solve_kernel(all_sums, pooled, coef_out, mid_out):
    tiles = [(all_sums[pl.ds(8 * i, 8), :], jnp.zeros((8, LANES), f32)) for i in range(32)]
    while len(tiles) > 1:
        merged = []
        for a, b in zip(tiles[0::2], tiles[1::2]):
            s, e = two_sum(a[0], b[0])
            merged.append((s, e + (a[1] + b[1])))
        tiles = merged
    s, e = tiles[0]
    for shift in (4, 2, 1):
        s, more = two_sum(s, pltpu.roll(s, shift, 0))
        e = e + pltpu.roll(e, shift, 0) + more
    lane = iota((8, LANES), 1)
    zero = jnp.zeros((8, LANES), f32)

    def over_lanes(x):
        return jnp.broadcast_to(jnp.sum(x, axis=1, keepdims=True), (8, LANES))

    n = []
    for i in range(6):
        high = over_lanes(jnp.where(lane == i, s, zero))
        low = over_lanes(jnp.where((lane == i + 8) | (lane == i + 16), s, jnp.where(lane == i, e, zero)))
        n.append(two_sum(high, low))
    c = coefficients(n)
    for i in range(3):
        coef_out[i] = c[i]
    for g in range(2):
        for q in range(H // 4 // 8):
            at = (g, pl.ds(8 * q, 8), slice(None))
            value = c[0] * pooled[(0, *at)] + c[1] * pooled[(1, *at)] + c[2] * pooled[(2, *at)]
            for d in range(16):
                mid_out[(d, *at)] = value


def solve(all_sums, pooled):
    return pl.pallas_call(
        solve_kernel,
        out_shape=(near((3, 8, LANES)), near((16, 2, H // 4, LANES))),
        in_specs=[WHOLE] * 2,
        out_specs=(WHOLE,) * 2,
        compiler_params=LIMIT,
        cost_estimate=cost(1),
        name="coefficients",
    )(*held(all_sums, pooled))


def half_matrix(rows):
    return jnp.where(iota((rows, rows // 2), 0) // 2 == iota((rows, rows // 2), 1), f32(0.25), f32(0.0))


def pooled_rows(parts):
    return jnp.dot(
        jnp.concatenate(parts, 1),
        half_matrix(2 * LANES),
        precision=lax.Precision.HIGHEST,
        preferred_element_type=f32,
    )


def store_mid(x, core, mid_out, sem):
    copies = []
    for g in range(2):
        to = mid_out.at[:, core, :, pl.ds(g * LANES, LANES)]
        copies.append(pltpu.make_async_copy(x.at[:, g], to, sem.at[g]))
        copies[-1].start()
    return copies


def store_coarse(x, core, coarse_out, scratch, sem):
    rows = H // 8
    parts = [
        jnp.concatenate(
            [x[d, g, pl.ds(0, rows, stride=2), :] + x[d, g, pl.ds(1, rows, stride=2), :] for d in range(16)], 0
        )
        for g in range(2)
    ]
    pooled = pooled_rows(parts)
    for d in range(16):
        scratch[d] = pooled[d * rows : (d + 1) * rows]
    copy = pltpu.make_async_copy(scratch, coarse_out.at[:, core], sem)
    copy.start()
    return copy


def own_kernel(
    x, coef, v0, v1, v2, blended_out, fine_out, mid_out, coarse_out, flat, stacked, fine, coarse, sem
):
    core = lax.axis_index("row_2")
    copies = store_mid(x, core, mid_out, sem)
    c = [coef[i] for i in range(3)]
    parts = 4
    for p in range(parts):
        for u in range(TILES // parts):
            base = 8 * (p * (TILES // parts) + u)
            for j in range(BLOCKS):
                at = (j, pl.ds(base + TOP, 8), slice(None))
                value = c[0] * v0[at] + c[1] * v1[at] + c[2] * v2[at]
                flat[pl.ds(base, 8), pl.ds(j * LANES, LANES)] = value
                stacked[j, pl.ds(base, 8), :] = value
        rows = pl.ds(p * H // parts, H // parts)
        copies.append(pltpu.make_async_copy(flat.at[rows, :], blended_out.at[rows, :], sem.at[3 + p]))
        copies[-1].start()
    for g in range(BLOCKS // 2):
        halves = [
            stacked[2 * g + i, pl.ds(0, H // 2, stride=2), :] + stacked[2 * g + i, pl.ds(1, H // 2, stride=2), :]
            for i in range(2)
        ]
        fine[:, pl.ds(g * LANES, LANES)] = pooled_rows(halves)
    copies.append(pltpu.make_async_copy(fine, fine_out, sem.at[3 + parts]))
    copies[-1].start()
    copies.append(store_coarse(x, core, coarse_out, coarse, sem.at[2]))
    for copy in copies:
        copy.wait()


LEVELS = (
    jax.ShapeDtypeStruct((16, 2, H // 4, W // 4), f32),
    jax.ShapeDtypeStruct((16, 2, H // 8, W // 8), f32),
)


def own_levels(x, coef, v0, v1, v2):
    return pl.pallas_call(
        own_kernel,
        out_shape=(
            jax.ShapeDtypeStruct((H, W), f32),
            jax.ShapeDtypeStruct((H // 2, W // 2), f32),
            *LEVELS,
        ),
        in_specs=[WHOLE] * 5,
        out_specs=(FAR,) * 4,
        scratch_shapes=[
            pltpu.VMEM((H, W), f32),
            pltpu.VMEM((BLOCKS, H, LANES), f32),
            pltpu.VMEM((H // 2, W // 2), f32),
            pltpu.VMEM((16, H // 8, LANES), f32),
            pltpu.SemaphoreType.DMA((8,)),
        ],
        compiler_params=LIMIT,
        cost_estimate=cost(2),
        name="own_levels",
    )(*held(x, coef, v0, v1, v2))


def other_kernel(x, mid_in, coarse_in, mid_out, coarse_out, coarse, sem):
    del mid_in, coarse_in
    core = 1 - lax.axis_index("row_2")
    copies = store_mid(x, core, mid_out, sem)
    copies.append(store_coarse(x, core, coarse_out, coarse, sem.at[2]))
    for copy in copies:
        copy.wait()


def other_levels(x, mid, coarse):
    return pl.pallas_call(
        other_kernel,
        out_shape=LEVELS,
        in_specs=[WHOLE, FAR, FAR],
        out_specs=(FAR,) * 2,
        scratch_shapes=[
            pltpu.VMEM((16, H // 8, LANES), f32),
            pltpu.SemaphoreType.DMA((3,)),
        ],
        input_output_aliases={1: 0, 2: 1},
        compiler_params=LIMIT,
        cost_estimate=cost(1),
        name="other_levels",
    )(*held(x), *far(mid, coarse))


def swaps(devices, first):
    pairs = [(i, i + 1) for i in range(first, devices - 1, 2)]
    return pairs + [(b, a) for a, b in pairs]


def exchange(even, odd, axis):
    devices = lax.axis_size(axis)
    odd = lax.ppermute(odd, axis, swaps(devices, 1))
    even = lax.ppermute(even, axis, swaps(devices, 0))
    return even, odd


def per_device(sources, labels):
    even, odd = pack_rows(sources, labels)
    even, odd, planes, marks = lax.optimization_barrier((even, odd, sources, labels))
    r_even, r_odd = exchange(even, odd, ROW)
    ext, lext, left, right, v0, v1, v2, totals, base = load(planes, marks)
    c_even, c_odd = exchange(*pack_columns(r_even, r_odd, left, right), "col")
    v0, v1, v2, base, totals = inner(ext, lext, v0, v1, v2, base, r_even, r_odd, totals)
    w, sums = seam(base, totals, c_even, c_odd)
    v0, v1, v2, pooled = pool(v0, v1, v2, w)
    sums = lax.all_to_all(sums, ALL, split_axis=0, concat_axis=0, tiled=True)
    coef, mid = solve(sums.reshape(256, LANES), pooled)
    mid = lax.all_to_all(mid, CHIP, split_axis=0, concat_axis=0, tiled=True)
    other = lax.ppermute(mid, "row_2", [(0, 1), (1, 0)])
    blended, fine, overview_mid, overview_coarse = own_levels(mid, coef, v0, v1, v2)
    overview_mid, overview_coarse = other_levels(other, overview_mid, overview_coarse)
    overview_mid = overview_mid.reshape(8 * H, W // 4)
    overview_coarse = overview_coarse.reshape(4 * H, W // 8)
    return (blended, fine, overview_mid, overview_coarse)


def solution(mesh):
    finer = Mesh(
        mesh.devices.reshape(4, 4, 2, mesh.shape["col"]), ("row_0", "row_1", "row_2", "col")
    )
    return jax.shard_map(
        per_device,
        mesh=finer,
        in_specs=(P(None, ROW, "col"), P(ROW, "col")),
        out_specs=(P(ROW, "col"), P(ROW, "col"), P(None, "col"), P(None, "col")),
        check_vma=False,
    )
```

```python
import jax
import jax.numpy as jnp
from jax import lax
from jax.experimental import pallas as pl
from jax.experimental.pallas import tpu as pltpu
from jax.sharding import Mesh
from jax.sharding import PartitionSpec as P


K = 3
H, W = 128, 1024
TOP = 16
ROWS = TOP + H + 24
LANES = 128
BLOCKS = W // LANES
HALO = 4
ROW = ("row_0", "row_1", "row_2")
CHIP = ("row_0", "row_1")
ALL = ("row_0", "row_1", "row_2", "col")
VMEM = pltpu.MemorySpace.VMEM
WHOLE = pl.BlockSpec(memory_space=VMEM)
FAR = pl.BlockSpec(memory_space=pltpu.MemorySpace.HBM)
LIMIT = pltpu.CompilerParams(vmem_limit_bytes=24 * 2**20)
TILES = H // 8
LEFT, RIGHT = HALO, 64
SEAM = 12
f32 = jnp.float32


def iota(shape, dim):
    return lax.broadcasted_iota(jnp.int32, shape, dim)


def place():
    row = (lax.axis_index("row_0") * 4 + lax.axis_index("row_1")) * 2 + lax.axis_index("row_2")
    return row, lax.axis_index("col")


def near(shape, dtype=f32):
    return pltpu.VMEM(shape, dtype)


def held(*values):
    return [pltpu.with_memory_space_constraint(v, VMEM) for v in values]


def far(*values):
    return [pltpu.with_memory_space_constraint(v, pltpu.MemorySpace.HBM) for v in values]


def cost(us):
    return pl.CostEstimate(flops=int(us * 3e8), bytes_accessed=0, transcendentals=0)


def pack_kernel(src, lab, even_out, odd_out, rows, lrows, sem):
    copies = []
    for side, start in ((0, 0), (1, H - 8)):
        for i, (a, b) in enumerate(
            (
                (src.at[:, pl.ds(start, 8), :], rows.at[side]),
                (lab.at[pl.ds(start, 8), :], lrows.at[side]),
            )
        ):
            c = pltpu.make_async_copy(a, b, sem.at[side, i])
            c.start()
            copies.append(c)
    for c in copies:
        c.wait()
    row, _ = place()
    even = (row % 2) == 0
    upper = iota((8, W), 0) < HALO

    def sides(side):
        a = [rows[side, k] for k in range(K)] + [lrows[side].astype(f32)]
        pairs = []
        for x, y in ((a[0], a[1]), (a[2], a[3])):
            if side == 0:
                pairs.append(jnp.where(upper, x, pltpu.roll(y, HALO, 0)))
            else:
                pairs.append(jnp.where(upper, pltpu.roll(x, HALO, 0), y))
        return pairs

    top, bottom = sides(0), sides(1)
    for i in range(2):
        even_out[pl.ds(8 * i, 8), :] = jnp.where(even, bottom[i], top[i])
        odd_out[pl.ds(8 * i, 8), :] = jnp.where(even, top[i], bottom[i])


def pack_rows(sources, labels):
    return pl.pallas_call(
        pack_kernel,
        out_shape=(near((16, W)), near((16, W))),
        in_specs=[FAR] * 2,
        out_specs=(WHOLE,) * 2,
        scratch_shapes=[
            pltpu.VMEM((2, K, 8, W), f32),
            pltpu.VMEM((2, 8, W), jnp.int32),
            pltpu.SemaphoreType.DMA((2, 2)),
        ],
        compiler_params=LIMIT,
        cost_estimate=cost(1),
        name="pack_rows",
    )(*far(sources, labels))


def window(lane, start, size):
    return (lane >= start) & (lane < start + size)


def turn(x, shift):
    shift %= LANES
    return pltpu.roll(x, shift, 1) if shift else x


def load_kernel(
    src, lab, ext, lext, left_out, right_out, v0, v1, v2, totals_out, seam_out
):
    own = pl.ds(TOP, H)
    for j in (0, BLOCKS - 1, *range(1, BLOCKS - 1)):
        lanes = pl.ds(j * LANES, LANES)
        for k in range(K):
            ext[k, j, own, :] = src[k, :, lanes]
        lext[j, own, :] = lab[:, lanes]
    lane = iota((8, LANES), 1)
    for j, out, first in ((0, left_out, 0), (BLOCKS - 1, right_out, LANES - HALO)):
        for half in range(2):
            total = jnp.zeros((8, LANES), f32)
            for g in range(8):
                at = pl.ds(TOP + 64 * half + 8 * g, 8)
                for k in range(K + 1):
                    x = ext[k, j, at, :] if k < K else lext[j, at, :].astype(f32)
                    to = 16 * g + HALO * k
                    total = jnp.where(window(lane, to, HALO), turn(x, to - first), total)
            out[pl.ds(8 * half, 8), :] = total

    over_tiles(1, TILES - 2, 7, lambda base, c: (right_side(ext, lext, v0, base), c)[1], 0)
    over_tiles(2, TILES - 3, 6, lambda base, c: (neighbours(v0, v1, base), c)[1], 0)
    over_tiles(3, TILES - 4, 5, lambda base, c: (neighbours(v1, v2, base), c)[1], 0)
    zero = jnp.zeros((8, LANES), f32)
    totals = over_tiles(3, TILES - 5, 3, lambda base, c: products(v0, v1, v2, base, c), (zero,) * 6)
    for i in range(6):
        totals_out[i] = totals[i]
    for tile in range(TILES):
        seam_base(ext, lext, seam_out, tile)


def load(sources, labels):
    field = near((BLOCKS, ROWS, LANES))
    return pl.pallas_call(
        load_kernel,
        out_shape=(
            near((K, BLOCKS, ROWS, LANES)),
            near((BLOCKS, ROWS, LANES), jnp.int32),
            near((16, LANES)),
            near((16, LANES)),
            field,
            field,
            field,
            near((6, 8, LANES)),
            near((K + 1, ROWS, LANES)),
        ),
        in_specs=[WHOLE] * 2,
        out_specs=(WHOLE,) * 9,
        compiler_params=LIMIT,
        cost_estimate=cost(3),
        name="load_block",
    )(*held(sources, labels))


def corner_kernel(got_even, got_odd, left, right, even_out, odd_out):
    row, col = place()
    row_even = (row % 2) == 0
    col_even = (col % 2) == 0
    upper = iota((8, LANES), 0) < HALO
    lane = iota((8, LANES), 1)
    strips = []
    for start, first in ((0, 0), (W - LANES, LANES - HALO)):
        total = jnp.zeros((8, LANES), f32)
        for k in range(K + 1):
            tile, half = divmod(k, 2)
            at = (pl.ds(8 * tile, 8), pl.ds(start, LANES))
            e, o = got_even[at], got_odd[at]
            above = jnp.where(row_even, o, e)
            below = jnp.where(row_even, e, o)
            if half:
                both = jnp.where(upper, pltpu.roll(above, HALO, 0), below)
            else:
                both = jnp.where(upper, above, pltpu.roll(below, HALO, 0))
            total = jnp.where(window(lane, HALO * k, HALO), turn(both, HALO * k - first), total)
        strips.append(total)
    even_out[pl.ds(0, 16), :] = jnp.where(col_even, right[...], left[...])
    odd_out[pl.ds(0, 16), :] = jnp.where(col_even, left[...], right[...])
    even_out[pl.ds(16, 8), :] = jnp.where(col_even, strips[1], strips[0])
    odd_out[pl.ds(16, 8), :] = jnp.where(col_even, strips[0], strips[1])


def pack_columns(got_even, got_odd, left, right):
    return pl.pallas_call(
        corner_kernel,
        out_shape=(near((24, LANES)),) * 2,
        in_specs=[WHOLE] * 4,
        out_specs=(WHOLE,) * 2,
        compiler_params=LIMIT,
        cost_estimate=cost(0.5),
        name="pack_columns",
    )(*held(got_even, got_odd, left, right))


def two_sum(a, b):
    s = a + b
    t = s - a
    return s, (a - (s - t)) + (b - t)


def shifted(tiles):
    lane = iota((8, LANES), 1)
    to_left = [pltpu.roll(t, LANES - 1, 1) for t in tiles]
    to_right = [pltpu.roll(t, 1, 1) for t in tiles]
    last, first = lane == LANES - 1, lane == 0
    n = len(tiles)
    after = [jnp.where(last, to_left[min(j + 1, n - 1)], to_left[j]) for j in range(n)]
    before = [jnp.where(first, to_right[max(j - 1, 0)], to_right[j]) for j in range(n)]
    return after, before


PAIRS = ((0, 0), (0, 1), (1, 1), (1, 2), (2, 2), (2, 3))


def right_side(ext, lext, out, base):
    at = pl.ds(base, 8)
    picked = [lext[j, at, :] for j in range(BLOCKS)]
    center, around = [None] * BLOCKS, [None] * BLOCKS
    for k in range(K):
        tiles = [ext[k, j, at, :] for j in range(BLOCKS)]
        after, before = shifted(tiles)
        for j in range(BLOCKS):
            near_sum = ext[k, j, pl.ds(base + 1, 8), :] + ext[k, j, pl.ds(base - 1, 8), :]
            near_sum = near_sum + after[j] + before[j]
            here = picked[j] == k
            center[j] = jnp.where(here, tiles[j], center[j]) if k else tiles[j]
            around[j] = jnp.where(here, near_sum, around[j]) if k else near_sum
    for j in range(BLOCKS):
        out[j, at, :] = 4.0 * center[j] - around[j]


def neighbours(source, target, base):
    tiles = [source[j, pl.ds(base, 8), :] for j in range(BLOCKS)]
    after, before = shifted(tiles)
    for j in range(BLOCKS):
        vertical = source[j, pl.ds(base + 1, 8), :] + source[j, pl.ds(base - 1, 8), :]
        target[j, pl.ds(base, 8), :] = vertical + after[j] + before[j]


def over_tiles(first, last, chunk, step, carry):
    def turn_of(t, carry):
        for u in range(chunk):
            carry = step(pl.multiple_of(TOP + 8 * first + 8 * (chunk * t + u), 8), carry)
        return carry

    return lax.fori_loop(0, (last - first + 1) // chunk, turn_of, carry)


def tree(x):
    while len(x) > 1:
        x = [sum(x[a : a + 2][1:], x[a]) for a in range(0, len(x), 2)]
    return x[0]


def products(v0, v1, v2, base, totals):
    lane = iota((8, LANES), 1)
    last = lane == LANES - 1
    kept = {0: lane >= HALO, BLOCKS - 1: lane < LANES - HALO}
    at = pl.ds(base, 8)
    found = [[] for _ in PAIRS]
    rolled = [turn(v2[j, at, :], -1) for j in range(BLOCKS)]
    for j in range(BLOCKS):
        x = [v[j, at, :] for v in (v0, v1, v2)]
        right = jnp.where(last, rolled[min(j + 1, BLOCKS - 1)], rolled[j])
        x.append(v2[j, pl.ds(base + 1, 8), :] + right)
        own = [jnp.where(kept[j], a, 0.0) for a in x[:3]] if j in kept else x
        for i, (a, b) in enumerate(PAIRS):
            found[i].append(own[a] * x[b])
    return tuple(total + tree(f) for total, f in zip(totals, found))


def seam_base(ext, lext, out, tile):
    lane = iota((8, LANES), 1)
    at = pl.ds(TOP + 8 * tile, 8)
    for k in range(K + 1):
        a, b = [ext[k, j, at, :] if k < K else lext[j, at, :].astype(f32) for j in (0, BLOCKS - 1)]
        out[k, at, :] = jnp.where(lane < 64, turn(a, LEFT), turn(b, RIGHT + SEAM))


def clear_rows(ref, row):
    @pl.when(row == 0)
    def _():
        for j in range(BLOCKS):
            ref[j, pl.ds(TOP - 8, 8), :] = jnp.zeros((8, LANES), f32)

    @pl.when(row == 31)
    def _():
        for j in range(BLOCKS):
            ref[j, pl.ds(TOP + H, 8), :] = jnp.zeros((8, LANES), f32)


def inner_kernel(*refs):
    r_even, r_odd, totals_in = refs[6:9]
    ext, lext, v0, v1, v2, seam_out, totals_out = refs[9:]
    row, _ = place()
    row_even = (row % 2) == 0
    for k in range(K + 1):
        at = pl.ds(HALO * k, HALO)
        for j in range(BLOCKS):
            lanes = pl.ds(j * LANES, LANES)
            e, o = r_even[at, lanes], r_odd[at, lanes]
            above, below = jnp.where(row_even, o, e), jnp.where(row_even, e, o)
            for start, value in ((TOP - HALO, above), (TOP + H, below)):
                if k < K:
                    ext[k, j, pl.ds(start, HALO), :] = value
                else:
                    lext[j, pl.ds(start, HALO), :] = value.astype(jnp.int32)
    seam_base(ext, lext, seam_out, -1)
    seam_base(ext, lext, seam_out, TILES)
    for t in (-1, 0, TILES - 1, TILES):
        right_side(ext, lext, v0, TOP + 8 * t)
    clear_rows(v0, row)
    for t in (-1, 0, 1, TILES - 2, TILES - 1, TILES):
        neighbours(v0, v1, TOP + 8 * t)
    clear_rows(v1, row)
    for t in (-1, 0, 1, 2, TILES - 3, TILES - 2, TILES - 1, TILES):
        neighbours(v1, v2, TOP + 8 * t)
    clear_rows(v2, row)
    totals = tuple(totals_in[i] for i in range(6))
    for t in (0, 1, 2, *range(TILES - 4, TILES)):
        totals = products(v0, v1, v2, TOP + 8 * t, totals)
    for i in range(6):
        totals_out[i] = totals[i]


def inner(ext, lext, v0, v1, v2, base, r_even, r_odd, totals):
    field = near((BLOCKS, ROWS, LANES))
    return pl.pallas_call(
        inner_kernel,
        out_shape=(
            near((K, BLOCKS, ROWS, LANES)),
            near((BLOCKS, ROWS, LANES), jnp.int32),
            field,
            field,
            field,
            near((K + 1, ROWS, LANES)),
            near((6, 8, LANES)),
        ),
        in_specs=[WHOLE] * 9,
        out_specs=(WHOLE,) * 7,
        input_output_aliases={i: i for i in range(6)},
        compiler_params=LIMIT,
        cost_estimate=cost(2),
        name="inner_fields",
    )(*held(ext, lext, v0, v1, v2, base, r_even, r_odd, totals))[2:]


def seam_kernel(base, totals_in, c_even, c_odd, w, sums_out, planes):
    row, col = place()
    col_even = (col % 2) == 0
    lane = iota((8, LANES), 1)
    from_left, from_right = lane < LEFT, window(lane, RIGHT + SEAM, HALO)
    outside = (from_left & (col == 0)) | (from_right & (col == 7))
    for t in range(TILES + 2):
        at = pl.ds(TOP - 8 + 8 * t, 8)
        corner = t in (0, TILES + 1)
        tile, g = (2, 0) if corner else divmod(t - 1, 8)
        e, o = c_even[pl.ds(8 * tile, 8), :], c_odd[pl.ds(8 * tile, 8), :]
        a, b = jnp.where(col_even, o, e), jnp.where(col_even, e, o)
        if corner:
            a, b = pltpu.roll(a, HALO, 0), pltpu.roll(b, HALO, 0)
        for k in range(K + 1):
            lanes = 16 * g + HALO * k
            planes[k, at, :] = jnp.where(
                from_left,
                turn(a, -lanes),
                jnp.where(from_right, turn(b, RIGHT + SEAM - lanes), base[k, at, :]),
            )

    def put(i, t, value):
        hidden = outside
        if t == 0:
            hidden = hidden | (row == 0)
        if t == TILES + 1:
            hidden = hidden | (row == 31)
        w[i, pl.ds(TOP - 8 + 8 * t, 8), :] = jnp.where(hidden, 0.0, value)

    for t in range(TILES + 2):
        start = TOP - 8 + 8 * t
        total = jnp.zeros((8, LANES), f32)
        picked = planes[K, pl.ds(start, 8), :]
        for k in range(K):
            x = planes[k, pl.ds(start, 8), :]
            vertical = planes[k, pl.ds(start + 1, 8), :] + planes[k, pl.ds(start - 1, 8), :]
            term = 4.0 * x - (vertical + turn(x, -1) + turn(x, 1))
            total = jnp.where(picked == k, term, total)
        put(0, t, total)
    for i in range(2):
        for t in range(TILES + 2):
            start = TOP - 8 + 8 * t
            x = w[i, pl.ds(start, 8), :]
            vertical = w[i, pl.ds(start + 1, 8), :] + w[i, pl.ds(start - 1, 8), :]
            put(i + 1, t, vertical + turn(x, -1) + turn(x, 1))
    own_lane = window(lane, LEFT, HALO) | window(lane, RIGHT + SEAM - HALO, HALO)
    found = [[] for _ in PAIRS]
    for t in range(TILES):
        start = TOP + 8 * t
        x = [w[i, pl.ds(start, 8), :] for i in range(3)]
        x.append(w[2, pl.ds(start + 1, 8), :] + turn(x[2], -1))
        for i, (a, b) in enumerate(PAIRS):
            found[i].append(x[a] * x[b])
    totals = [totals_in[i] + jnp.where(own_lane, tree(found[i]), 0.0) for i in range(6)]

    line = jnp.zeros((8, LANES), f32)
    for i in range(6):
        x = totals[i] + totals[i] if i == 5 else totals[i]
        big = 512.0 * jnp.max(jnp.abs(x), axis=1, keepdims=True)
        high = (x + big) - big
        line = jnp.where(
            (lane == i) | (lane == i + 16),
            jnp.sum(high, axis=1, keepdims=True),
            jnp.where(lane == i + 8, jnp.sum(x - high, axis=1, keepdims=True), line),
        )
    s, e = line, jnp.zeros_like(line)
    for shift in (4, 2, 1):
        s, more = two_sum(s, pltpu.roll(s, shift, 0))
        e = e + pltpu.roll(e, shift, 0) + more
    line = jnp.where(lane < 16, s, e)[:1].reshape(1, 1, LANES)
    sums_out[...] = jnp.broadcast_to(line, (256, 1, LANES))


def seam(base, totals, c_even, c_odd):
    return pl.pallas_call(
        seam_kernel,
        out_shape=(near((3, ROWS, LANES)), near((256, 1, LANES))),
        in_specs=[WHOLE] * 4,
        out_specs=(WHOLE,) * 2,
        scratch_shapes=[pltpu.VMEM((K + 1, ROWS, LANES), f32)],
        compiler_params=LIMIT,
        cost_estimate=cost(1),
        name="seam_fields",
    )(*held(base, totals, c_even, c_odd))


def pool_kernel(v0, v1, v2, out):
    spread = jnp.where(iota((512, LANES), 0) // 4 == iota((512, LANES), 1), f32(0.0625), f32(0.0))
    for i, ref in enumerate((v0, v1, v2)):
        for g in range(2):
            parts = []
            for j in range(4):
                at = [ref[4 * g + j, pl.ds(TOP + q, H // 4, stride=4), :] for q in range(4)]
                parts.append((at[0] + at[1]) + (at[2] + at[3]))
            out[i, g] = jnp.dot(
                jnp.concatenate(parts, 1), spread, precision=lax.Precision.HIGHEST, preferred_element_type=f32
            )


def pool(v0, v1, v2):
    return pl.pallas_call(
        pool_kernel,
        out_shape=near((3, 2, H // 4, LANES)),
        in_specs=[WHOLE] * 3,
        out_specs=WHOLE,
        compiler_params=LIMIT,
        cost_estimate=cost(1),
        name="pool_fields",
    )(*held(v0, v1, v2))


def two_product(a, b):
    p = a * b
    big = f32(4097.0)
    t = big * a
    ah = t - (t - a)
    al = a - ah
    t = big * b
    bh = t - (t - b)
    bl = b - bh
    return p, ((ah * bh - p) + ah * bl + al * bh) + al * bl


def less_scaled(a, b, scale):
    p, low = two_product(b[0], scale)
    low = low + b[1] * scale
    s, e = two_sum(a[0], -p)
    e = e + (a[1] - low)
    return two_sum(s, e)


def coefficients(n):
    shift = n[1][0] / n[0][0]
    current = n
    m = [n[0][0]]
    for _ in range(5):
        current = [less_scaled(current[i + 1], current[i], shift) for i in range(len(current) - 1)]
        m.append(current[0][0] + current[0][1])
    m0, m1, m2, m3, m4, m5 = m
    t = m1 / m0
    theta0 = shift + t
    m5 = m5 - 5.0 * t * m4
    m4 = m4 - 4.0 * t * m3
    m3 = m3 - 3.0 * t * m2
    m2 = m2 - t * m1
    one = jnp.ones_like(m0)
    zero = jnp.zeros_like(m0)
    second = m2 > 0.0
    safe2 = jnp.where(second, m2, one)
    b1 = jnp.where(second, m2 / m0, zero)
    s = jnp.where(second, m3 / safe2, zero)
    h2 = m4 - s * m3 - b1 * m2
    third = second & (h2 > 0.0)
    safe3 = jnp.where(third, h2, one)
    theta1 = theta0 + s
    theta2 = theta0 - s + (m5 - s * m4 - b1 * m3) / safe3
    b2 = h2 / safe2
    d0, d1, d2 = 4.0 - theta0, 4.0 - theta1, 4.0 - theta2
    e = d1 * d2 - b2
    y2 = jnp.where(third, one / (d0 * e - b1 * d2), zero)
    y1 = jnp.where(third, d2 * y2, jnp.where(second, one / (d0 * d1 - b1), zero))
    y0 = jnp.where(third, e * y2, jnp.where(second, d1 * y1, one / d0))
    return (
        y0 - theta0 * y1 + (theta0 * theta1 - b1) * y2,
        y1 - (theta0 + theta1) * y2,
        y2,
    )


def solve_kernel(all_sums, pooled, w, coef_out, mid_out):
    frm, to = iota((LANES, LANES), 0), iota((LANES, LANES), 1)
    first = window(frm, LEFT, HALO) & (to == 0)
    final = window(frm, RIGHT + SEAM - HALO, HALO) & (to == LANES - 1)
    rows = []
    for i in range(3):
        at = [w[i, pl.ds(TOP + q, H // 4, stride=4), :] for q in range(4)]
        rows.append((at[0] + at[1]) + (at[2] + at[3]))
    edges = jnp.dot(
        jnp.concatenate(rows, 0),
        jnp.where(first | final, f32(0.0625), f32(0.0)),
        precision=lax.Precision.HIGHEST,
        preferred_element_type=f32,
    )
    tiles = [(all_sums[pl.ds(8 * i, 8), :], jnp.zeros((8, LANES), f32)) for i in range(32)]
    while len(tiles) > 1:
        merged = []
        for a, b in zip(tiles[0::2], tiles[1::2]):
            s, e = two_sum(a[0], b[0])
            merged.append((s, e + (a[1] + b[1])))
        tiles = merged
    s, e = tiles[0]
    for shift in (4, 2, 1):
        s, more = two_sum(s, pltpu.roll(s, shift, 0))
        e = e + pltpu.roll(e, shift, 0) + more
    lane = iota((8, LANES), 1)
    zero = jnp.zeros((8, LANES), f32)

    def over_lanes(x):
        return jnp.broadcast_to(jnp.sum(x, axis=1, keepdims=True), (8, LANES))

    n = []
    for i in range(6):
        high = over_lanes(jnp.where(lane == i, s, zero))
        low = over_lanes(jnp.where((lane == i + 8) | (lane == i + 16), s, jnp.where(lane == i, e, zero)))
        n.append(two_sum(high, low))
    c = coefficients(n)
    for i in range(3):
        coef_out[i] = c[i]
    for g in range(2):
        edge = lane == (LANES - 1 if g else 0)
        for q in range(H // 4 // 8):
            at = (g, pl.ds(8 * q, 8), slice(None))
            value = zero
            for i in range(3):
                start = H // 4 * i + 8 * q
                value = value + c[i] * jnp.where(edge, edges[start : start + 8], pooled[(i, *at)])
            for d in range(16):
                mid_out[(d, *at)] = value


def solve(all_sums, pooled, w):
    return pl.pallas_call(
        solve_kernel,
        out_shape=(near((3, 8, LANES)), near((16, 2, H // 4, LANES))),
        in_specs=[WHOLE] * 3,
        out_specs=(WHOLE,) * 2,
        compiler_params=LIMIT,
        cost_estimate=cost(1),
        name="coefficients",
    )(*held(all_sums, pooled, w))


def half_matrix(rows):
    return jnp.where(iota((rows, rows // 2), 0) // 2 == iota((rows, rows // 2), 1), f32(0.25), f32(0.0))


def pooled_rows(parts):
    return jnp.dot(
        jnp.concatenate(parts, 1),
        half_matrix(2 * LANES),
        precision=lax.Precision.HIGHEST,
        preferred_element_type=f32,
    )


def store_mid(x, core, mid_out, sem):
    copies = []
    for g in range(2):
        to = mid_out.at[:, core, :, pl.ds(g * LANES, LANES)]
        copies.append(pltpu.make_async_copy(x.at[:, g], to, sem.at[g]))
        copies[-1].start()
    return copies


def store_coarse(x, core, coarse_out, scratch, sem):
    rows = H // 8
    parts = [
        jnp.concatenate(
            [x[d, g, pl.ds(0, rows, stride=2), :] + x[d, g, pl.ds(1, rows, stride=2), :] for d in range(16)], 0
        )
        for g in range(2)
    ]
    pooled = pooled_rows(parts)
    for d in range(16):
        scratch[d] = pooled[d * rows : (d + 1) * rows]
    copy = pltpu.make_async_copy(scratch, coarse_out.at[:, core], sem)
    copy.start()
    return copy


def own_kernel(
    x, coef, v0, v1, v2, w, blended_out, fine_out, mid_out, coarse_out, flat, stacked, fine, coarse, sem
):
    core = lax.axis_index("row_2")
    copies = store_mid(x, core, mid_out, sem)
    c = [coef[i] for i in range(3)]
    lane = iota((8, LANES), 1)
    parts = 4
    for p in range(parts):
        for u in range(TILES // parts):
            base = 8 * (p * (TILES // parts) + u)
            rows = pl.ds(base + TOP, 8)
            seams = c[0] * w[0, rows, :] + c[1] * w[1, rows, :] + c[2] * w[2, rows, :]
            for j in range(BLOCKS):
                at = (j, rows, slice(None))
                value = c[0] * v0[at] + c[1] * v1[at] + c[2] * v2[at]
                if j == 0:
                    value = jnp.where(lane < HALO, turn(seams, -LEFT), value)
                if j == BLOCKS - 1:
                    value = jnp.where(lane >= LANES - HALO, turn(seams, LANES - RIGHT - SEAM), value)
                flat[pl.ds(base, 8), pl.ds(j * LANES, LANES)] = value
                stacked[j, pl.ds(base, 8), :] = value
        rows = pl.ds(p * H // parts, H // parts)
        copies.append(pltpu.make_async_copy(flat.at[rows, :], blended_out.at[rows, :], sem.at[3 + p]))
        copies[-1].start()
    for g in range(BLOCKS // 2):
        halves = [
            stacked[2 * g + i, pl.ds(0, H // 2, stride=2), :] + stacked[2 * g + i, pl.ds(1, H // 2, stride=2), :]
            for i in range(2)
        ]
        fine[:, pl.ds(g * LANES, LANES)] = pooled_rows(halves)
    copies.append(pltpu.make_async_copy(fine, fine_out, sem.at[3 + parts]))
    copies[-1].start()
    copies.append(store_coarse(x, core, coarse_out, coarse, sem.at[2]))
    for copy in copies:
        copy.wait()


LEVELS = (
    jax.ShapeDtypeStruct((16, 2, H // 4, W // 4), f32),
    jax.ShapeDtypeStruct((16, 2, H // 8, W // 8), f32),
)


def own_levels(x, coef, v0, v1, v2, w):
    return pl.pallas_call(
        own_kernel,
        out_shape=(
            jax.ShapeDtypeStruct((H, W), f32),
            jax.ShapeDtypeStruct((H // 2, W // 2), f32),
            *LEVELS,
        ),
        in_specs=[WHOLE] * 6,
        out_specs=(FAR,) * 4,
        scratch_shapes=[
            pltpu.VMEM((H, W), f32),
            pltpu.VMEM((BLOCKS, H, LANES), f32),
            pltpu.VMEM((H // 2, W // 2), f32),
            pltpu.VMEM((16, H // 8, LANES), f32),
            pltpu.SemaphoreType.DMA((8,)),
        ],
        compiler_params=LIMIT,
        cost_estimate=cost(2),
        name="own_levels",
    )(*held(x, coef, v0, v1, v2, w))


def other_kernel(x, mid_in, coarse_in, mid_out, coarse_out, coarse, sem):
    del mid_in, coarse_in
    core = 1 - lax.axis_index("row_2")
    copies = store_mid(x, core, mid_out, sem)
    copies.append(store_coarse(x, core, coarse_out, coarse, sem.at[2]))
    for copy in copies:
        copy.wait()


def other_levels(x, mid, coarse):
    return pl.pallas_call(
        other_kernel,
        out_shape=LEVELS,
        in_specs=[WHOLE, FAR, FAR],
        out_specs=(FAR,) * 2,
        scratch_shapes=[
            pltpu.VMEM((16, H // 8, LANES), f32),
            pltpu.SemaphoreType.DMA((3,)),
        ],
        input_output_aliases={1: 0, 2: 1},
        compiler_params=LIMIT,
        cost_estimate=cost(1),
        name="other_levels",
    )(*held(x), *far(mid, coarse))


def swaps(devices, first):
    pairs = [(i, i + 1) for i in range(first, devices - 1, 2)]
    return pairs + [(b, a) for a, b in pairs]


def exchange(even, odd, axis):
    devices = lax.axis_size(axis)
    odd = lax.ppermute(odd, axis, swaps(devices, 1))
    even = lax.ppermute(even, axis, swaps(devices, 0))
    return even, odd


def per_device(sources, labels):
    even, odd = pack_rows(sources, labels)
    even, odd, planes, marks = lax.optimization_barrier((even, odd, sources, labels))
    r_even, r_odd = exchange(even, odd, ROW)
    ext, lext, left, right, v0, v1, v2, totals, base = load(planes, marks)
    c_even, c_odd = exchange(*pack_columns(r_even, r_odd, left, right), "col")
    v0, v1, v2, base, totals = inner(ext, lext, v0, v1, v2, base, r_even, r_odd, totals)
    pooled, totals = lax.optimization_barrier((pool(v0, v1, v2), totals))
    w, sums = seam(base, totals, c_even, c_odd)
    sums = lax.all_to_all(sums, ALL, split_axis=0, concat_axis=0, tiled=True)
    coef, mid = solve(sums.reshape(256, LANES), pooled, w)
    mid = lax.all_to_all(mid, CHIP, split_axis=0, concat_axis=0, tiled=True)
    other = lax.ppermute(mid, "row_2", [(0, 1), (1, 0)])
    blended, fine, overview_mid, overview_coarse = own_levels(mid, coef, v0, v1, v2, w)
    overview_mid, overview_coarse = other_levels(other, overview_mid, overview_coarse)
    overview_mid = overview_mid.reshape(8 * H, W // 4)
    overview_coarse = overview_coarse.reshape(4 * H, W // 8)
    return (blended, fine, overview_mid, overview_coarse)


def solution(mesh):
    finer = Mesh(
        mesh.devices.reshape(4, 4, 2, mesh.shape["col"]), ("row_0", "row_1", "row_2", "col")
    )
    return jax.shard_map(
        per_device,
        mesh=finer,
        in_specs=(P(None, ROW, "col"), P(ROW, "col")),
        out_specs=(P(ROW, "col"), P(ROW, "col"), P(None, "col"), P(None, "col")),
        check_vma=False,
    )
```

```python
import jax
import jax.numpy as jnp
from jax import lax
from jax.experimental import pallas as pl
from jax.experimental.pallas import tpu as pltpu
from jax.sharding import Mesh
from jax.sharding import PartitionSpec as P


K = 3
H, W = 128, 1024
TOP = 16
ROWS = TOP + H + 24
LANES = 128
BLOCKS = W // LANES
HALO = 4
ROW = ("row_0", "row_1", "row_2")
CHIP = ("row_0", "row_1")
ALL = ("row_0", "row_1", "row_2", "col")
VMEM = pltpu.MemorySpace.VMEM
WHOLE = pl.BlockSpec(memory_space=VMEM)
FAR = pl.BlockSpec(memory_space=pltpu.MemorySpace.HBM)
LIMIT = pltpu.CompilerParams(vmem_limit_bytes=24 * 2**20)
TILES = H // 8
LEFT, RIGHT = HALO, 64
SEAM = 12
f32 = jnp.float32


def iota(shape, dim):
    return lax.broadcasted_iota(jnp.int32, shape, dim)


def place():
    row = (lax.axis_index("row_0") * 4 + lax.axis_index("row_1")) * 2 + lax.axis_index("row_2")
    return row, lax.axis_index("col")


def near(shape, dtype=f32):
    return pltpu.VMEM(shape, dtype)


def held(*values):
    return [pltpu.with_memory_space_constraint(v, VMEM) for v in values]


def far(*values):
    return [pltpu.with_memory_space_constraint(v, pltpu.MemorySpace.HBM) for v in values]


def cost(us):
    return pl.CostEstimate(flops=int(us * 3e8), bytes_accessed=0, transcendentals=0)


def sums_of(x, weights):
    total = None
    for _ in range(3):
        part = x.astype(jnp.bfloat16)
        x = x - part.astype(f32)
        term = jnp.dot(part, weights, preferred_element_type=f32)
        total = term if total is None else total + term
    return total


def pack_kernel(src, lab, even_out, odd_out, rows, lrows, sem):
    copies = []
    for side, start in ((0, 0), (1, H - 8)):
        for i, (a, b) in enumerate(
            (
                (src.at[:, pl.ds(start, 8), :], rows.at[side]),
                (lab.at[pl.ds(start, 8), :], lrows.at[side]),
            )
        ):
            c = pltpu.make_async_copy(a, b, sem.at[side, i])
            c.start()
            copies.append(c)
    for c in copies:
        c.wait()
    row, _ = place()
    even = (row % 2) == 0
    upper = iota((8, W), 0) < HALO

    def sides(side):
        a = [rows[side, k] for k in range(K)] + [lrows[side].astype(f32)]
        pairs = []
        for x, y in ((a[0], a[1]), (a[2], a[3])):
            if side == 0:
                pairs.append(jnp.where(upper, x, pltpu.roll(y, HALO, 0)))
            else:
                pairs.append(jnp.where(upper, pltpu.roll(x, HALO, 0), y))
        return pairs

    top, bottom = sides(0), sides(1)
    for i in range(2):
        even_out[pl.ds(8 * i, 8), :] = jnp.where(even, bottom[i], top[i])
        odd_out[pl.ds(8 * i, 8), :] = jnp.where(even, top[i], bottom[i])


def pack_rows(sources, labels):
    return pl.pallas_call(
        pack_kernel,
        out_shape=(near((16, W)), near((16, W))),
        in_specs=[FAR] * 2,
        out_specs=(WHOLE,) * 2,
        scratch_shapes=[
            pltpu.VMEM((2, K, 8, W), f32),
            pltpu.VMEM((2, 8, W), jnp.int32),
            pltpu.SemaphoreType.DMA((2, 2)),
        ],
        compiler_params=LIMIT,
        cost_estimate=cost(1),
        name="pack_rows",
    )(*far(sources, labels))


def window(lane, start, size):
    return (lane >= start) & (lane < start + size)


def turn(x, shift):
    shift %= LANES
    return pltpu.roll(x, shift, 1) if shift else x


def load_kernel(
    src, lab, ext, lext, left_out, right_out, v0, v1, v2, totals_out, seam_out
):
    own = pl.ds(TOP, H)
    for j in (0, BLOCKS - 1, *range(1, BLOCKS - 1)):
        lanes = pl.ds(j * LANES, LANES)
        for k in range(K):
            ext[k, j, own, :] = src[k, :, lanes]
        lext[j, own, :] = lab[:, lanes]
    lane = iota((8, LANES), 1)
    for j, out, first in ((0, left_out, 0), (BLOCKS - 1, right_out, LANES - HALO)):
        for half in range(2):
            total = jnp.zeros((8, LANES), f32)
            for g in range(8):
                at = pl.ds(TOP + 64 * half + 8 * g, 8)
                for k in range(K + 1):
                    x = ext[k, j, at, :] if k < K else lext[j, at, :].astype(f32)
                    to = 16 * g + HALO * k
                    total = jnp.where(window(lane, to, HALO), turn(x, to - first), total)
            out[pl.ds(8 * half, 8), :] = total

    over_tiles(1, TILES - 2, 7, lambda base, c: (right_side(ext, lext, v0, base), c)[1], 0)
    over_tiles(2, TILES - 3, 6, lambda base, c: (neighbours(v0, v1, base), c)[1], 0)
    over_tiles(3, TILES - 4, 5, lambda base, c: (neighbours(v1, v2, base), c)[1], 0)
    zero = jnp.zeros((8, LANES), f32)
    totals = over_tiles(3, TILES - 5, 3, lambda base, c: products(v0, v1, v2, base, c), (zero,) * 6)
    for i in range(6):
        totals_out[i] = totals[i]
    for tile in range(TILES):
        seam_base(ext, lext, seam_out, tile)


def load(sources, labels):
    field = near((BLOCKS, ROWS, LANES))
    return pl.pallas_call(
        load_kernel,
        out_shape=(
            near((K, BLOCKS, ROWS, LANES)),
            near((BLOCKS, ROWS, LANES), jnp.int32),
            near((16, LANES)),
            near((16, LANES)),
            field,
            field,
            field,
            near((6, 8, LANES)),
            near((K + 1, ROWS, LANES)),
        ),
        in_specs=[WHOLE] * 2,
        out_specs=(WHOLE,) * 9,
        compiler_params=LIMIT,
        cost_estimate=cost(3),
        name="load_block",
    )(*held(sources, labels))


def corner_kernel(got_even, got_odd, left, right, even_out, odd_out):
    row, col = place()
    row_even = (row % 2) == 0
    col_even = (col % 2) == 0
    upper = iota((8, LANES), 0) < HALO
    lane = iota((8, LANES), 1)
    strips = []
    for start, first in ((0, 0), (W - LANES, LANES - HALO)):
        total = jnp.zeros((8, LANES), f32)
        for k in range(K + 1):
            tile, half = divmod(k, 2)
            at = (pl.ds(8 * tile, 8), pl.ds(start, LANES))
            e, o = got_even[at], got_odd[at]
            above = jnp.where(row_even, o, e)
            below = jnp.where(row_even, e, o)
            if half:
                both = jnp.where(upper, pltpu.roll(above, HALO, 0), below)
            else:
                both = jnp.where(upper, above, pltpu.roll(below, HALO, 0))
            total = jnp.where(window(lane, HALO * k, HALO), turn(both, HALO * k - first), total)
        strips.append(total)
    even_out[pl.ds(0, 16), :] = jnp.where(col_even, right[...], left[...])
    odd_out[pl.ds(0, 16), :] = jnp.where(col_even, left[...], right[...])
    even_out[pl.ds(16, 8), :] = jnp.where(col_even, strips[1], strips[0])
    odd_out[pl.ds(16, 8), :] = jnp.where(col_even, strips[0], strips[1])


def pack_columns(got_even, got_odd, left, right):
    return pl.pallas_call(
        corner_kernel,
        out_shape=(near((24, LANES)),) * 2,
        in_specs=[WHOLE] * 4,
        out_specs=(WHOLE,) * 2,
        compiler_params=LIMIT,
        cost_estimate=cost(0.5),
        name="pack_columns",
    )(*held(got_even, got_odd, left, right))


def two_sum(a, b):
    s = a + b
    t = s - a
    return s, (a - (s - t)) + (b - t)


def shifted(tiles):
    lane = iota((8, LANES), 1)
    to_left = [pltpu.roll(t, LANES - 1, 1) for t in tiles]
    to_right = [pltpu.roll(t, 1, 1) for t in tiles]
    last, first = lane == LANES - 1, lane == 0
    n = len(tiles)
    after = [jnp.where(last, to_left[min(j + 1, n - 1)], to_left[j]) for j in range(n)]
    before = [jnp.where(first, to_right[max(j - 1, 0)], to_right[j]) for j in range(n)]
    return after, before


PAIRS = ((0, 0), (0, 1), (1, 1), (1, 2), (2, 2), (2, 3))


def right_side(ext, lext, out, base):
    at = pl.ds(base, 8)
    picked = [lext[j, at, :] for j in range(BLOCKS)]
    center, around = [None] * BLOCKS, [None] * BLOCKS
    for k in range(K):
        tiles = [ext[k, j, at, :] for j in range(BLOCKS)]
        after, before = shifted(tiles)
        for j in range(BLOCKS):
            near_sum = ext[k, j, pl.ds(base + 1, 8), :] + ext[k, j, pl.ds(base - 1, 8), :]
            near_sum = near_sum + after[j] + before[j]
            here = picked[j] == k
            center[j] = jnp.where(here, tiles[j], center[j]) if k else tiles[j]
            around[j] = jnp.where(here, near_sum, around[j]) if k else near_sum
    for j in range(BLOCKS):
        out[j, at, :] = 4.0 * center[j] - around[j]


def neighbours(source, target, base):
    tiles = [source[j, pl.ds(base, 8), :] for j in range(BLOCKS)]
    after, before = shifted(tiles)
    for j in range(BLOCKS):
        vertical = source[j, pl.ds(base + 1, 8), :] + source[j, pl.ds(base - 1, 8), :]
        target[j, pl.ds(base, 8), :] = vertical + after[j] + before[j]


def over_tiles(first, last, chunk, step, carry):
    def turn_of(t, carry):
        for u in range(chunk):
            carry = step(pl.multiple_of(TOP + 8 * first + 8 * (chunk * t + u), 8), carry)
        return carry

    return lax.fori_loop(0, (last - first + 1) // chunk, turn_of, carry)


def tree(x):
    while len(x) > 1:
        x = [sum(x[a : a + 2][1:], x[a]) for a in range(0, len(x), 2)]
    return x[0]


def products(v0, v1, v2, base, totals):
    lane = iota((8, LANES), 1)
    last = lane == LANES - 1
    kept = {0: lane >= HALO, BLOCKS - 1: lane < LANES - HALO}
    at = pl.ds(base, 8)
    found = [[] for _ in PAIRS]
    rolled = [turn(v2[j, at, :], -1) for j in range(BLOCKS)]
    for j in range(BLOCKS):
        x = [v[j, at, :] for v in (v0, v1, v2)]
        right = jnp.where(last, rolled[min(j + 1, BLOCKS - 1)], rolled[j])
        x.append(v2[j, pl.ds(base + 1, 8), :] + right)
        own = [jnp.where(kept[j], a, 0.0) for a in x[:3]] if j in kept else x
        for i, (a, b) in enumerate(PAIRS):
            found[i].append(own[a] * x[b])
    return tuple(total + tree(f) for total, f in zip(totals, found))


def seam_base(ext, lext, out, tile):
    lane = iota((8, LANES), 1)
    at = pl.ds(TOP + 8 * tile, 8)
    for k in range(K + 1):
        a, b = [ext[k, j, at, :] if k < K else lext[j, at, :].astype(f32) for j in (0, BLOCKS - 1)]
        out[k, at, :] = jnp.where(lane < 64, turn(a, LEFT), turn(b, RIGHT + SEAM))


def clear_rows(ref, row):
    @pl.when(row == 0)
    def _():
        for j in range(BLOCKS):
            ref[j, pl.ds(TOP - 8, 8), :] = jnp.zeros((8, LANES), f32)

    @pl.when(row == 31)
    def _():
        for j in range(BLOCKS):
            ref[j, pl.ds(TOP + H, 8), :] = jnp.zeros((8, LANES), f32)


def inner_kernel(*refs):
    r_even, r_odd, totals_in = refs[6:9]
    ext, lext, v0, v1, v2, seam_out, totals_out = refs[9:]
    row, _ = place()
    row_even = (row % 2) == 0
    for k in range(K + 1):
        at = pl.ds(HALO * k, HALO)
        for j in range(BLOCKS):
            lanes = pl.ds(j * LANES, LANES)
            e, o = r_even[at, lanes], r_odd[at, lanes]
            above, below = jnp.where(row_even, o, e), jnp.where(row_even, e, o)
            for start, value in ((TOP - HALO, above), (TOP + H, below)):
                if k < K:
                    ext[k, j, pl.ds(start, HALO), :] = value
                else:
                    lext[j, pl.ds(start, HALO), :] = value.astype(jnp.int32)
    seam_base(ext, lext, seam_out, -1)
    seam_base(ext, lext, seam_out, TILES)
    for t in (-1, 0, TILES - 1, TILES):
        right_side(ext, lext, v0, TOP + 8 * t)
    clear_rows(v0, row)
    for t in (-1, 0, 1, TILES - 2, TILES - 1, TILES):
        neighbours(v0, v1, TOP + 8 * t)
    clear_rows(v1, row)
    for t in (-1, 0, 1, 2, TILES - 3, TILES - 2, TILES - 1, TILES):
        neighbours(v1, v2, TOP + 8 * t)
    clear_rows(v2, row)
    totals = tuple(totals_in[i] for i in range(6))
    for t in (0, 1, 2, *range(TILES - 4, TILES)):
        totals = products(v0, v1, v2, TOP + 8 * t, totals)
    for i in range(6):
        totals_out[i] = totals[i]


def inner(ext, lext, v0, v1, v2, base, r_even, r_odd, totals):
    field = near((BLOCKS, ROWS, LANES))
    return pl.pallas_call(
        inner_kernel,
        out_shape=(
            near((K, BLOCKS, ROWS, LANES)),
            near((BLOCKS, ROWS, LANES), jnp.int32),
            field,
            field,
            field,
            near((K + 1, ROWS, LANES)),
            near((6, 8, LANES)),
        ),
        in_specs=[WHOLE] * 9,
        out_specs=(WHOLE,) * 7,
        input_output_aliases={i: i for i in range(6)},
        compiler_params=LIMIT,
        cost_estimate=cost(2),
        name="inner_fields",
    )(*held(ext, lext, v0, v1, v2, base, r_even, r_odd, totals))[2:]


def seam_kernel(base, totals_in, c_even, c_odd, w, sums_out, planes):
    row, col = place()
    col_even = (col % 2) == 0
    lane = iota((8, LANES), 1)
    from_left, from_right = lane < LEFT, window(lane, RIGHT + SEAM, HALO)
    outside = (from_left & (col == 0)) | (from_right & (col == 7))
    for t in range(TILES + 2):
        at = pl.ds(TOP - 8 + 8 * t, 8)
        corner = t in (0, TILES + 1)
        tile, g = (2, 0) if corner else divmod(t - 1, 8)
        e, o = c_even[pl.ds(8 * tile, 8), :], c_odd[pl.ds(8 * tile, 8), :]
        a, b = jnp.where(col_even, o, e), jnp.where(col_even, e, o)
        if corner:
            a, b = pltpu.roll(a, HALO, 0), pltpu.roll(b, HALO, 0)
        for k in range(K + 1):
            lanes = 16 * g + HALO * k
            planes[k, at, :] = jnp.where(
                from_left,
                turn(a, -lanes),
                jnp.where(from_right, turn(b, RIGHT + SEAM - lanes), base[k, at, :]),
            )

    def put(i, t, value):
        hidden = outside
        if t == 0:
            hidden = hidden | (row == 0)
        if t == TILES + 1:
            hidden = hidden | (row == 31)
        w[i, pl.ds(TOP - 8 + 8 * t, 8), :] = jnp.where(hidden, 0.0, value)

    for t in range(TILES + 2):
        start = TOP - 8 + 8 * t
        total = jnp.zeros((8, LANES), f32)
        picked = planes[K, pl.ds(start, 8), :]
        for k in range(K):
            x = planes[k, pl.ds(start, 8), :]
            vertical = planes[k, pl.ds(start + 1, 8), :] + planes[k, pl.ds(start - 1, 8), :]
            term = 4.0 * x - (vertical + turn(x, -1) + turn(x, 1))
            total = jnp.where(picked == k, term, total)
        put(0, t, total)
    for i in range(2):
        for t in range(TILES + 2):
            start = TOP - 8 + 8 * t
            x = w[i, pl.ds(start, 8), :]
            vertical = w[i, pl.ds(start + 1, 8), :] + w[i, pl.ds(start - 1, 8), :]
            put(i + 1, t, vertical + turn(x, -1) + turn(x, 1))
    own_lane = window(lane, LEFT, HALO) | window(lane, RIGHT + SEAM - HALO, HALO)
    found = [[] for _ in PAIRS]
    for t in range(TILES):
        start = TOP + 8 * t
        x = [w[i, pl.ds(start, 8), :] for i in range(3)]
        x.append(w[2, pl.ds(start + 1, 8), :] + turn(x[2], -1))
        for i, (a, b) in enumerate(PAIRS):
            found[i].append(x[a] * x[b])
    totals = [totals_in[i] + jnp.where(own_lane, tree(found[i]), 0.0) for i in range(6)]

    line = jnp.zeros((8, LANES), f32)
    for i in range(6):
        x = totals[i] + totals[i] if i == 5 else totals[i]
        big = 512.0 * jnp.max(jnp.abs(x), axis=1, keepdims=True)
        high = (x + big) - big
        line = jnp.where(
            (lane == i) | (lane == i + 16),
            jnp.sum(high, axis=1, keepdims=True),
            jnp.where(lane == i + 8, jnp.sum(x - high, axis=1, keepdims=True), line),
        )
    s, e = line, jnp.zeros_like(line)
    for shift in (4, 2, 1):
        s, more = two_sum(s, pltpu.roll(s, shift, 0))
        e = e + pltpu.roll(e, shift, 0) + more
    line = jnp.where(lane < 16, s, e)[:1].reshape(1, 1, LANES)
    sums_out[...] = jnp.broadcast_to(line, (256, 1, LANES))


def seam(base, totals, c_even, c_odd):
    return pl.pallas_call(
        seam_kernel,
        out_shape=(near((3, ROWS, LANES)), near((256, 1, LANES))),
        in_specs=[WHOLE] * 4,
        out_specs=(WHOLE,) * 2,
        scratch_shapes=[pltpu.VMEM((K + 1, ROWS, LANES), f32)],
        compiler_params=LIMIT,
        cost_estimate=cost(1),
        name="seam_fields",
    )(*held(base, totals, c_even, c_odd))


def pool_kernel(v0, v1, v2, out):
    spread = jnp.where(iota((512, LANES), 0) // 4 == iota((512, LANES), 1), f32(0.0625), f32(0.0))
    for i, ref in enumerate((v0, v1, v2)):
        for g in range(2):
            parts = []
            for j in range(4):
                at = [ref[4 * g + j, pl.ds(TOP + q, H // 4, stride=4), :] for q in range(4)]
                parts.append((at[0] + at[1]) + (at[2] + at[3]))
            out[i, g] = sums_of(jnp.concatenate(parts, 1), spread.astype(jnp.bfloat16))


def pool(v0, v1, v2):
    return pl.pallas_call(
        pool_kernel,
        out_shape=near((3, 2, H // 4, LANES)),
        in_specs=[WHOLE] * 3,
        out_specs=WHOLE,
        compiler_params=LIMIT,
        cost_estimate=cost(1),
        name="pool_fields",
    )(*held(v0, v1, v2))


def two_product(a, b):
    p = a * b
    big = f32(4097.0)
    t = big * a
    ah = t - (t - a)
    al = a - ah
    t = big * b
    bh = t - (t - b)
    bl = b - bh
    return p, ((ah * bh - p) + ah * bl + al * bh) + al * bl


def less_scaled(a, b, scale):
    p, low = two_product(b[0], scale)
    low = low + b[1] * scale
    s, e = two_sum(a[0], -p)
    e = e + (a[1] - low)
    return two_sum(s, e)


def coefficients(n):
    shift = n[1][0] / n[0][0]
    current = n
    m = [n[0][0]]
    for _ in range(5):
        current = [less_scaled(current[i + 1], current[i], shift) for i in range(len(current) - 1)]
        m.append(current[0][0] + current[0][1])
    m0, m1, m2, m3, m4, m5 = m
    t = m1 / m0
    theta0 = shift + t
    m5 = m5 - 5.0 * t * m4
    m4 = m4 - 4.0 * t * m3
    m3 = m3 - 3.0 * t * m2
    m2 = m2 - t * m1
    one = jnp.ones_like(m0)
    zero = jnp.zeros_like(m0)
    second = m2 > 0.0
    safe2 = jnp.where(second, m2, one)
    b1 = jnp.where(second, m2 / m0, zero)
    s = jnp.where(second, m3 / safe2, zero)
    h2 = m4 - s * m3 - b1 * m2
    third = second & (h2 > 0.0)
    safe3 = jnp.where(third, h2, one)
    theta1 = jnp.clip(theta0 + s, -4.0, 4.0)
    theta2 = jnp.clip(theta0 - s + (m5 - s * m4 - b1 * m3) / safe3, -4.0, 4.0)
    b2 = h2 / safe2
    d0, d1, d2 = 4.0 - theta0, 4.0 - theta1, 4.0 - theta2
    e = d1 * d2 - b2
    two, three = d0 * d1 - b1, d0 * e - b1 * d2
    second = second & (two > 0.0)
    third = second & third & (three > 0.0)
    y2 = jnp.where(third, one / three, zero)
    y1 = jnp.where(third, d2 * y2, jnp.where(second, one / two, zero))
    y0 = jnp.where(third, e * y2, jnp.where(second, d1 * y1, one / d0))
    return (
        y0 - theta0 * y1 + (theta0 * theta1 - b1) * y2,
        y1 - (theta0 + theta1) * y2,
        y2,
    )


def solve_kernel(all_sums, pooled, w, coef_out, mid_out):
    frm, to = iota((LANES, LANES), 0), iota((LANES, LANES), 1)
    first = window(frm, LEFT, HALO) & (to == 0)
    final = window(frm, RIGHT + SEAM - HALO, HALO) & (to == LANES - 1)
    rows = []
    for i in range(3):
        at = [w[i, pl.ds(TOP + q, H // 4, stride=4), :] for q in range(4)]
        rows.append((at[0] + at[1]) + (at[2] + at[3]))
    weights = jnp.where(first | final, f32(0.0625), f32(0.0)).astype(jnp.bfloat16)
    edges = sums_of(jnp.concatenate(rows, 0), weights)
    tiles = [(all_sums[pl.ds(8 * i, 8), :], jnp.zeros((8, LANES), f32)) for i in range(32)]
    while len(tiles) > 1:
        merged = []
        for a, b in zip(tiles[0::2], tiles[1::2]):
            s, e = two_sum(a[0], b[0])
            merged.append((s, e + (a[1] + b[1])))
        tiles = merged
    s, e = tiles[0]
    for shift in (4, 2, 1):
        s, more = two_sum(s, pltpu.roll(s, shift, 0))
        e = e + pltpu.roll(e, shift, 0) + more
    lane = iota((8, LANES), 1)
    zero = jnp.zeros((8, LANES), f32)

    def over_lanes(x):
        return jnp.broadcast_to(jnp.sum(x, axis=1, keepdims=True), (8, LANES))

    n = []
    for i in range(6):
        high = over_lanes(jnp.where(lane == i, s, zero))
        low = over_lanes(jnp.where((lane == i + 8) | (lane == i + 16), s, jnp.where(lane == i, e, zero)))
        n.append(two_sum(high, low))
    c = coefficients(n)
    for i in range(3):
        coef_out[i] = c[i]
    for g in range(2):
        edge = lane == (LANES - 1 if g else 0)
        for q in range(H // 4 // 8):
            at = (g, pl.ds(8 * q, 8), slice(None))
            value = zero
            for i in range(3):
                start = H // 4 * i + 8 * q
                value = value + c[i] * jnp.where(edge, edges[start : start + 8], pooled[(i, *at)])
            for d in range(16):
                mid_out[(d, *at)] = value


def solve(all_sums, pooled, w):
    return pl.pallas_call(
        solve_kernel,
        out_shape=(near((3, 8, LANES)), near((16, 2, H // 4, LANES))),
        in_specs=[WHOLE] * 3,
        out_specs=(WHOLE,) * 2,
        compiler_params=LIMIT,
        cost_estimate=cost(1),
        name="coefficients",
    )(*held(all_sums, pooled, w))


def half_matrix(rows):
    return jnp.where(iota((rows, rows // 2), 0) // 2 == iota((rows, rows // 2), 1), f32(0.25), f32(0.0))


def pooled_rows(parts):
    return sums_of(jnp.concatenate(parts, 1), half_matrix(2 * LANES).astype(jnp.bfloat16))


def store_mid(x, core, mid_out, sem):
    copies = []
    for g in range(2):
        to = mid_out.at[:, core, :, pl.ds(g * LANES, LANES)]
        copies.append(pltpu.make_async_copy(x.at[:, g], to, sem.at[g]))
        copies[-1].start()
    return copies


def store_coarse(x, core, coarse_out, scratch, sem):
    rows = H // 8
    parts = [
        jnp.concatenate(
            [x[d, g, pl.ds(0, rows, stride=2), :] + x[d, g, pl.ds(1, rows, stride=2), :] for d in range(16)], 0
        )
        for g in range(2)
    ]
    pooled = pooled_rows(parts)
    for d in range(16):
        scratch[d] = pooled[d * rows : (d + 1) * rows]
    copy = pltpu.make_async_copy(scratch, coarse_out.at[:, core], sem)
    copy.start()
    return copy


def own_kernel(
    x, coef, v0, v1, v2, w, blended_out, fine_out, mid_out, coarse_out, flat, stacked, fine, coarse, sem
):
    core = lax.axis_index("row_2")
    copies = store_mid(x, core, mid_out, sem)
    c = [coef[i] for i in range(3)]
    lane = iota((8, LANES), 1)
    parts = 4
    for p in range(parts):
        for u in range(TILES // parts):
            base = 8 * (p * (TILES // parts) + u)
            rows = pl.ds(base + TOP, 8)
            seams = c[0] * w[0, rows, :] + c[1] * w[1, rows, :] + c[2] * w[2, rows, :]
            for j in range(BLOCKS):
                at = (j, rows, slice(None))
                value = c[0] * v0[at] + c[1] * v1[at] + c[2] * v2[at]
                if j == 0:
                    value = jnp.where(lane < HALO, turn(seams, -LEFT), value)
                if j == BLOCKS - 1:
                    value = jnp.where(lane >= LANES - HALO, turn(seams, LANES - RIGHT - SEAM), value)
                flat[pl.ds(base, 8), pl.ds(j * LANES, LANES)] = value
                stacked[j, pl.ds(base, 8), :] = value
        rows = pl.ds(p * H // parts, H // parts)
        copies.append(pltpu.make_async_copy(flat.at[rows, :], blended_out.at[rows, :], sem.at[3 + p]))
        copies[-1].start()
    for g in range(BLOCKS // 2):
        halves = [
            stacked[2 * g + i, pl.ds(0, H // 2, stride=2), :] + stacked[2 * g + i, pl.ds(1, H // 2, stride=2), :]
            for i in range(2)
        ]
        fine[:, pl.ds(g * LANES, LANES)] = pooled_rows(halves)
    copies.append(pltpu.make_async_copy(fine, fine_out, sem.at[3 + parts]))
    copies[-1].start()
    copies.append(store_coarse(x, core, coarse_out, coarse, sem.at[2]))
    for copy in copies:
        copy.wait()


LEVELS = (
    jax.ShapeDtypeStruct((16, 2, H // 4, W // 4), f32),
    jax.ShapeDtypeStruct((16, 2, H // 8, W // 8), f32),
)


def own_levels(x, coef, v0, v1, v2, w):
    return pl.pallas_call(
        own_kernel,
        out_shape=(
            jax.ShapeDtypeStruct((H, W), f32),
            jax.ShapeDtypeStruct((H // 2, W // 2), f32),
            *LEVELS,
        ),
        in_specs=[WHOLE] * 6,
        out_specs=(FAR,) * 4,
        scratch_shapes=[
            pltpu.VMEM((H, W), f32),
            pltpu.VMEM((BLOCKS, H, LANES), f32),
            pltpu.VMEM((H // 2, W // 2), f32),
            pltpu.VMEM((16, H // 8, LANES), f32),
            pltpu.SemaphoreType.DMA((8,)),
        ],
        compiler_params=LIMIT,
        cost_estimate=cost(2),
        name="own_levels",
    )(*held(x, coef, v0, v1, v2, w))


def other_kernel(x, mid_in, coarse_in, mid_out, coarse_out, coarse, sem):
    del mid_in, coarse_in
    core = 1 - lax.axis_index("row_2")
    copies = store_mid(x, core, mid_out, sem)
    copies.append(store_coarse(x, core, coarse_out, coarse, sem.at[2]))
    for copy in copies:
        copy.wait()


def other_levels(x, mid, coarse):
    return pl.pallas_call(
        other_kernel,
        out_shape=LEVELS,
        in_specs=[WHOLE, FAR, FAR],
        out_specs=(FAR,) * 2,
        scratch_shapes=[
            pltpu.VMEM((16, H // 8, LANES), f32),
            pltpu.SemaphoreType.DMA((3,)),
        ],
        input_output_aliases={1: 0, 2: 1},
        compiler_params=LIMIT,
        cost_estimate=cost(1),
        name="other_levels",
    )(*held(x), *far(mid, coarse))


def swaps(devices, first):
    pairs = [(i, i + 1) for i in range(first, devices - 1, 2)]
    return pairs + [(b, a) for a, b in pairs]


def exchange(even, odd, axis):
    devices = lax.axis_size(axis)
    odd = lax.ppermute(odd, axis, swaps(devices, 1))
    even = lax.ppermute(even, axis, swaps(devices, 0))
    return even, odd


def per_device(sources, labels):
    even, odd = pack_rows(sources, labels)
    even, odd, planes, marks = lax.optimization_barrier((even, odd, sources, labels))
    r_even, r_odd = exchange(even, odd, ROW)
    ext, lext, left, right, v0, v1, v2, totals, base = load(planes, marks)
    c_even, c_odd = exchange(*pack_columns(r_even, r_odd, left, right), "col")
    v0, v1, v2, base, totals = inner(ext, lext, v0, v1, v2, base, r_even, r_odd, totals)
    pooled, totals = lax.optimization_barrier((pool(v0, v1, v2), totals))
    w, sums = seam(base, totals, c_even, c_odd)
    sums = lax.all_to_all(sums, ALL, split_axis=0, concat_axis=0, tiled=True)
    coef, mid = solve(sums.reshape(256, LANES), pooled, w)
    mid = lax.all_to_all(mid, CHIP, split_axis=0, concat_axis=0, tiled=True)
    other = lax.ppermute(mid, "row_2", [(0, 1), (1, 0)])
    blended, fine, overview_mid, overview_coarse = own_levels(mid, coef, v0, v1, v2, w)
    overview_mid, overview_coarse = other_levels(other, overview_mid, overview_coarse)
    overview_mid = overview_mid.reshape(8 * H, W // 4)
    overview_coarse = overview_coarse.reshape(4 * H, W // 8)
    return (blended, fine, overview_mid, overview_coarse)


def solution(mesh):
    finer = Mesh(
        mesh.devices.reshape(4, 4, 2, mesh.shape["col"]), ("row_0", "row_1", "row_2", "col")
    )
    return jax.shard_map(
        per_device,
        mesh=finer,
        in_specs=(P(None, ROW, "col"), P(ROW, "col")),
        out_specs=(P(ROW, "col"), P(ROW, "col"), P(None, "col"), P(None, "col")),
        check_vma=False,
    )
```

```python
import jax
import jax.numpy as jnp
from jax import lax
from jax.experimental import pallas as pl
from jax.experimental.pallas import tpu as pltpu
from jax.sharding import Mesh
from jax.sharding import PartitionSpec as P


K = 3
H, W = 128, 1024
TOP = 16
ROWS = TOP + H + 24
LANES = 128
BLOCKS = W // LANES
HALO = 4
ROW = ("row_0", "row_1", "row_2")
CHIP = ("row_0", "row_1")
ALL = ("row_0", "row_1", "row_2", "col")
VMEM = pltpu.MemorySpace.VMEM
WHOLE = pl.BlockSpec(memory_space=VMEM)
FAR = pl.BlockSpec(memory_space=pltpu.MemorySpace.HBM)
LIMIT = pltpu.CompilerParams(vmem_limit_bytes=24 * 2**20)
TILES = H // 8
LEFT, RIGHT = HALO, 64
SEAM = 12
f32 = jnp.float32


def iota(shape, dim):
    return lax.broadcasted_iota(jnp.int32, shape, dim)


def place():
    row = (lax.axis_index("row_0") * 4 + lax.axis_index("row_1")) * 2 + lax.axis_index("row_2")
    return row, lax.axis_index("col")


def near(shape, dtype=f32):
    return pltpu.VMEM(shape, dtype)


def held(*values):
    return [pltpu.with_memory_space_constraint(v, VMEM) for v in values]


def far(*values):
    return [pltpu.with_memory_space_constraint(v, pltpu.MemorySpace.HBM) for v in values]


def cost(us):
    return pl.CostEstimate(flops=int(us * 3e8), bytes_accessed=0, transcendentals=0)


def sums_of(x, weights):
    total = None
    for _ in range(3):
        part = x.astype(jnp.bfloat16)
        x = x - part.astype(f32)
        term = jnp.dot(part, weights, preferred_element_type=f32)
        total = term if total is None else total + term
    return total


def pack_kernel(src, lab, even_out, odd_out, rows, lrows, sem):
    copies = []
    for side, start in ((0, 0), (1, H - 8)):
        for i, (a, b) in enumerate(
            (
                (src.at[:, pl.ds(start, 8), :], rows.at[side]),
                (lab.at[pl.ds(start, 8), :], lrows.at[side]),
            )
        ):
            c = pltpu.make_async_copy(a, b, sem.at[side, i])
            c.start()
            copies.append(c)
    for c in copies:
        c.wait()
    row, _ = place()
    even = (row % 2) == 0
    upper = iota((8, W), 0) < HALO

    def sides(side):
        a = [rows[side, k] for k in range(K)] + [lrows[side].astype(f32)]
        pairs = []
        for x, y in ((a[0], a[1]), (a[2], a[3])):
            if side == 0:
                pairs.append(jnp.where(upper, x, pltpu.roll(y, HALO, 0)))
            else:
                pairs.append(jnp.where(upper, pltpu.roll(x, HALO, 0), y))
        return pairs

    top, bottom = sides(0), sides(1)
    for i in range(2):
        even_out[pl.ds(8 * i, 8), :] = jnp.where(even, bottom[i], top[i])
        odd_out[pl.ds(8 * i, 8), :] = jnp.where(even, top[i], bottom[i])


def pack_rows(sources, labels):
    return pl.pallas_call(
        pack_kernel,
        out_shape=(near((16, W)), near((16, W))),
        in_specs=[FAR] * 2,
        out_specs=(WHOLE,) * 2,
        scratch_shapes=[
            pltpu.VMEM((2, K, 8, W), f32),
            pltpu.VMEM((2, 8, W), jnp.int32),
            pltpu.SemaphoreType.DMA((2, 2)),
        ],
        compiler_params=LIMIT,
        cost_estimate=cost(1),
        name="pack_rows",
    )(*far(sources, labels))


def window(lane, start, size):
    return (lane >= start) & (lane < start + size)


def turn(x, shift):
    shift %= LANES
    return pltpu.roll(x, shift, 1) if shift else x


def load_kernel(
    src, lab, ext, lext, left_out, right_out, v0, v1, v2, totals_out, seam_out
):
    own = pl.ds(TOP, H)
    for j in (0, BLOCKS - 1, *range(1, BLOCKS - 1)):
        lanes = pl.ds(j * LANES, LANES)
        for k in range(K):
            ext[k, j, own, :] = src[k, :, lanes]
        lext[j, own, :] = lab[:, lanes]
    lane = iota((8, LANES), 1)
    for j, out, first in ((0, left_out, 0), (BLOCKS - 1, right_out, LANES - HALO)):
        for half in range(2):
            total = jnp.zeros((8, LANES), f32)
            for g in range(8):
                at = pl.ds(TOP + 64 * half + 8 * g, 8)
                for k in range(K + 1):
                    x = ext[k, j, at, :] if k < K else lext[j, at, :].astype(f32)
                    to = 16 * g + HALO * k
                    total = jnp.where(window(lane, to, HALO), turn(x, to - first), total)
            out[pl.ds(8 * half, 8), :] = total

    over_tiles(1, TILES - 2, 7, lambda base, c: (right_side(ext, lext, v0, base), c)[1], 0)
    over_tiles(2, TILES - 3, 6, lambda base, c: (neighbours(v0, v1, base), c)[1], 0)
    over_tiles(3, TILES - 4, 5, lambda base, c: (neighbours(v1, v2, base), c)[1], 0)
    zero = jnp.zeros((8, LANES), f32)
    totals = over_tiles(3, TILES - 5, 3, lambda base, c: products(v0, v1, v2, base, c), (zero,) * 6)
    for i in range(6):
        totals_out[i] = totals[i]
    for tile in range(TILES):
        seam_base(ext, lext, seam_out, tile)


def load(sources, labels):
    field = near((BLOCKS, ROWS, LANES))
    return pl.pallas_call(
        load_kernel,
        out_shape=(
            near((K, BLOCKS, ROWS, LANES)),
            near((BLOCKS, ROWS, LANES), jnp.int32),
            near((16, LANES)),
            near((16, LANES)),
            field,
            field,
            field,
            near((6, 8, LANES)),
            near((K + 1, ROWS, LANES)),
        ),
        in_specs=[WHOLE] * 2,
        out_specs=(WHOLE,) * 9,
        compiler_params=LIMIT,
        cost_estimate=cost(3),
        name="load_block",
    )(*held(sources, labels))


def corner_kernel(got_even, got_odd, left, right, even_out, odd_out):
    row, col = place()
    row_even = (row % 2) == 0
    col_even = (col % 2) == 0
    upper = iota((8, LANES), 0) < HALO
    lane = iota((8, LANES), 1)
    strips = []
    for start, first in ((0, 0), (W - LANES, LANES - HALO)):
        total = jnp.zeros((8, LANES), f32)
        for k in range(K + 1):
            tile, half = divmod(k, 2)
            at = (pl.ds(8 * tile, 8), pl.ds(start, LANES))
            e, o = got_even[at], got_odd[at]
            above = jnp.where(row_even, o, e)
            below = jnp.where(row_even, e, o)
            if half:
                both = jnp.where(upper, pltpu.roll(above, HALO, 0), below)
            else:
                both = jnp.where(upper, above, pltpu.roll(below, HALO, 0))
            total = jnp.where(window(lane, HALO * k, HALO), turn(both, HALO * k - first), total)
        strips.append(total)
    even_out[pl.ds(0, 16), :] = jnp.where(col_even, right[...], left[...])
    odd_out[pl.ds(0, 16), :] = jnp.where(col_even, left[...], right[...])
    even_out[pl.ds(16, 8), :] = jnp.where(col_even, strips[1], strips[0])
    odd_out[pl.ds(16, 8), :] = jnp.where(col_even, strips[0], strips[1])


def pack_columns(got_even, got_odd, left, right):
    return pl.pallas_call(
        corner_kernel,
        out_shape=(near((24, LANES)),) * 2,
        in_specs=[WHOLE] * 4,
        out_specs=(WHOLE,) * 2,
        compiler_params=LIMIT,
        cost_estimate=cost(0.5),
        name="pack_columns",
    )(*held(got_even, got_odd, left, right))


def two_sum(a, b):
    s = a + b
    t = s - a
    return s, (a - (s - t)) + (b - t)


def shifted(tiles):
    lane = iota((8, LANES), 1)
    to_left = [pltpu.roll(t, LANES - 1, 1) for t in tiles]
    to_right = [pltpu.roll(t, 1, 1) for t in tiles]
    last, first = lane == LANES - 1, lane == 0
    n = len(tiles)
    after = [jnp.where(last, to_left[min(j + 1, n - 1)], to_left[j]) for j in range(n)]
    before = [jnp.where(first, to_right[max(j - 1, 0)], to_right[j]) for j in range(n)]
    return after, before


PAIRS = ((0, 0), (0, 1), (1, 1), (1, 2), (2, 2), (2, 3))


def right_side(ext, lext, out, base):
    at = pl.ds(base, 8)
    picked = [lext[j, at, :] for j in range(BLOCKS)]
    center, around = [None] * BLOCKS, [None] * BLOCKS
    for k in range(K):
        tiles = [ext[k, j, at, :] for j in range(BLOCKS)]
        after, before = shifted(tiles)
        for j in range(BLOCKS):
            near_sum = ext[k, j, pl.ds(base + 1, 8), :] + ext[k, j, pl.ds(base - 1, 8), :]
            near_sum = near_sum + after[j] + before[j]
            here = picked[j] == k
            center[j] = jnp.where(here, tiles[j], center[j]) if k else tiles[j]
            around[j] = jnp.where(here, near_sum, around[j]) if k else near_sum
    for j in range(BLOCKS):
        out[j, at, :] = 4.0 * center[j] - around[j]


def neighbours(source, target, base):
    tiles = [source[j, pl.ds(base, 8), :] for j in range(BLOCKS)]
    after, before = shifted(tiles)
    for j in range(BLOCKS):
        vertical = source[j, pl.ds(base + 1, 8), :] + source[j, pl.ds(base - 1, 8), :]
        target[j, pl.ds(base, 8), :] = vertical + after[j] + before[j]


def over_tiles(first, last, chunk, step, carry):
    def turn_of(t, carry):
        for u in range(chunk):
            carry = step(pl.multiple_of(TOP + 8 * first + 8 * (chunk * t + u), 8), carry)
        return carry

    return lax.fori_loop(0, (last - first + 1) // chunk, turn_of, carry)


def tree(x):
    while len(x) > 1:
        x = [sum(x[a : a + 2][1:], x[a]) for a in range(0, len(x), 2)]
    return x[0]


def products(v0, v1, v2, base, totals):
    lane = iota((8, LANES), 1)
    last = lane == LANES - 1
    kept = {0: lane >= HALO, BLOCKS - 1: lane < LANES - HALO}
    at = pl.ds(base, 8)
    found = [[] for _ in PAIRS]
    rolled = [turn(v2[j, at, :], -1) for j in range(BLOCKS)]
    for j in range(BLOCKS):
        x = [v[j, at, :] for v in (v0, v1, v2)]
        right = jnp.where(last, rolled[min(j + 1, BLOCKS - 1)], rolled[j])
        x.append(v2[j, pl.ds(base + 1, 8), :] + right)
        own = [jnp.where(kept[j], a, 0.0) for a in x[:3]] if j in kept else x
        for i, (a, b) in enumerate(PAIRS):
            found[i].append(own[a] * x[b])
    return tuple(total + tree(f) for total, f in zip(totals, found))


def seam_base(ext, lext, out, tile):
    lane = iota((8, LANES), 1)
    at = pl.ds(TOP + 8 * tile, 8)
    for k in range(K + 1):
        a, b = [ext[k, j, at, :] if k < K else lext[j, at, :].astype(f32) for j in (0, BLOCKS - 1)]
        out[k, at, :] = jnp.where(lane < 64, turn(a, LEFT), turn(b, RIGHT + SEAM))


def clear_rows(ref, row):
    @pl.when(row == 0)
    def _():
        for j in range(BLOCKS):
            ref[j, pl.ds(TOP - 8, 8), :] = jnp.zeros((8, LANES), f32)

    @pl.when(row == 31)
    def _():
        for j in range(BLOCKS):
            ref[j, pl.ds(TOP + H, 8), :] = jnp.zeros((8, LANES), f32)


def inner_kernel(*refs):
    r_even, r_odd, totals_in = refs[6:9]
    ext, lext, v0, v1, v2, seam_out, totals_out = refs[9:]
    row, _ = place()
    row_even = (row % 2) == 0
    for k in range(K + 1):
        at = pl.ds(HALO * k, HALO)
        for j in range(BLOCKS):
            lanes = pl.ds(j * LANES, LANES)
            e, o = r_even[at, lanes], r_odd[at, lanes]
            above, below = jnp.where(row_even, o, e), jnp.where(row_even, e, o)
            for start, value in ((TOP - HALO, above), (TOP + H, below)):
                if k < K:
                    ext[k, j, pl.ds(start, HALO), :] = value
                else:
                    lext[j, pl.ds(start, HALO), :] = value.astype(jnp.int32)
    seam_base(ext, lext, seam_out, -1)
    seam_base(ext, lext, seam_out, TILES)
    for t in (-1, 0, TILES - 1, TILES):
        right_side(ext, lext, v0, TOP + 8 * t)
    clear_rows(v0, row)
    for t in (-1, 0, 1, TILES - 2, TILES - 1, TILES):
        neighbours(v0, v1, TOP + 8 * t)
    clear_rows(v1, row)
    for t in (-1, 0, 1, 2, TILES - 3, TILES - 2, TILES - 1, TILES):
        neighbours(v1, v2, TOP + 8 * t)
    clear_rows(v2, row)
    totals = tuple(totals_in[i] for i in range(6))
    for t in (0, 1, 2, *range(TILES - 4, TILES)):
        totals = products(v0, v1, v2, TOP + 8 * t, totals)
    for i in range(6):
        totals_out[i] = totals[i]


def inner(ext, lext, v0, v1, v2, base, r_even, r_odd, totals):
    field = near((BLOCKS, ROWS, LANES))
    return pl.pallas_call(
        inner_kernel,
        out_shape=(
            near((K, BLOCKS, ROWS, LANES)),
            near((BLOCKS, ROWS, LANES), jnp.int32),
            field,
            field,
            field,
            near((K + 1, ROWS, LANES)),
            near((6, 8, LANES)),
        ),
        in_specs=[WHOLE] * 9,
        out_specs=(WHOLE,) * 7,
        input_output_aliases={i: i for i in range(6)},
        compiler_params=LIMIT,
        cost_estimate=cost(2),
        name="inner_fields",
    )(*held(ext, lext, v0, v1, v2, base, r_even, r_odd, totals))[2:]


def seam_kernel(base, totals_in, c_even, c_odd, w, sums_out, planes):
    row, col = place()
    col_even = (col % 2) == 0
    lane = iota((8, LANES), 1)
    from_left, from_right = lane < LEFT, window(lane, RIGHT + SEAM, HALO)
    outside = (from_left & (col == 0)) | (from_right & (col == 7))
    for t in range(TILES + 2):
        at = pl.ds(TOP - 8 + 8 * t, 8)
        corner = t in (0, TILES + 1)
        tile, g = (2, 0) if corner else divmod(t - 1, 8)
        e, o = c_even[pl.ds(8 * tile, 8), :], c_odd[pl.ds(8 * tile, 8), :]
        a, b = jnp.where(col_even, o, e), jnp.where(col_even, e, o)
        if corner:
            a, b = pltpu.roll(a, HALO, 0), pltpu.roll(b, HALO, 0)
        for k in range(K + 1):
            lanes = 16 * g + HALO * k
            planes[k, at, :] = jnp.where(
                from_left,
                turn(a, -lanes),
                jnp.where(from_right, turn(b, RIGHT + SEAM - lanes), base[k, at, :]),
            )

    def put(i, t, value):
        hidden = outside
        if t == 0:
            hidden = hidden | (row == 0)
        if t == TILES + 1:
            hidden = hidden | (row == 31)
        w[i, pl.ds(TOP - 8 + 8 * t, 8), :] = jnp.where(hidden, 0.0, value)

    for t in range(TILES + 2):
        start = TOP - 8 + 8 * t
        total = jnp.zeros((8, LANES), f32)
        picked = planes[K, pl.ds(start, 8), :]
        for k in range(K):
            x = planes[k, pl.ds(start, 8), :]
            vertical = planes[k, pl.ds(start + 1, 8), :] + planes[k, pl.ds(start - 1, 8), :]
            term = 4.0 * x - (vertical + turn(x, -1) + turn(x, 1))
            total = jnp.where(picked == k, term, total)
        put(0, t, total)
    for i in range(2):
        for t in range(TILES + 2):
            start = TOP - 8 + 8 * t
            x = w[i, pl.ds(start, 8), :]
            vertical = w[i, pl.ds(start + 1, 8), :] + w[i, pl.ds(start - 1, 8), :]
            put(i + 1, t, vertical + turn(x, -1) + turn(x, 1))
    own_lane = window(lane, LEFT, HALO) | window(lane, RIGHT + SEAM - HALO, HALO)
    found = [[] for _ in PAIRS]
    for t in range(TILES):
        start = TOP + 8 * t
        x = [w[i, pl.ds(start, 8), :] for i in range(3)]
        x.append(w[2, pl.ds(start + 1, 8), :] + turn(x[2], -1))
        for i, (a, b) in enumerate(PAIRS):
            found[i].append(x[a] * x[b])
    totals = [totals_in[i] + jnp.where(own_lane, tree(found[i]), 0.0) for i in range(6)]

    line = jnp.zeros((8, LANES), f32)
    for i in range(6):
        x = totals[i] + totals[i] if i == 5 else totals[i]
        big = 512.0 * jnp.max(jnp.abs(x), axis=1, keepdims=True)
        high = (x + big) - big
        line = jnp.where(
            (lane == i) | (lane == i + 16),
            jnp.sum(high, axis=1, keepdims=True),
            jnp.where(lane == i + 8, jnp.sum(x - high, axis=1, keepdims=True), line),
        )
    s, e = line, jnp.zeros_like(line)
    for shift in (4, 2, 1):
        s, more = two_sum(s, pltpu.roll(s, shift, 0))
        e = e + pltpu.roll(e, shift, 0) + more
    line = jnp.where(lane < 16, s, e)
    for i in range(32):
        sums_out[pl.ds(8 * i, 8), :] = line


def seam(base, totals, c_even, c_odd):
    return pl.pallas_call(
        seam_kernel,
        out_shape=(near((3, ROWS, LANES)), near((256, LANES))),
        in_specs=[WHOLE] * 4,
        out_specs=(WHOLE,) * 2,
        scratch_shapes=[pltpu.VMEM((K + 1, ROWS, LANES), f32)],
        compiler_params=LIMIT,
        cost_estimate=cost(1),
        name="seam_fields",
    )(*held(base, totals, c_even, c_odd))


def pool_kernel(v0, v1, v2, out):
    spread = jnp.where(iota((512, LANES), 0) // 4 == iota((512, LANES), 1), f32(0.0625), f32(0.0))
    for i, ref in enumerate((v0, v1, v2)):
        for g in range(2):
            parts = []
            for j in range(4):
                at = [ref[4 * g + j, pl.ds(TOP + q, H // 4, stride=4), :] for q in range(4)]
                parts.append((at[0] + at[1]) + (at[2] + at[3]))
            out[i, g] = sums_of(jnp.concatenate(parts, 1), spread.astype(jnp.bfloat16))


def pool(v0, v1, v2):
    return pl.pallas_call(
        pool_kernel,
        out_shape=near((3, 2, H // 4, LANES)),
        in_specs=[WHOLE] * 3,
        out_specs=WHOLE,
        compiler_params=LIMIT,
        cost_estimate=cost(1),
        name="pool_fields",
    )(*held(v0, v1, v2))


def two_product(a, b):
    p = a * b
    big = f32(4097.0)
    t = big * a
    ah = t - (t - a)
    al = a - ah
    t = big * b
    bh = t - (t - b)
    bl = b - bh
    return p, ((ah * bh - p) + ah * bl + al * bh) + al * bl


def less_scaled(a, b, scale):
    p, low = two_product(b[0], scale)
    low = low + b[1] * scale
    s, e = two_sum(a[0], -p)
    e = e + (a[1] - low)
    return two_sum(s, e)


def coefficients(n):
    shift = n[1][0] / n[0][0]
    current = n
    m = [n[0][0]]
    for _ in range(5):
        current = [less_scaled(current[i + 1], current[i], shift) for i in range(len(current) - 1)]
        m.append(current[0][0] + current[0][1])
    m0, m1, m2, m3, m4, m5 = m
    t = m1 / m0
    theta0 = shift + t
    m5 = m5 - 5.0 * t * m4
    m4 = m4 - 4.0 * t * m3
    m3 = m3 - 3.0 * t * m2
    m2 = m2 - t * m1
    one = jnp.ones_like(m0)
    zero = jnp.zeros_like(m0)
    second = m2 > 0.0
    safe2 = jnp.where(second, m2, one)
    b1 = jnp.where(second, m2 / m0, zero)
    s = jnp.where(second, m3 / safe2, zero)
    h2 = m4 - s * m3 - b1 * m2
    third = second & (h2 > 0.0)
    safe3 = jnp.where(third, h2, one)
    theta1 = jnp.clip(theta0 + s, -4.0, 4.0)
    theta2 = jnp.clip(theta0 - s + (m5 - s * m4 - b1 * m3) / safe3, -4.0, 4.0)
    b2 = h2 / safe2
    d0, d1, d2 = 4.0 - theta0, 4.0 - theta1, 4.0 - theta2
    e = d1 * d2 - b2
    two, three = d0 * d1 - b1, d0 * e - b1 * d2
    second = second & (two > 0.0)
    third = second & third & (three > 0.0)
    y2 = jnp.where(third, one / three, zero)
    y1 = jnp.where(third, d2 * y2, jnp.where(second, one / two, zero))
    y0 = jnp.where(third, e * y2, jnp.where(second, d1 * y1, one / d0))
    return (
        y0 - theta0 * y1 + (theta0 * theta1 - b1) * y2,
        y1 - (theta0 + theta1) * y2,
        y2,
    )


def solve_kernel(all_sums, pooled, w, coef_out, mid_out):
    frm, to = iota((LANES, LANES), 0), iota((LANES, LANES), 1)
    first = window(frm, LEFT, HALO) & (to == 0)
    final = window(frm, RIGHT + SEAM - HALO, HALO) & (to == LANES - 1)
    rows = []
    for i in range(3):
        at = [w[i, pl.ds(TOP + q, H // 4, stride=4), :] for q in range(4)]
        rows.append((at[0] + at[1]) + (at[2] + at[3]))
    weights = jnp.where(first | final, f32(0.0625), f32(0.0)).astype(jnp.bfloat16)
    edges = sums_of(jnp.concatenate(rows, 0), weights)
    tiles = [(all_sums[pl.ds(8 * i, 8), :], jnp.zeros((8, LANES), f32)) for i in range(32)]
    while len(tiles) > 1:
        merged = []
        for a, b in zip(tiles[0::2], tiles[1::2]):
            s, e = two_sum(a[0], b[0])
            merged.append((s, e + (a[1] + b[1])))
        tiles = merged
    s, e = tiles[0]
    for shift in (4, 2, 1):
        s, more = two_sum(s, pltpu.roll(s, shift, 0))
        e = e + pltpu.roll(e, shift, 0) + more
    lane = iota((8, LANES), 1)
    zero = jnp.zeros((8, LANES), f32)

    def over_lanes(x):
        return jnp.broadcast_to(jnp.sum(x, axis=1, keepdims=True), (8, LANES))

    n = []
    for i in range(6):
        high = over_lanes(jnp.where(lane == i, s, zero))
        low = over_lanes(jnp.where((lane == i + 8) | (lane == i + 16), s, jnp.where(lane == i, e, zero)))
        n.append(two_sum(high, low))
    c = coefficients(n)
    for i in range(3):
        coef_out[i] = c[i]
    for g in range(2):
        edge = lane == (LANES - 1 if g else 0)
        for q in range(H // 4 // 8):
            at = (g, pl.ds(8 * q, 8), slice(None))
            value = zero
            for i in range(3):
                start = H // 4 * i + 8 * q
                value = value + c[i] * jnp.where(edge, edges[start : start + 8], pooled[(i, *at)])
            for d in range(16):
                mid_out[(d, *at)] = value


def solve(all_sums, pooled, w):
    return pl.pallas_call(
        solve_kernel,
        out_shape=(near((3, 8, LANES)), near((16, 2, H // 4, LANES))),
        in_specs=[WHOLE] * 3,
        out_specs=(WHOLE,) * 2,
        compiler_params=LIMIT,
        cost_estimate=cost(1),
        name="coefficients",
    )(*held(all_sums, pooled, w))


def half_matrix(rows):
    return jnp.where(iota((rows, rows // 2), 0) // 2 == iota((rows, rows // 2), 1), f32(0.25), f32(0.0))


def pooled_rows(parts):
    return sums_of(jnp.concatenate(parts, 1), half_matrix(2 * LANES).astype(jnp.bfloat16))


def store_mid(x, core, mid_out, sem):
    copies = []
    for g in range(2):
        to = mid_out.at[:, core, :, pl.ds(g * LANES, LANES)]
        copies.append(pltpu.make_async_copy(x.at[:, g], to, sem.at[g]))
        copies[-1].start()
    return copies


def store_coarse(x, core, coarse_out, scratch, sem):
    rows = H // 8
    parts = [
        jnp.concatenate(
            [x[d, g, pl.ds(0, rows, stride=2), :] + x[d, g, pl.ds(1, rows, stride=2), :] for d in range(16)], 0
        )
        for g in range(2)
    ]
    pooled = pooled_rows(parts)
    for d in range(16):
        scratch[d] = pooled[d * rows : (d + 1) * rows]
    copy = pltpu.make_async_copy(scratch, coarse_out.at[:, core], sem)
    copy.start()
    return copy


def own_kernel(
    x, coef, v0, v1, v2, w, blended_out, fine_out, mid_out, coarse_out, flat, stacked, fine, coarse, sem
):
    core = lax.axis_index("row_2")
    copies = store_mid(x, core, mid_out, sem)
    c = [coef[i] for i in range(3)]
    lane = iota((8, LANES), 1)
    parts = 4
    for p in range(parts):
        for u in range(TILES // parts):
            base = 8 * (p * (TILES // parts) + u)
            rows = pl.ds(base + TOP, 8)
            seams = c[0] * w[0, rows, :] + c[1] * w[1, rows, :] + c[2] * w[2, rows, :]
            for j in range(BLOCKS):
                at = (j, rows, slice(None))
                value = c[0] * v0[at] + c[1] * v1[at] + c[2] * v2[at]
                if j == 0:
                    value = jnp.where(lane < HALO, turn(seams, -LEFT), value)
                if j == BLOCKS - 1:
                    value = jnp.where(lane >= LANES - HALO, turn(seams, LANES - RIGHT - SEAM), value)
                flat[pl.ds(base, 8), pl.ds(j * LANES, LANES)] = value
                stacked[j, pl.ds(base, 8), :] = value
        rows = pl.ds(p * H // parts, H // parts)
        copies.append(pltpu.make_async_copy(flat.at[rows, :], blended_out.at[rows, :], sem.at[3 + p]))
        copies[-1].start()
    for g in range(BLOCKS // 2):
        halves = [
            stacked[2 * g + i, pl.ds(0, H // 2, stride=2), :] + stacked[2 * g + i, pl.ds(1, H // 2, stride=2), :]
            for i in range(2)
        ]
        fine[:, pl.ds(g * LANES, LANES)] = pooled_rows(halves)
    copies.append(pltpu.make_async_copy(fine, fine_out, sem.at[3 + parts]))
    copies[-1].start()
    copies.append(store_coarse(x, core, coarse_out, coarse, sem.at[2]))
    for copy in copies:
        copy.wait()


LEVELS = (
    jax.ShapeDtypeStruct((16, 2, H // 4, W // 4), f32),
    jax.ShapeDtypeStruct((16, 2, H // 8, W // 8), f32),
)


def own_levels(x, coef, v0, v1, v2, w):
    return pl.pallas_call(
        own_kernel,
        out_shape=(
            jax.ShapeDtypeStruct((H, W), f32),
            jax.ShapeDtypeStruct((H // 2, W // 2), f32),
            *LEVELS,
        ),
        in_specs=[WHOLE] * 6,
        out_specs=(FAR,) * 4,
        scratch_shapes=[
            pltpu.VMEM((H, W), f32),
            pltpu.VMEM((BLOCKS, H, LANES), f32),
            pltpu.VMEM((H // 2, W // 2), f32),
            pltpu.VMEM((16, H // 8, LANES), f32),
            pltpu.SemaphoreType.DMA((8,)),
        ],
        compiler_params=LIMIT,
        cost_estimate=cost(2),
        name="own_levels",
    )(*held(x, coef, v0, v1, v2, w))


def other_kernel(x, mid_in, coarse_in, mid_out, coarse_out, coarse, sem):
    del mid_in, coarse_in
    core = 1 - lax.axis_index("row_2")
    copies = store_mid(x, core, mid_out, sem)
    copies.append(store_coarse(x, core, coarse_out, coarse, sem.at[2]))
    for copy in copies:
        copy.wait()


def other_levels(x, mid, coarse):
    return pl.pallas_call(
        other_kernel,
        out_shape=LEVELS,
        in_specs=[WHOLE, FAR, FAR],
        out_specs=(FAR,) * 2,
        scratch_shapes=[
            pltpu.VMEM((16, H // 8, LANES), f32),
            pltpu.SemaphoreType.DMA((3,)),
        ],
        input_output_aliases={1: 0, 2: 1},
        compiler_params=LIMIT,
        cost_estimate=cost(1),
        name="other_levels",
    )(*held(x), *far(mid, coarse))


def swaps(devices, first):
    pairs = [(i, i + 1) for i in range(first, devices - 1, 2)]
    return pairs + [(b, a) for a, b in pairs]


def exchange(even, odd, axis):
    devices = lax.axis_size(axis)
    odd = lax.ppermute(odd, axis, swaps(devices, 1))
    even = lax.ppermute(even, axis, swaps(devices, 0))
    return even, odd


def per_device(sources, labels):
    even, odd = pack_rows(sources, labels)
    even, odd, planes, marks = lax.optimization_barrier((even, odd, sources, labels))
    r_even, r_odd = exchange(even, odd, ROW)
    ext, lext, left, right, v0, v1, v2, totals, base = load(planes, marks)
    c_even, c_odd = exchange(*pack_columns(r_even, r_odd, left, right), "col")
    v0, v1, v2, base, totals = inner(ext, lext, v0, v1, v2, base, r_even, r_odd, totals)
    pooled, totals = lax.optimization_barrier((pool(v0, v1, v2), totals))
    w, sums = seam(base, totals, c_even, c_odd)
    sums = sums.reshape(256, 1, LANES)
    sums = lax.all_to_all(sums, ALL, split_axis=0, concat_axis=0, tiled=True)
    coef, mid = solve(sums.reshape(256, LANES), pooled, w)
    mid = lax.all_to_all(mid, CHIP, split_axis=0, concat_axis=0, tiled=True)
    other = lax.ppermute(mid, "row_2", [(0, 1), (1, 0)])
    blended, fine, overview_mid, overview_coarse = own_levels(mid, coef, v0, v1, v2, w)
    overview_mid, overview_coarse = other_levels(other, overview_mid, overview_coarse)
    overview_mid = overview_mid.reshape(8 * H, W // 4)
    overview_coarse = overview_coarse.reshape(4 * H, W // 8)
    return (blended, fine, overview_mid, overview_coarse)


def solution(mesh):
    finer = Mesh(
        mesh.devices.reshape(4, 4, 2, mesh.shape["col"]), ("row_0", "row_1", "row_2", "col")
    )
    return jax.shard_map(
        per_device,
        mesh=finer,
        in_specs=(P(None, ROW, "col"), P(ROW, "col")),
        out_specs=(P(ROW, "col"), P(ROW, "col"), P(None, "col"), P(None, "col")),
        check_vma=False,
    )
```

```python
import jax
import jax.numpy as jnp
from jax import lax
from jax.experimental import pallas as pl
from jax.experimental.pallas import tpu as pltpu
from jax.sharding import Mesh
from jax.sharding import PartitionSpec as P


K = 3
H, W = 128, 1024
TOP = 16
ROWS = TOP + H + 24
LANES = 128
BLOCKS = W // LANES
HALO = 4
ROW = ("row_0", "row_1", "row_2")
CHIP = ("row_0", "row_1")
VMEM = pltpu.MemorySpace.VMEM
WHOLE = pl.BlockSpec(memory_space=VMEM)
FAR = pl.BlockSpec(memory_space=pltpu.MemorySpace.HBM)
LIMIT = pltpu.CompilerParams(vmem_limit_bytes=24 * 2**20)
TILES = H // 8
LEFT, RIGHT = HALO, 64
SEAM = 12
f32 = jnp.float32


def iota(shape, dim):
    return lax.broadcasted_iota(jnp.int32, shape, dim)


def place():
    row = (lax.axis_index("row_0") * 4 + lax.axis_index("row_1")) * 2 + lax.axis_index("row_2")
    return row, lax.axis_index("col")


def near(shape, dtype=f32):
    return pltpu.VMEM(shape, dtype)


def held(*values):
    return [pltpu.with_memory_space_constraint(v, VMEM) for v in values]


def far(*values):
    return [pltpu.with_memory_space_constraint(v, pltpu.MemorySpace.HBM) for v in values]


def cost(us):
    return pl.CostEstimate(flops=int(us * 3e8), bytes_accessed=0, transcendentals=0)


def sums_of(x, weights):
    total = None
    for _ in range(3):
        part = x.astype(jnp.bfloat16)
        x = x - part.astype(f32)
        term = jnp.dot(part, weights, preferred_element_type=f32)
        total = term if total is None else total + term
    return total


def pack_kernel(src, lab, even_out, odd_out, rows, lrows, sem):
    copies = []
    for side, start in ((0, 0), (1, H - 8)):
        for i, (a, b) in enumerate(
            (
                (src.at[:, pl.ds(start, 8), :], rows.at[side]),
                (lab.at[pl.ds(start, 8), :], lrows.at[side]),
            )
        ):
            c = pltpu.make_async_copy(a, b, sem.at[side, i])
            c.start()
            copies.append(c)
    for c in copies:
        c.wait()
    row, _ = place()
    even = (row % 2) == 0
    upper = iota((8, W), 0) < HALO

    def sides(side):
        a = [rows[side, k] for k in range(K)] + [lrows[side].astype(f32)]
        pairs = []
        for x, y in ((a[0], a[1]), (a[2], a[3])):
            if side == 0:
                pairs.append(jnp.where(upper, x, pltpu.roll(y, HALO, 0)))
            else:
                pairs.append(jnp.where(upper, pltpu.roll(x, HALO, 0), y))
        return pairs

    top, bottom = sides(0), sides(1)
    for i in range(2):
        even_out[pl.ds(8 * i, 8), :] = jnp.where(even, bottom[i], top[i])
        odd_out[pl.ds(8 * i, 8), :] = jnp.where(even, top[i], bottom[i])


def pack_rows(sources, labels):
    return pl.pallas_call(
        pack_kernel,
        out_shape=(near((16, W)), near((16, W))),
        in_specs=[FAR] * 2,
        out_specs=(WHOLE,) * 2,
        scratch_shapes=[
            pltpu.VMEM((2, K, 8, W), f32),
            pltpu.VMEM((2, 8, W), jnp.int32),
            pltpu.SemaphoreType.DMA((2, 2)),
        ],
        compiler_params=LIMIT,
        cost_estimate=cost(1),
        name="pack_rows",
    )(*far(sources, labels))


def window(lane, start, size):
    return (lane >= start) & (lane < start + size)


def turn(x, shift):
    shift %= LANES
    return pltpu.roll(x, shift, 1) if shift else x


def load_kernel(
    src, lab, ext, lext, left_out, right_out, v0, v1, v2, totals_out, seam_out
):
    own = pl.ds(TOP, H)
    for j in (0, BLOCKS - 1, *range(1, BLOCKS - 1)):
        lanes = pl.ds(j * LANES, LANES)
        for k in range(K):
            ext[k, j, own, :] = src[k, :, lanes]
        lext[j, own, :] = lab[:, lanes]
    lane = iota((8, LANES), 1)
    for j, out, first in ((0, left_out, 0), (BLOCKS - 1, right_out, LANES - HALO)):
        for half in range(2):
            total = jnp.zeros((8, LANES), f32)
            for g in range(8):
                at = pl.ds(TOP + 64 * half + 8 * g, 8)
                for k in range(K + 1):
                    x = ext[k, j, at, :] if k < K else lext[j, at, :].astype(f32)
                    to = 16 * g + HALO * k
                    total = jnp.where(window(lane, to, HALO), turn(x, to - first), total)
            out[pl.ds(8 * half, 8), :] = total

    over_tiles(1, TILES - 2, 7, lambda base, c: (right_side(ext, lext, v0, base), c)[1], 0)
    over_tiles(2, TILES - 3, 6, lambda base, c: (neighbours(v0, v1, base), c)[1], 0)
    over_tiles(3, TILES - 4, 5, lambda base, c: (neighbours(v1, v2, base), c)[1], 0)
    zero = jnp.zeros((8, LANES), f32)
    totals = over_tiles(3, TILES - 5, 3, lambda base, c: products(v0, v1, v2, base, c), (zero,) * 6)
    for i in range(6):
        totals_out[i] = totals[i]
    for tile in range(TILES):
        seam_base(ext, lext, seam_out, tile)


def load(sources, labels):
    field = near((BLOCKS, ROWS, LANES))
    return pl.pallas_call(
        load_kernel,
        out_shape=(
            near((K, BLOCKS, ROWS, LANES)),
            near((BLOCKS, ROWS, LANES), jnp.int32),
            near((16, LANES)),
            near((16, LANES)),
            field,
            field,
            field,
            near((6, 8, LANES)),
            near((K + 1, ROWS, LANES)),
        ),
        in_specs=[WHOLE] * 2,
        out_specs=(WHOLE,) * 9,
        compiler_params=LIMIT,
        cost_estimate=cost(3),
        name="load_block",
    )(*held(sources, labels))


def corner_kernel(got_even, got_odd, left, right, even_out, odd_out):
    row, col = place()
    row_even = (row % 2) == 0
    col_even = (col % 2) == 0
    upper = iota((8, LANES), 0) < HALO
    lane = iota((8, LANES), 1)
    strips = []
    for start, first in ((0, 0), (W - LANES, LANES - HALO)):
        total = jnp.zeros((8, LANES), f32)
        for k in range(K + 1):
            tile, half = divmod(k, 2)
            at = (pl.ds(8 * tile, 8), pl.ds(start, LANES))
            e, o = got_even[at], got_odd[at]
            above = jnp.where(row_even, o, e)
            below = jnp.where(row_even, e, o)
            if half:
                both = jnp.where(upper, pltpu.roll(above, HALO, 0), below)
            else:
                both = jnp.where(upper, above, pltpu.roll(below, HALO, 0))
            total = jnp.where(window(lane, HALO * k, HALO), turn(both, HALO * k - first), total)
        strips.append(total)
    even_out[pl.ds(0, 16), :] = jnp.where(col_even, right[...], left[...])
    odd_out[pl.ds(0, 16), :] = jnp.where(col_even, left[...], right[...])
    even_out[pl.ds(16, 8), :] = jnp.where(col_even, strips[1], strips[0])
    odd_out[pl.ds(16, 8), :] = jnp.where(col_even, strips[0], strips[1])


def pack_columns(got_even, got_odd, left, right):
    return pl.pallas_call(
        corner_kernel,
        out_shape=(near((24, LANES)),) * 2,
        in_specs=[WHOLE] * 4,
        out_specs=(WHOLE,) * 2,
        compiler_params=LIMIT,
        cost_estimate=cost(0.5),
        name="pack_columns",
    )(*held(got_even, got_odd, left, right))


def two_sum(a, b):
    s = a + b
    t = s - a
    return s, (a - (s - t)) + (b - t)


def shifted(tiles):
    lane = iota((8, LANES), 1)
    to_left = [pltpu.roll(t, LANES - 1, 1) for t in tiles]
    to_right = [pltpu.roll(t, 1, 1) for t in tiles]
    last, first = lane == LANES - 1, lane == 0
    n = len(tiles)
    after = [jnp.where(last, to_left[min(j + 1, n - 1)], to_left[j]) for j in range(n)]
    before = [jnp.where(first, to_right[max(j - 1, 0)], to_right[j]) for j in range(n)]
    return after, before


PAIRS = ((0, 0), (0, 1), (1, 1), (1, 2), (2, 2), (2, 3))


def right_side(ext, lext, out, base):
    at = pl.ds(base, 8)
    picked = [lext[j, at, :] for j in range(BLOCKS)]
    center, around = [None] * BLOCKS, [None] * BLOCKS
    for k in range(K):
        tiles = [ext[k, j, at, :] for j in range(BLOCKS)]
        after, before = shifted(tiles)
        for j in range(BLOCKS):
            near_sum = ext[k, j, pl.ds(base + 1, 8), :] + ext[k, j, pl.ds(base - 1, 8), :]
            near_sum = near_sum + after[j] + before[j]
            here = picked[j] == k
            center[j] = jnp.where(here, tiles[j], center[j]) if k else tiles[j]
            around[j] = jnp.where(here, near_sum, around[j]) if k else near_sum
    for j in range(BLOCKS):
        out[j, at, :] = 4.0 * center[j] - around[j]


def neighbours(source, target, base):
    tiles = [source[j, pl.ds(base, 8), :] for j in range(BLOCKS)]
    after, before = shifted(tiles)
    for j in range(BLOCKS):
        vertical = source[j, pl.ds(base + 1, 8), :] + source[j, pl.ds(base - 1, 8), :]
        target[j, pl.ds(base, 8), :] = vertical + after[j] + before[j]


def over_tiles(first, last, chunk, step, carry):
    def turn_of(t, carry):
        for u in range(chunk):
            carry = step(pl.multiple_of(TOP + 8 * first + 8 * (chunk * t + u), 8), carry)
        return carry

    return lax.fori_loop(0, (last - first + 1) // chunk, turn_of, carry)


def tree(x):
    while len(x) > 1:
        x = [sum(x[a : a + 2][1:], x[a]) for a in range(0, len(x), 2)]
    return x[0]


def products(v0, v1, v2, base, totals):
    lane = iota((8, LANES), 1)
    last = lane == LANES - 1
    kept = {0: lane >= HALO, BLOCKS - 1: lane < LANES - HALO}
    at = pl.ds(base, 8)
    found = [[] for _ in PAIRS]
    rolled = [turn(v2[j, at, :], -1) for j in range(BLOCKS)]
    for j in range(BLOCKS):
        x = [v[j, at, :] for v in (v0, v1, v2)]
        right = jnp.where(last, rolled[min(j + 1, BLOCKS - 1)], rolled[j])
        x.append(v2[j, pl.ds(base + 1, 8), :] + right)
        own = [jnp.where(kept[j], a, 0.0) for a in x[:3]] if j in kept else x
        for i, (a, b) in enumerate(PAIRS):
            found[i].append(own[a] * x[b])
    return tuple(total + tree(f) for total, f in zip(totals, found))


def seam_base(ext, lext, out, tile):
    lane = iota((8, LANES), 1)
    at = pl.ds(TOP + 8 * tile, 8)
    for k in range(K + 1):
        a, b = [ext[k, j, at, :] if k < K else lext[j, at, :].astype(f32) for j in (0, BLOCKS - 1)]
        out[k, at, :] = jnp.where(lane < 64, turn(a, LEFT), turn(b, RIGHT + SEAM))


def clear_rows(ref, row):
    @pl.when(row == 0)
    def _():
        for j in range(BLOCKS):
            ref[j, pl.ds(TOP - 8, 8), :] = jnp.zeros((8, LANES), f32)

    @pl.when(row == 31)
    def _():
        for j in range(BLOCKS):
            ref[j, pl.ds(TOP + H, 8), :] = jnp.zeros((8, LANES), f32)


def inner_kernel(*refs):
    r_even, r_odd, totals_in = refs[6:9]
    ext, lext, v0, v1, v2, seam_out, totals_out = refs[9:]
    row, _ = place()
    row_even = (row % 2) == 0
    for k in range(K + 1):
        at = pl.ds(HALO * k, HALO)
        for j in range(BLOCKS):
            lanes = pl.ds(j * LANES, LANES)
            e, o = r_even[at, lanes], r_odd[at, lanes]
            above, below = jnp.where(row_even, o, e), jnp.where(row_even, e, o)
            for start, value in ((TOP - HALO, above), (TOP + H, below)):
                if k < K:
                    ext[k, j, pl.ds(start, HALO), :] = value
                else:
                    lext[j, pl.ds(start, HALO), :] = value.astype(jnp.int32)
    seam_base(ext, lext, seam_out, -1)
    seam_base(ext, lext, seam_out, TILES)
    for t in (-1, 0, TILES - 1, TILES):
        right_side(ext, lext, v0, TOP + 8 * t)
    clear_rows(v0, row)
    for t in (-1, 0, 1, TILES - 2, TILES - 1, TILES):
        neighbours(v0, v1, TOP + 8 * t)
    clear_rows(v1, row)
    for t in (-1, 0, 1, 2, TILES - 3, TILES - 2, TILES - 1, TILES):
        neighbours(v1, v2, TOP + 8 * t)
    clear_rows(v2, row)
    totals = tuple(totals_in[i] for i in range(6))
    for t in (0, 1, 2, *range(TILES - 4, TILES)):
        totals = products(v0, v1, v2, TOP + 8 * t, totals)
    for i in range(6):
        totals_out[i] = totals[i]


def inner(ext, lext, v0, v1, v2, base, r_even, r_odd, totals):
    field = near((BLOCKS, ROWS, LANES))
    return pl.pallas_call(
        inner_kernel,
        out_shape=(
            near((K, BLOCKS, ROWS, LANES)),
            near((BLOCKS, ROWS, LANES), jnp.int32),
            field,
            field,
            field,
            near((K + 1, ROWS, LANES)),
            near((6, 8, LANES)),
        ),
        in_specs=[WHOLE] * 9,
        out_specs=(WHOLE,) * 7,
        input_output_aliases={i: i for i in range(6)},
        compiler_params=LIMIT,
        cost_estimate=cost(2),
        name="inner_fields",
    )(*held(ext, lext, v0, v1, v2, base, r_even, r_odd, totals))[2:]


def seam_kernel(base, totals_in, c_even, c_odd, w, sums_out, planes):
    row, col = place()
    col_even = (col % 2) == 0
    lane = iota((8, LANES), 1)
    from_left, from_right = lane < LEFT, window(lane, RIGHT + SEAM, HALO)
    outside = (from_left & (col == 0)) | (from_right & (col == 7))
    for t in range(TILES + 2):
        at = pl.ds(TOP - 8 + 8 * t, 8)
        corner = t in (0, TILES + 1)
        tile, g = (2, 0) if corner else divmod(t - 1, 8)
        e, o = c_even[pl.ds(8 * tile, 8), :], c_odd[pl.ds(8 * tile, 8), :]
        a, b = jnp.where(col_even, o, e), jnp.where(col_even, e, o)
        if corner:
            a, b = pltpu.roll(a, HALO, 0), pltpu.roll(b, HALO, 0)
        for k in range(K + 1):
            lanes = 16 * g + HALO * k
            planes[k, at, :] = jnp.where(
                from_left,
                turn(a, -lanes),
                jnp.where(from_right, turn(b, RIGHT + SEAM - lanes), base[k, at, :]),
            )

    def put(i, t, value):
        hidden = outside
        if t == 0:
            hidden = hidden | (row == 0)
        if t == TILES + 1:
            hidden = hidden | (row == 31)
        w[i, pl.ds(TOP - 8 + 8 * t, 8), :] = jnp.where(hidden, 0.0, value)

    for t in range(TILES + 2):
        start = TOP - 8 + 8 * t
        total = jnp.zeros((8, LANES), f32)
        picked = planes[K, pl.ds(start, 8), :]
        for k in range(K):
            x = planes[k, pl.ds(start, 8), :]
            vertical = planes[k, pl.ds(start + 1, 8), :] + planes[k, pl.ds(start - 1, 8), :]
            term = 4.0 * x - (vertical + turn(x, -1) + turn(x, 1))
            total = jnp.where(picked == k, term, total)
        put(0, t, total)
    for i in range(2):
        for t in range(TILES + 2):
            start = TOP - 8 + 8 * t
            x = w[i, pl.ds(start, 8), :]
            vertical = w[i, pl.ds(start + 1, 8), :] + w[i, pl.ds(start - 1, 8), :]
            put(i + 1, t, vertical + turn(x, -1) + turn(x, 1))
    own_lane = window(lane, LEFT, HALO) | window(lane, RIGHT + SEAM - HALO, HALO)
    found = [[] for _ in PAIRS]
    for t in range(TILES):
        start = TOP + 8 * t
        x = [w[i, pl.ds(start, 8), :] for i in range(3)]
        x.append(w[2, pl.ds(start + 1, 8), :] + turn(x[2], -1))
        for i, (a, b) in enumerate(PAIRS):
            found[i].append(x[a] * x[b])
    totals = [totals_in[i] + jnp.where(own_lane, tree(found[i]), 0.0) for i in range(6)]

    line = jnp.zeros((8, LANES), f32)
    for i in range(6):
        x = totals[i] + totals[i] if i == 5 else totals[i]
        big = 512.0 * jnp.max(jnp.abs(x), axis=1, keepdims=True)
        high = (x + big) - big
        line = jnp.where(
            (lane == i) | (lane == i + 16) | (lane == i + 24),
            jnp.sum(high, axis=1, keepdims=True),
            jnp.where(lane == i + 8, jnp.sum(x - high, axis=1, keepdims=True), line),
        )
    s, e = line, jnp.zeros_like(line)
    for shift in (4, 2, 1):
        s, more = two_sum(s, pltpu.roll(s, shift, 0))
        e = e + pltpu.roll(e, shift, 0) + more
    sums_out[...] = jnp.where(lane < 24, s, e)


def seam(base, totals, c_even, c_odd):
    return pl.pallas_call(
        seam_kernel,
        out_shape=(near((3, ROWS, LANES)), near((8, LANES))),
        in_specs=[WHOLE] * 4,
        out_specs=(WHOLE,) * 2,
        scratch_shapes=[pltpu.VMEM((K + 1, ROWS, LANES), f32)],
        compiler_params=LIMIT,
        cost_estimate=cost(1),
        name="seam_fields",
    )(*held(base, totals, c_even, c_odd))


def merge_kernel(own, other, out):
    s, e = two_sum(own[...], other[...])
    line = jnp.where(window(iota((8, LANES), 1), 16, 8), e, s)
    out[...] = jnp.broadcast_to(line[:1].reshape(1, 1, LANES), (128, 1, LANES))


def merge(own, other):
    return pl.pallas_call(
        merge_kernel,
        out_shape=near((128, 1, LANES)),
        in_specs=[WHOLE] * 2,
        out_specs=WHOLE,
        compiler_params=LIMIT,
        cost_estimate=cost(0.2),
        name="merge_cores",
    )(*held(own, other))


def pool_kernel(v0, v1, v2, out):
    spread = jnp.where(iota((512, LANES), 0) // 4 == iota((512, LANES), 1), f32(0.0625), f32(0.0))
    for i, ref in enumerate((v0, v1, v2)):
        for g in range(2):
            parts = []
            for j in range(4):
                at = [ref[4 * g + j, pl.ds(TOP + q, H // 4, stride=4), :] for q in range(4)]
                parts.append((at[0] + at[1]) + (at[2] + at[3]))
            out[i, g] = sums_of(jnp.concatenate(parts, 1), spread.astype(jnp.bfloat16))


def pool(v0, v1, v2):
    return pl.pallas_call(
        pool_kernel,
        out_shape=near((3, 2, H // 4, LANES)),
        in_specs=[WHOLE] * 3,
        out_specs=WHOLE,
        compiler_params=LIMIT,
        cost_estimate=cost(1),
        name="pool_fields",
    )(*held(v0, v1, v2))


def two_product(a, b):
    p = a * b
    big = f32(4097.0)
    t = big * a
    ah = t - (t - a)
    al = a - ah
    t = big * b
    bh = t - (t - b)
    bl = b - bh
    return p, ((ah * bh - p) + ah * bl + al * bh) + al * bl


def less_scaled(a, b, scale):
    p, low = two_product(b[0], scale)
    low = low + b[1] * scale
    s, e = two_sum(a[0], -p)
    e = e + (a[1] - low)
    return two_sum(s, e)


def coefficients(n):
    shift = n[1][0] / n[0][0]
    current = n
    m = [n[0][0]]
    for _ in range(5):
        current = [less_scaled(current[i + 1], current[i], shift) for i in range(len(current) - 1)]
        m.append(current[0][0] + current[0][1])
    m0, m1, m2, m3, m4, m5 = m
    t = m1 / m0
    theta0 = shift + t
    m5 = m5 - 5.0 * t * m4
    m4 = m4 - 4.0 * t * m3
    m3 = m3 - 3.0 * t * m2
    m2 = m2 - t * m1
    one = jnp.ones_like(m0)
    zero = jnp.zeros_like(m0)
    second = m2 > 0.0
    safe2 = jnp.where(second, m2, one)
    b1 = jnp.where(second, m2 / m0, zero)
    s = jnp.where(second, m3 / safe2, zero)
    h2 = m4 - s * m3 - b1 * m2
    third = second & (h2 > 0.0)
    safe3 = jnp.where(third, h2, one)
    theta1 = jnp.clip(theta0 + s, -4.0, 4.0)
    theta2 = jnp.clip(theta0 - s + (m5 - s * m4 - b1 * m3) / safe3, -4.0, 4.0)
    b2 = h2 / safe2
    d0, d1, d2 = 4.0 - theta0, 4.0 - theta1, 4.0 - theta2
    e = d1 * d2 - b2
    two, three = d0 * d1 - b1, d0 * e - b1 * d2
    second = second & (two > 0.0)
    third = second & third & (three > 0.0)
    y2 = jnp.where(third, one / three, zero)
    y1 = jnp.where(third, d2 * y2, jnp.where(second, one / two, zero))
    y0 = jnp.where(third, e * y2, jnp.where(second, d1 * y1, one / d0))
    return (
        y0 - theta0 * y1 + (theta0 * theta1 - b1) * y2,
        y1 - (theta0 + theta1) * y2,
        y2,
    )


def solve_kernel(all_sums, pooled, w, coef_out, mid_out):
    frm, to = iota((LANES, LANES), 0), iota((LANES, LANES), 1)
    first = window(frm, LEFT, HALO) & (to == 0)
    final = window(frm, RIGHT + SEAM - HALO, HALO) & (to == LANES - 1)
    rows = []
    for i in range(3):
        at = [w[i, pl.ds(TOP + q, H // 4, stride=4), :] for q in range(4)]
        rows.append((at[0] + at[1]) + (at[2] + at[3]))
    weights = jnp.where(first | final, f32(0.0625), f32(0.0)).astype(jnp.bfloat16)
    edges = sums_of(jnp.concatenate(rows, 0), weights)
    tiles = [(all_sums[pl.ds(8 * i, 8), :], jnp.zeros((8, LANES), f32)) for i in range(16)]
    while len(tiles) > 1:
        merged = []
        for a, b in zip(tiles[0::2], tiles[1::2]):
            s, e = two_sum(a[0], b[0])
            merged.append((s, e + (a[1] + b[1])))
        tiles = merged
    s, e = tiles[0]
    for shift in (4, 2, 1):
        s, more = two_sum(s, pltpu.roll(s, shift, 0))
        e = e + pltpu.roll(e, shift, 0) + more
    lane = iota((8, LANES), 1)
    zero = jnp.zeros((8, LANES), f32)

    def over_lanes(x):
        return jnp.broadcast_to(jnp.sum(x, axis=1, keepdims=True), (8, LANES))

    n = []
    for i in range(6):
        high = over_lanes(jnp.where(lane == i, s, zero))
        low = over_lanes(
            jnp.where((lane == i + 8) | (lane == i + 16) | (lane == i + 24), s, jnp.where(lane == i, e, zero))
        )
        n.append(two_sum(high, low))
    c = coefficients(n)
    for i in range(3):
        coef_out[i] = c[i]
    for g in range(2):
        edge = lane == (LANES - 1 if g else 0)
        for q in range(H // 4 // 8):
            at = (g, pl.ds(8 * q, 8), slice(None))
            value = zero
            for i in range(3):
                start = H // 4 * i + 8 * q
                value = value + c[i] * jnp.where(edge, edges[start : start + 8], pooled[(i, *at)])
            for d in range(16):
                mid_out[(d, *at)] = value


def solve(all_sums, pooled, w):
    return pl.pallas_call(
        solve_kernel,
        out_shape=(near((3, 8, LANES)), near((16, 2, H // 4, LANES))),
        in_specs=[WHOLE] * 3,
        out_specs=(WHOLE,) * 2,
        compiler_params=LIMIT,
        cost_estimate=cost(1),
        name="coefficients",
    )(*held(all_sums, pooled, w))


def half_matrix(rows):
    return jnp.where(iota((rows, rows // 2), 0) // 2 == iota((rows, rows // 2), 1), f32(0.25), f32(0.0))


def pooled_rows(parts):
    return sums_of(jnp.concatenate(parts, 1), half_matrix(2 * LANES).astype(jnp.bfloat16))


def store_mid(x, core, mid_out, sem):
    copies = []
    for g in range(2):
        to = mid_out.at[:, core, :, pl.ds(g * LANES, LANES)]
        copies.append(pltpu.make_async_copy(x.at[:, g], to, sem.at[g]))
        copies[-1].start()
    return copies


def store_coarse(x, core, coarse_out, scratch, sem):
    rows = H // 8
    parts = [
        jnp.concatenate(
            [x[d, g, pl.ds(0, rows, stride=2), :] + x[d, g, pl.ds(1, rows, stride=2), :] for d in range(16)], 0
        )
        for g in range(2)
    ]
    pooled = pooled_rows(parts)
    for d in range(16):
        scratch[d] = pooled[d * rows : (d + 1) * rows]
    copy = pltpu.make_async_copy(scratch, coarse_out.at[:, core], sem)
    copy.start()
    return copy


def own_kernel(
    x, coef, v0, v1, v2, w, blended_out, fine_out, mid_out, coarse_out, flat, stacked, fine, coarse, sem
):
    core = lax.axis_index("row_2")
    copies = store_mid(x, core, mid_out, sem)
    c = [coef[i] for i in range(3)]
    lane = iota((8, LANES), 1)
    parts = 4
    for p in range(parts):
        for u in range(TILES // parts):
            base = 8 * (p * (TILES // parts) + u)
            rows = pl.ds(base + TOP, 8)
            seams = c[0] * w[0, rows, :] + c[1] * w[1, rows, :] + c[2] * w[2, rows, :]
            for j in range(BLOCKS):
                at = (j, rows, slice(None))
                value = c[0] * v0[at] + c[1] * v1[at] + c[2] * v2[at]
                if j == 0:
                    value = jnp.where(lane < HALO, turn(seams, -LEFT), value)
                if j == BLOCKS - 1:
                    value = jnp.where(lane >= LANES - HALO, turn(seams, LANES - RIGHT - SEAM), value)
                flat[pl.ds(base, 8), pl.ds(j * LANES, LANES)] = value
                stacked[j, pl.ds(base, 8), :] = value
        rows = pl.ds(p * H // parts, H // parts)
        copies.append(pltpu.make_async_copy(flat.at[rows, :], blended_out.at[rows, :], sem.at[3 + p]))
        copies[-1].start()
    for g in range(BLOCKS // 2):
        halves = [
            stacked[2 * g + i, pl.ds(0, H // 2, stride=2), :] + stacked[2 * g + i, pl.ds(1, H // 2, stride=2), :]
            for i in range(2)
        ]
        fine[:, pl.ds(g * LANES, LANES)] = pooled_rows(halves)
    copies.append(pltpu.make_async_copy(fine, fine_out, sem.at[3 + parts]))
    copies[-1].start()
    copies.append(store_coarse(x, core, coarse_out, coarse, sem.at[2]))
    for copy in copies:
        copy.wait()


LEVELS = (
    jax.ShapeDtypeStruct((16, 2, H // 4, W // 4), f32),
    jax.ShapeDtypeStruct((16, 2, H // 8, W // 8), f32),
)


def own_levels(x, coef, v0, v1, v2, w):
    return pl.pallas_call(
        own_kernel,
        out_shape=(
            jax.ShapeDtypeStruct((H, W), f32),
            jax.ShapeDtypeStruct((H // 2, W // 2), f32),
            *LEVELS,
        ),
        in_specs=[WHOLE] * 6,
        out_specs=(FAR,) * 4,
        scratch_shapes=[
            pltpu.VMEM((H, W), f32),
            pltpu.VMEM((BLOCKS, H, LANES), f32),
            pltpu.VMEM((H // 2, W // 2), f32),
            pltpu.VMEM((16, H // 8, LANES), f32),
            pltpu.SemaphoreType.DMA((8,)),
        ],
        compiler_params=LIMIT,
        cost_estimate=cost(2),
        name="own_levels",
    )(*held(x, coef, v0, v1, v2, w))


def other_kernel(x, mid_in, coarse_in, mid_out, coarse_out, coarse, sem):
    del mid_in, coarse_in
    core = 1 - lax.axis_index("row_2")
    copies = store_mid(x, core, mid_out, sem)
    copies.append(store_coarse(x, core, coarse_out, coarse, sem.at[2]))
    for copy in copies:
        copy.wait()


def other_levels(x, mid, coarse):
    return pl.pallas_call(
        other_kernel,
        out_shape=LEVELS,
        in_specs=[WHOLE, FAR, FAR],
        out_specs=(FAR,) * 2,
        scratch_shapes=[
            pltpu.VMEM((16, H // 8, LANES), f32),
            pltpu.SemaphoreType.DMA((3,)),
        ],
        input_output_aliases={1: 0, 2: 1},
        compiler_params=LIMIT,
        cost_estimate=cost(1),
        name="other_levels",
    )(*held(x), *far(mid, coarse))


def swaps(devices, first):
    pairs = [(i, i + 1) for i in range(first, devices - 1, 2)]
    return pairs + [(b, a) for a, b in pairs]


def exchange(even, odd, axis):
    devices = lax.axis_size(axis)
    odd = lax.ppermute(odd, axis, swaps(devices, 1))
    even = lax.ppermute(even, axis, swaps(devices, 0))
    return even, odd


def per_device(sources, labels):
    even, odd = pack_rows(sources, labels)
    even, odd, planes, marks = lax.optimization_barrier((even, odd, sources, labels))
    r_even, r_odd = exchange(even, odd, ROW)
    ext, lext, left, right, v0, v1, v2, totals, base = load(planes, marks)
    c_even, c_odd = exchange(*pack_columns(r_even, r_odd, left, right), "col")
    v0, v1, v2, base, totals = inner(ext, lext, v0, v1, v2, base, r_even, r_odd, totals)
    pooled, totals = lax.optimization_barrier((pool(v0, v1, v2), totals))
    w, sums = seam(base, totals, c_even, c_odd)
    sums = merge(sums, lax.ppermute(sums, "row_2", [(0, 1), (1, 0)]))
    sums = lax.all_to_all(sums, (*CHIP, "col"), split_axis=0, concat_axis=0, tiled=True)
    coef, mid = solve(sums.reshape(128, LANES), pooled, w)
    mid = lax.all_to_all(mid, CHIP, split_axis=0, concat_axis=0, tiled=True)
    other = lax.ppermute(mid, "row_2", [(0, 1), (1, 0)])
    blended, fine, overview_mid, overview_coarse = own_levels(mid, coef, v0, v1, v2, w)
    overview_mid, overview_coarse = other_levels(other, overview_mid, overview_coarse)
    overview_mid = overview_mid.reshape(8 * H, W // 4)
    overview_coarse = overview_coarse.reshape(4 * H, W // 8)
    return (blended, fine, overview_mid, overview_coarse)


def solution(mesh):
    finer = Mesh(
        mesh.devices.reshape(4, 4, 2, mesh.shape["col"]), ("row_0", "row_1", "row_2", "col")
    )
    return jax.shard_map(
        per_device,
        mesh=finer,
        in_specs=(P(None, ROW, "col"), P(ROW, "col")),
        out_specs=(P(ROW, "col"), P(ROW, "col"), P(None, "col"), P(None, "col")),
        check_vma=False,
    )
```

```python
import jax
import jax.numpy as jnp
from jax import lax
from jax.experimental import pallas as pl
from jax.experimental.pallas import tpu as pltpu
from jax.sharding import Mesh
from jax.sharding import PartitionSpec as P


K = 3
H, W = 128, 1024
TOP = 16
ROWS = TOP + H + 24
LANES = 128
BLOCKS = W // LANES
HALO = 4
ROW = ("row_0", "row_1", "row_2")
CHIP = ("row_0", "row_1")
VMEM = pltpu.MemorySpace.VMEM
WHOLE = pl.BlockSpec(memory_space=VMEM)
FAR = pl.BlockSpec(memory_space=pltpu.MemorySpace.HBM)
LIMIT = pltpu.CompilerParams(vmem_limit_bytes=24 * 2**20)
TILES = H // 8
LEFT, RIGHT = HALO, 64
SEAM = 12
f32 = jnp.float32


def iota(shape, dim):
    return lax.broadcasted_iota(jnp.int32, shape, dim)


def place():
    row = (lax.axis_index("row_0") * 4 + lax.axis_index("row_1")) * 2 + lax.axis_index("row_2")
    return row, lax.axis_index("col")


def near(shape, dtype=f32):
    return pltpu.VMEM(shape, dtype)


def held(*values):
    return [pltpu.with_memory_space_constraint(v, VMEM) for v in values]


def far(*values):
    return [pltpu.with_memory_space_constraint(v, pltpu.MemorySpace.HBM) for v in values]


def cost(us):
    return pl.CostEstimate(flops=int(us * 3e8), bytes_accessed=0, transcendentals=0)


def sums_of(x, weights):
    total = None
    for _ in range(3):
        part = x.astype(jnp.bfloat16)
        x = x - part.astype(f32)
        term = jnp.dot(part, weights, preferred_element_type=f32)
        total = term if total is None else total + term
    return total


def pack_kernel(src, lab, even_out, odd_out, rows, lrows, sem):
    copies = []
    for side, start in ((0, 0), (1, H - 8)):
        for i, (a, b) in enumerate(
            (
                (src.at[:, pl.ds(start, 8), :], rows.at[side]),
                (lab.at[pl.ds(start, 8), :], lrows.at[side]),
            )
        ):
            c = pltpu.make_async_copy(a, b, sem.at[side, i])
            c.start()
            copies.append(c)
    for c in copies:
        c.wait()
    row, _ = place()
    even = (row % 2) == 0
    upper = iota((8, W), 0) < HALO

    def sides(side):
        a = [rows[side, k] for k in range(K)] + [lrows[side].astype(f32)]
        pairs = []
        for x, y in ((a[0], a[1]), (a[2], a[3])):
            if side == 0:
                pairs.append(jnp.where(upper, x, pltpu.roll(y, HALO, 0)))
            else:
                pairs.append(jnp.where(upper, pltpu.roll(x, HALO, 0), y))
        return pairs

    top, bottom = sides(0), sides(1)
    for i in range(2):
        even_out[pl.ds(8 * i, 8), :] = jnp.where(even, bottom[i], top[i])
        odd_out[pl.ds(8 * i, 8), :] = jnp.where(even, top[i], bottom[i])


def pack_rows(sources, labels):
    return pl.pallas_call(
        pack_kernel,
        out_shape=(near((16, W)), near((16, W))),
        in_specs=[FAR] * 2,
        out_specs=(WHOLE,) * 2,
        scratch_shapes=[
            pltpu.VMEM((2, K, 8, W), f32),
            pltpu.VMEM((2, 8, W), jnp.int32),
            pltpu.SemaphoreType.DMA((2, 2)),
        ],
        compiler_params=LIMIT,
        cost_estimate=cost(1),
        name="pack_rows",
    )(*far(sources, labels))


def window(lane, start, size):
    return (lane >= start) & (lane < start + size)


def turn(x, shift):
    shift %= LANES
    return pltpu.roll(x, shift, 1) if shift else x


def load_kernel(
    src, lab, ext, lext, left_out, right_out, v0, v1, v2, totals_out, seam_out
):
    own = pl.ds(TOP, H)
    for j in (0, BLOCKS - 1, *range(1, BLOCKS - 1)):
        lanes = pl.ds(j * LANES, LANES)
        for k in range(K):
            ext[k, j, own, :] = src[k, :, lanes]
        lext[j, own, :] = lab[:, lanes]
    lane = iota((8, LANES), 1)
    for j, out, first in ((0, left_out, 0), (BLOCKS - 1, right_out, LANES - HALO)):
        for half in range(2):
            total = jnp.zeros((8, LANES), f32)
            for g in range(8):
                at = pl.ds(TOP + 64 * half + 8 * g, 8)
                for k in range(K + 1):
                    x = ext[k, j, at, :] if k < K else lext[j, at, :].astype(f32)
                    to = 16 * g + HALO * k
                    total = jnp.where(window(lane, to, HALO), turn(x, to - first), total)
            out[pl.ds(8 * half, 8), :] = total

    over_tiles(1, TILES - 2, 7, lambda base, c: (right_side(ext, lext, v0, base), c)[1], 0)
    over_tiles(2, TILES - 3, 6, lambda base, c: (neighbours(v0, v1, base), c)[1], 0)
    over_tiles(3, TILES - 4, 5, lambda base, c: (neighbours(v1, v2, base), c)[1], 0)
    zero = jnp.zeros((8, LANES), f32)
    totals = over_tiles(3, TILES - 5, 3, lambda base, c: products(v0, v1, v2, base, c), (zero,) * 6)
    for i in range(6):
        totals_out[i] = totals[i]
    for tile in range(TILES):
        seam_base(ext, lext, seam_out, tile)


def load(sources, labels):
    field = near((BLOCKS, ROWS, LANES))
    return pl.pallas_call(
        load_kernel,
        out_shape=(
            near((K, BLOCKS, ROWS, LANES)),
            near((BLOCKS, ROWS, LANES), jnp.int32),
            near((16, LANES)),
            near((16, LANES)),
            field,
            field,
            field,
            near((6, 8, LANES)),
            near((K + 1, ROWS, LANES)),
        ),
        in_specs=[WHOLE] * 2,
        out_specs=(WHOLE,) * 9,
        compiler_params=LIMIT,
        cost_estimate=cost(3),
        name="load_block",
    )(*held(sources, labels))


def corner_kernel(got_even, got_odd, left, right, even_out, odd_out):
    row, col = place()
    row_even = (row % 2) == 0
    col_even = (col % 2) == 0
    upper = iota((8, LANES), 0) < HALO
    lane = iota((8, LANES), 1)
    strips = []
    for start, first in ((0, 0), (W - LANES, LANES - HALO)):
        total = jnp.zeros((8, LANES), f32)
        for k in range(K + 1):
            tile, half = divmod(k, 2)
            at = (pl.ds(8 * tile, 8), pl.ds(start, LANES))
            e, o = got_even[at], got_odd[at]
            above = jnp.where(row_even, o, e)
            below = jnp.where(row_even, e, o)
            if half:
                both = jnp.where(upper, pltpu.roll(above, HALO, 0), below)
            else:
                both = jnp.where(upper, above, pltpu.roll(below, HALO, 0))
            total = jnp.where(window(lane, HALO * k, HALO), turn(both, HALO * k - first), total)
        strips.append(total)
    even_out[pl.ds(0, 16), :] = jnp.where(col_even, right[...], left[...])
    odd_out[pl.ds(0, 16), :] = jnp.where(col_even, left[...], right[...])
    even_out[pl.ds(16, 8), :] = jnp.where(col_even, strips[1], strips[0])
    odd_out[pl.ds(16, 8), :] = jnp.where(col_even, strips[0], strips[1])


def pack_columns(got_even, got_odd, left, right):
    return pl.pallas_call(
        corner_kernel,
        out_shape=(near((24, LANES)),) * 2,
        in_specs=[WHOLE] * 4,
        out_specs=(WHOLE,) * 2,
        compiler_params=LIMIT,
        cost_estimate=cost(0.5),
        name="pack_columns",
    )(*held(got_even, got_odd, left, right))


def two_sum(a, b):
    s = a + b
    t = s - a
    return s, (a - (s - t)) + (b - t)


def shifted(tiles):
    lane = iota((8, LANES), 1)
    to_left = [pltpu.roll(t, LANES - 1, 1) for t in tiles]
    to_right = [pltpu.roll(t, 1, 1) for t in tiles]
    last, first = lane == LANES - 1, lane == 0
    n = len(tiles)
    after = [jnp.where(last, to_left[min(j + 1, n - 1)], to_left[j]) for j in range(n)]
    before = [jnp.where(first, to_right[max(j - 1, 0)], to_right[j]) for j in range(n)]
    return after, before


PAIRS = ((0, 0), (0, 1), (1, 1), (1, 2), (2, 2), (2, 3))


def right_side(ext, lext, out, base):
    at = pl.ds(base, 8)
    picked = [lext[j, at, :] for j in range(BLOCKS)]
    center, around = [None] * BLOCKS, [None] * BLOCKS
    for k in range(K):
        tiles = [ext[k, j, at, :] for j in range(BLOCKS)]
        after, before = shifted(tiles)
        for j in range(BLOCKS):
            near_sum = ext[k, j, pl.ds(base + 1, 8), :] + ext[k, j, pl.ds(base - 1, 8), :]
            near_sum = near_sum + after[j] + before[j]
            here = picked[j] == k
            center[j] = jnp.where(here, tiles[j], center[j]) if k else tiles[j]
            around[j] = jnp.where(here, near_sum, around[j]) if k else near_sum
    for j in range(BLOCKS):
        out[j, at, :] = 4.0 * center[j] - around[j]


def neighbours(source, target, base):
    tiles = [source[j, pl.ds(base, 8), :] for j in range(BLOCKS)]
    after, before = shifted(tiles)
    for j in range(BLOCKS):
        vertical = source[j, pl.ds(base + 1, 8), :] + source[j, pl.ds(base - 1, 8), :]
        target[j, pl.ds(base, 8), :] = vertical + after[j] + before[j]


def over_tiles(first, last, chunk, step, carry):
    def turn_of(t, carry):
        for u in range(chunk):
            carry = step(pl.multiple_of(TOP + 8 * first + 8 * (chunk * t + u), 8), carry)
        return carry

    return lax.fori_loop(0, (last - first + 1) // chunk, turn_of, carry)


def tree(x):
    while len(x) > 1:
        x = [sum(x[a : a + 2][1:], x[a]) for a in range(0, len(x), 2)]
    return x[0]


def products(v0, v1, v2, base, totals):
    lane = iota((8, LANES), 1)
    last = lane == LANES - 1
    kept = {0: lane >= HALO, BLOCKS - 1: lane < LANES - HALO}
    at = pl.ds(base, 8)
    found = [[] for _ in PAIRS]
    rolled = [turn(v2[j, at, :], -1) for j in range(BLOCKS)]
    for j in range(BLOCKS):
        x = [v[j, at, :] for v in (v0, v1, v2)]
        right = jnp.where(last, rolled[min(j + 1, BLOCKS - 1)], rolled[j])
        x.append(v2[j, pl.ds(base + 1, 8), :] + right)
        own = [jnp.where(kept[j], a, 0.0) for a in x[:3]] if j in kept else x
        for i, (a, b) in enumerate(PAIRS):
            found[i].append(own[a] * x[b])
    return tuple(total + tree(f) for total, f in zip(totals, found))


def seam_base(ext, lext, out, tile):
    lane = iota((8, LANES), 1)
    at = pl.ds(TOP + 8 * tile, 8)
    for k in range(K + 1):
        a, b = [ext[k, j, at, :] if k < K else lext[j, at, :].astype(f32) for j in (0, BLOCKS - 1)]
        out[k, at, :] = jnp.where(lane < 64, turn(a, LEFT), turn(b, RIGHT + SEAM))


def clear_rows(ref, row):
    @pl.when(row == 0)
    def _():
        for j in range(BLOCKS):
            ref[j, pl.ds(TOP - 8, 8), :] = jnp.zeros((8, LANES), f32)

    @pl.when(row == 31)
    def _():
        for j in range(BLOCKS):
            ref[j, pl.ds(TOP + H, 8), :] = jnp.zeros((8, LANES), f32)


def inner_kernel(*refs):
    r_even, r_odd, totals_in = refs[6:9]
    ext, lext, v0, v1, v2, seam_out, totals_out = refs[9:]
    row, _ = place()
    row_even = (row % 2) == 0
    for k in range(K + 1):
        at = pl.ds(HALO * k, HALO)
        for j in range(BLOCKS):
            lanes = pl.ds(j * LANES, LANES)
            e, o = r_even[at, lanes], r_odd[at, lanes]
            above, below = jnp.where(row_even, o, e), jnp.where(row_even, e, o)
            for start, value in ((TOP - HALO, above), (TOP + H, below)):
                if k < K:
                    ext[k, j, pl.ds(start, HALO), :] = value
                else:
                    lext[j, pl.ds(start, HALO), :] = value.astype(jnp.int32)
    seam_base(ext, lext, seam_out, -1)
    seam_base(ext, lext, seam_out, TILES)
    for t in (-1, 0, TILES - 1, TILES):
        right_side(ext, lext, v0, TOP + 8 * t)
    clear_rows(v0, row)
    for t in (-1, 0, 1, TILES - 2, TILES - 1, TILES):
        neighbours(v0, v1, TOP + 8 * t)
    clear_rows(v1, row)
    for t in (-1, 0, 1, 2, TILES - 3, TILES - 2, TILES - 1, TILES):
        neighbours(v1, v2, TOP + 8 * t)
    clear_rows(v2, row)
    totals = tuple(totals_in[i] for i in range(6))
    for t in (0, 1, 2, *range(TILES - 4, TILES)):
        totals = products(v0, v1, v2, TOP + 8 * t, totals)
    for i in range(6):
        totals_out[i] = totals[i]


def inner(ext, lext, v0, v1, v2, base, r_even, r_odd, totals):
    field = near((BLOCKS, ROWS, LANES))
    return pl.pallas_call(
        inner_kernel,
        out_shape=(
            near((K, BLOCKS, ROWS, LANES)),
            near((BLOCKS, ROWS, LANES), jnp.int32),
            field,
            field,
            field,
            near((K + 1, ROWS, LANES)),
            near((6, 8, LANES)),
        ),
        in_specs=[WHOLE] * 9,
        out_specs=(WHOLE,) * 7,
        input_output_aliases={i: i for i in range(6)},
        compiler_params=LIMIT,
        cost_estimate=cost(2),
        name="inner_fields",
    )(*held(ext, lext, v0, v1, v2, base, r_even, r_odd, totals))[2:]


def seam_kernel(base, totals_in, c_even, c_odd, w, sums_out, planes):
    row, col = place()
    col_even = (col % 2) == 0
    lane = iota((8, LANES), 1)
    from_left, from_right = lane < LEFT, window(lane, RIGHT + SEAM, HALO)
    outside = (from_left & (col == 0)) | (from_right & (col == 7))
    for t in range(TILES + 2):
        at = pl.ds(TOP - 8 + 8 * t, 8)
        corner = t in (0, TILES + 1)
        tile, g = (2, 0) if corner else divmod(t - 1, 8)
        e, o = c_even[pl.ds(8 * tile, 8), :], c_odd[pl.ds(8 * tile, 8), :]
        a, b = jnp.where(col_even, o, e), jnp.where(col_even, e, o)
        if corner:
            a, b = pltpu.roll(a, HALO, 0), pltpu.roll(b, HALO, 0)
        for k in range(K + 1):
            lanes = 16 * g + HALO * k
            planes[k, at, :] = jnp.where(
                from_left,
                turn(a, -lanes),
                jnp.where(from_right, turn(b, RIGHT + SEAM - lanes), base[k, at, :]),
            )

    def put(i, t, value):
        hidden = outside
        if t == 0:
            hidden = hidden | (row == 0)
        if t == TILES + 1:
            hidden = hidden | (row == 31)
        w[i, pl.ds(TOP - 8 + 8 * t, 8), :] = jnp.where(hidden, 0.0, value)

    for t in range(TILES + 2):
        start = TOP - 8 + 8 * t
        total = jnp.zeros((8, LANES), f32)
        picked = planes[K, pl.ds(start, 8), :]
        for k in range(K):
            x = planes[k, pl.ds(start, 8), :]
            vertical = planes[k, pl.ds(start + 1, 8), :] + planes[k, pl.ds(start - 1, 8), :]
            term = 4.0 * x - (vertical + turn(x, -1) + turn(x, 1))
            total = jnp.where(picked == k, term, total)
        put(0, t, total)
    for i in range(2):
        for t in range(TILES + 2):
            start = TOP - 8 + 8 * t
            x = w[i, pl.ds(start, 8), :]
            vertical = w[i, pl.ds(start + 1, 8), :] + w[i, pl.ds(start - 1, 8), :]
            put(i + 1, t, vertical + turn(x, -1) + turn(x, 1))
    own_lane = window(lane, LEFT, HALO) | window(lane, RIGHT + SEAM - HALO, HALO)
    found = [[] for _ in PAIRS]
    for t in range(TILES):
        start = TOP + 8 * t
        x = [w[i, pl.ds(start, 8), :] for i in range(3)]
        x.append(w[2, pl.ds(start + 1, 8), :] + turn(x[2], -1))
        for i, (a, b) in enumerate(PAIRS):
            found[i].append(x[a] * x[b])
    totals = [totals_in[i] + jnp.where(own_lane, tree(found[i]), 0.0) for i in range(6)]

    line = jnp.zeros((8, LANES), f32)
    for i in range(6):
        x = totals[i] + totals[i] if i == 5 else totals[i]
        big = 512.0 * jnp.max(jnp.abs(x), axis=1, keepdims=True)
        high = (x + big) - big
        line = jnp.where(
            (lane == i) | (lane == i + 16) | (lane == i + 24),
            jnp.sum(high, axis=1, keepdims=True),
            jnp.where(lane == i + 8, jnp.sum(x - high, axis=1, keepdims=True), line),
        )
    s, e = line, jnp.zeros_like(line)
    for shift in (4, 2, 1):
        s, more = two_sum(s, pltpu.roll(s, shift, 0))
        e = e + pltpu.roll(e, shift, 0) + more
    sums_out[...] = jnp.where(lane < 24, s, e)


def seam(base, totals, c_even, c_odd):
    return pl.pallas_call(
        seam_kernel,
        out_shape=(near((3, ROWS, LANES)), near((8, LANES))),
        in_specs=[WHOLE] * 4,
        out_specs=(WHOLE,) * 2,
        scratch_shapes=[pltpu.VMEM((K + 1, ROWS, LANES), f32)],
        compiler_params=LIMIT,
        cost_estimate=cost(1),
        name="seam_fields",
    )(*held(base, totals, c_even, c_odd))


def merge_kernel(own, other, out):
    s, e = two_sum(own[...], other[...])
    line = jnp.where(window(iota((8, LANES), 1), 16, 8), e, s)
    out[...] = jnp.broadcast_to(line[:1].reshape(1, 1, LANES), (128, 1, LANES))


def merge(own, other):
    return pl.pallas_call(
        merge_kernel,
        out_shape=near((128, 1, LANES)),
        in_specs=[WHOLE] * 2,
        out_specs=WHOLE,
        compiler_params=LIMIT,
        cost_estimate=cost(0.2),
        name="merge_cores",
    )(*held(own, other))


def pool_kernel(v0, v1, v2, out):
    spread = jnp.where(iota((512, LANES), 0) // 4 == iota((512, LANES), 1), f32(0.0625), f32(0.0))
    for i, ref in enumerate((v0, v1, v2)):
        for g in range(2):
            parts = []
            for j in range(4):
                at = [ref[4 * g + j, pl.ds(TOP + q, H // 4, stride=4), :] for q in range(4)]
                parts.append((at[0] + at[1]) + (at[2] + at[3]))
            out[i, g] = sums_of(jnp.concatenate(parts, 1), spread.astype(jnp.bfloat16))


def pool(v0, v1, v2):
    return pl.pallas_call(
        pool_kernel,
        out_shape=near((3, 2, H // 4, LANES)),
        in_specs=[WHOLE] * 3,
        out_specs=WHOLE,
        compiler_params=LIMIT,
        cost_estimate=cost(1),
        name="pool_fields",
    )(*held(v0, v1, v2))


def two_product(a, b):
    p = a * b
    big = f32(4097.0)
    t = big * a
    ah = t - (t - a)
    al = a - ah
    t = big * b
    bh = t - (t - b)
    bl = b - bh
    return p, ((ah * bh - p) + ah * bl + al * bh) + al * bl


def less_scaled(a, b, scale):
    p, low = two_product(b[0], scale)
    low = low + b[1] * scale
    s, e = two_sum(a[0], -p)
    e = e + (a[1] - low)
    return two_sum(s, e)


def coefficients(n):
    shift = n[1][0] / n[0][0]
    current = n
    m = [n[0][0]]
    for _ in range(5):
        current = [less_scaled(current[i + 1], current[i], shift) for i in range(len(current) - 1)]
        m.append(current[0][0] + current[0][1])
    m0, m1, m2, m3, m4, m5 = m
    t = m1 / m0
    theta0 = shift + t
    m5 = m5 - 5.0 * t * m4
    m4 = m4 - 4.0 * t * m3
    m3 = m3 - 3.0 * t * m2
    m2 = m2 - t * m1
    one = jnp.ones_like(m0)
    zero = jnp.zeros_like(m0)
    second = m2 > 0.0
    safe2 = jnp.where(second, m2, one)
    b1 = jnp.where(second, m2 / m0, zero)
    s = jnp.where(second, m3 / safe2, zero)
    h2 = m4 - s * m3 - b1 * m2
    third = second & (h2 > 0.0)
    safe3 = jnp.where(third, h2, one)
    theta1 = jnp.clip(theta0 + s, -4.0, 4.0)
    theta2 = jnp.clip(theta0 - s + (m5 - s * m4 - b1 * m3) / safe3, -4.0, 4.0)
    b2 = h2 / safe2
    d0, d1, d2 = 4.0 - theta0, 4.0 - theta1, 4.0 - theta2
    e = d1 * d2 - b2
    two, three = d0 * d1 - b1, d0 * e - b1 * d2
    second = second & (two > 0.0)
    third = second & third & (three > 0.0)
    y2 = jnp.where(third, one / three, zero)
    y1 = jnp.where(third, d2 * y2, jnp.where(second, one / two, zero))
    y0 = jnp.where(third, e * y2, jnp.where(second, d1 * y1, one / d0))
    return (
        y0 - theta0 * y1 + (theta0 * theta1 - b1) * y2,
        y1 - (theta0 + theta1) * y2,
        y2,
    )


def solve_kernel(all_sums, pooled, w, coef_out, mid_out):
    frm, to = iota((LANES, LANES), 0), iota((LANES, LANES), 1)
    first = window(frm, LEFT, HALO) & (to == 0)
    final = window(frm, RIGHT + SEAM - HALO, HALO) & (to == LANES - 1)
    rows = []
    for i in range(3):
        at = [w[i, pl.ds(TOP + q, H // 4, stride=4), :] for q in range(4)]
        rows.append((at[0] + at[1]) + (at[2] + at[3]))
    weights = jnp.where(first | final, f32(0.0625), f32(0.0)).astype(jnp.bfloat16)
    edges = sums_of(jnp.concatenate(rows, 0), weights)
    tiles = [(all_sums[pl.ds(8 * i, 8), :], jnp.zeros((8, LANES), f32)) for i in range(16)]
    while len(tiles) > 1:
        merged = []
        for a, b in zip(tiles[0::2], tiles[1::2]):
            s, e = two_sum(a[0], b[0])
            merged.append((s, e + (a[1] + b[1])))
        tiles = merged
    s, e = tiles[0]
    for shift in (4, 2, 1):
        s, more = two_sum(s, pltpu.roll(s, shift, 0))
        e = e + pltpu.roll(e, shift, 0) + more
    lane = iota((8, LANES), 1)
    zero = jnp.zeros((8, LANES), f32)

    def over_lanes(x):
        return jnp.broadcast_to(jnp.sum(x, axis=1, keepdims=True), (8, LANES))

    n = []
    for i in range(6):
        high = over_lanes(jnp.where(lane == i, s, zero))
        low = over_lanes(
            jnp.where((lane == i + 8) | (lane == i + 16) | (lane == i + 24), s, jnp.where(lane == i, e, zero))
        )
        n.append(two_sum(high, low))
    c = coefficients(n)
    for i in range(3):
        coef_out[i] = c[i]
    for g in range(2):
        edge = lane == (LANES - 1 if g else 0)
        for q in range(H // 4 // 8):
            at = (g, pl.ds(8 * q, 8), slice(None))
            value = zero
            for i in range(3):
                start = H // 4 * i + 8 * q
                value = value + c[i] * jnp.where(edge, edges[start : start + 8], pooled[(i, *at)])
            for d in range(16):
                mid_out[(d, *at)] = value


def solve(all_sums, pooled, w):
    return pl.pallas_call(
        solve_kernel,
        out_shape=(near((3, 8, LANES)), near((16, 2, H // 4, LANES))),
        in_specs=[WHOLE] * 3,
        out_specs=(WHOLE,) * 2,
        compiler_params=LIMIT,
        cost_estimate=cost(1),
        name="coefficients",
    )(*held(all_sums, pooled, w))


def half_matrix(rows):
    return jnp.where(iota((rows, rows // 2), 0) // 2 == iota((rows, rows // 2), 1), f32(0.25), f32(0.0))


def pooled_rows(parts):
    return sums_of(jnp.concatenate(parts, 1), half_matrix(2 * LANES).astype(jnp.bfloat16))


def store_mid(x, core, mid_out, sem):
    copies = []
    for g in range(2):
        to = mid_out.at[:, core, :, pl.ds(g * LANES, LANES)]
        copies.append(pltpu.make_async_copy(x.at[:, g], to, sem.at[g]))
        copies[-1].start()
    return copies


def store_coarse(x, core, coarse_out, scratch, sem):
    rows = H // 8
    parts = [
        jnp.concatenate(
            [x[d, g, pl.ds(0, rows, stride=2), :] + x[d, g, pl.ds(1, rows, stride=2), :] for d in range(16)], 0
        )
        for g in range(2)
    ]
    pooled = pooled_rows(parts)
    for d in range(16):
        scratch[d] = pooled[d * rows : (d + 1) * rows]
    copy = pltpu.make_async_copy(scratch, coarse_out.at[:, core], sem)
    copy.start()
    return copy


def own_kernel(
    x, coef, v0, v1, v2, w, blended_out, fine_out, mid_out, coarse_out, flat, stacked, fine, coarse, sem
):
    core = lax.axis_index("row_2")
    copies = store_mid(x, core, mid_out, sem)
    c = [coef[i] for i in range(3)]
    lane = iota((8, LANES), 1)
    parts = 4
    for p in range(parts):
        for u in range(TILES // parts):
            base = 8 * (p * (TILES // parts) + u)
            rows = pl.ds(base + TOP, 8)
            seams = c[0] * w[0, rows, :] + c[1] * w[1, rows, :] + c[2] * w[2, rows, :]
            for j in range(BLOCKS):
                at = (j, rows, slice(None))
                value = c[0] * v0[at] + c[1] * v1[at] + c[2] * v2[at]
                if j == 0:
                    value = jnp.where(lane < HALO, turn(seams, -LEFT), value)
                if j == BLOCKS - 1:
                    value = jnp.where(lane >= LANES - HALO, turn(seams, LANES - RIGHT - SEAM), value)
                flat[pl.ds(base, 8), pl.ds(j * LANES, LANES)] = value
                stacked[j, pl.ds(base, 8), :] = value
        rows = pl.ds(p * H // parts, H // parts)
        copies.append(pltpu.make_async_copy(flat.at[rows, :], blended_out.at[rows, :], sem.at[3 + p]))
        copies[-1].start()
    for g in range(BLOCKS // 2):
        halves = [
            stacked[2 * g + i, pl.ds(0, H // 2, stride=2), :] + stacked[2 * g + i, pl.ds(1, H // 2, stride=2), :]
            for i in range(2)
        ]
        fine[:, pl.ds(g * LANES, LANES)] = pooled_rows(halves)
    copies.append(pltpu.make_async_copy(fine, fine_out, sem.at[3 + parts]))
    copies[-1].start()
    copies.append(store_coarse(x, core, coarse_out, coarse, sem.at[2]))
    for copy in copies:
        copy.wait()


LEVELS = (
    jax.ShapeDtypeStruct((16, 2, H // 4, W // 4), f32),
    jax.ShapeDtypeStruct((16, 2, H // 8, W // 8), f32),
)


def own_levels(x, coef, v0, v1, v2, w):
    return pl.pallas_call(
        own_kernel,
        out_shape=(
            jax.ShapeDtypeStruct((H, W), f32),
            jax.ShapeDtypeStruct((H // 2, W // 2), f32),
            *LEVELS,
        ),
        in_specs=[WHOLE] * 6,
        out_specs=(FAR,) * 4,
        scratch_shapes=[
            pltpu.VMEM((H, W), f32),
            pltpu.VMEM((BLOCKS, H, LANES), f32),
            pltpu.VMEM((H // 2, W // 2), f32),
            pltpu.VMEM((16, H // 8, LANES), f32),
            pltpu.SemaphoreType.DMA((8,)),
        ],
        compiler_params=LIMIT,
        cost_estimate=cost(2),
        name="own_levels",
    )(*held(x, coef, v0, v1, v2, w))


def other_kernel(x, mid_in, coarse_in, mid_out, coarse_out, coarse, sem):
    del mid_in, coarse_in
    core = 1 - lax.axis_index("row_2")
    copies = store_mid(x, core, mid_out, sem)
    copies.append(store_coarse(x, core, coarse_out, coarse, sem.at[2]))
    for copy in copies:
        copy.wait()


def other_levels(x, mid, coarse):
    return pl.pallas_call(
        other_kernel,
        out_shape=LEVELS,
        in_specs=[WHOLE, FAR, FAR],
        out_specs=(FAR,) * 2,
        scratch_shapes=[
            pltpu.VMEM((16, H // 8, LANES), f32),
            pltpu.SemaphoreType.DMA((3,)),
        ],
        input_output_aliases={1: 0, 2: 1},
        compiler_params=LIMIT,
        cost_estimate=cost(1),
        name="other_levels",
    )(*held(x), *far(mid, coarse))


def swaps(devices, first):
    pairs = [(i, i + 1) for i in range(first, devices - 1, 2)]
    return pairs + [(b, a) for a, b in pairs]


def exchange(even, odd, axis):
    devices = lax.axis_size(axis)
    odd = lax.ppermute(odd, axis, swaps(devices, 1))
    even = lax.ppermute(even, axis, swaps(devices, 0))
    return even, odd


def per_device(sources, labels):
    even, odd = pack_rows(sources, labels)
    even, odd, planes, marks = lax.optimization_barrier((even, odd, sources, labels))
    r_even, r_odd = exchange(even, odd, ROW)
    ext, lext, left, right, v0, v1, v2, totals, base = load(planes, marks)
    c_even, c_odd = exchange(*pack_columns(r_even, r_odd, left, right), "col")
    v0, v1, v2, base, totals = inner(ext, lext, v0, v1, v2, base, r_even, r_odd, totals)
    w, sums = seam(base, totals, c_even, c_odd)
    swapped = lax.ppermute(sums, "row_2", [(0, 1), (1, 0)])
    pooled, sums = lax.optimization_barrier((pool(v0, v1, v2), sums))
    sums = merge(sums, swapped)
    sums = lax.all_to_all(sums, (*CHIP, "col"), split_axis=0, concat_axis=0, tiled=True)
    coef, mid = solve(sums.reshape(128, LANES), pooled, w)
    mid = lax.all_to_all(mid, CHIP, split_axis=0, concat_axis=0, tiled=True)
    other = lax.ppermute(mid, "row_2", [(0, 1), (1, 0)])
    blended, fine, overview_mid, overview_coarse = own_levels(mid, coef, v0, v1, v2, w)
    overview_mid, overview_coarse = other_levels(other, overview_mid, overview_coarse)
    overview_mid = overview_mid.reshape(8 * H, W // 4)
    overview_coarse = overview_coarse.reshape(4 * H, W // 8)
    return (blended, fine, overview_mid, overview_coarse)


def solution(mesh):
    finer = Mesh(
        mesh.devices.reshape(4, 4, 2, mesh.shape["col"]), ("row_0", "row_1", "row_2", "col")
    )
    return jax.shard_map(
        per_device,
        mesh=finer,
        in_specs=(P(None, ROW, "col"), P(ROW, "col")),
        out_specs=(P(ROW, "col"), P(ROW, "col"), P(None, "col"), P(None, "col")),
        check_vma=False,
    )
```
